256 devices in a mesh: dp: 32 (over z, y), mp: 8 (over x, core).
Axes of the slice: x: 4, y: 4, z: 8, core: 2. Of those that a mesh axis runs over, the one named last changes fastest.
Arguments:
- queries: bfloat16 [512, 8192], P('dp', 'mp'), may hold values from -8 to 8
- incoming_key: bfloat16 [512, 1024], P('dp', 'mp'), may hold values from -4 to 4
- incoming_value: bfloat16 [512, 1024], P('dp', 'mp'), may hold values from -4 to 4
- key_cache: bfloat16 [1024, 256, 1024], P('dp', None, 'mp'), may hold values from -8 to 8
- cached_values: bfloat16 [1024, 256, 1024], P('dp', None, 'mp'), may hold values from -4 to 4
- task_key_scale: bfloat16 [256, 1024], P(None, 'mp'), may hold values from 0.099609375 to 1.8984375
- task_value_scale: bfloat16 [256, 1024], P(None, 'mp'), may hold values from 0.099609375 to 1.8984375
- out_weight: bfloat16 [8192, 8192], P('mp', 'dp'), may hold values from -0.0625 to 0.0625
- task_id: int32 [512], P('dp'), may hold values from 0 to 255, as said below
- cached_length: int32 [512], P('dp'), may hold values from 1 to 256, as said below
- task_owner: int32 [256], replicated, may hold values from 0 to 31, as said below
- cache_slot: int32 [512], P('dp'), may hold values from 0 to 31, as said below
Outputs:
- layer_out: bfloat16 [512, 8192], P('dp', 'mp')
The draws below stay inside these ranges and needn't reach their ends.
Inputs may be any that keep to these rules, and one draw needn't show every extreme that they name: `task_owner`: every dp index owns the same number of tasks. `task_id`: among the 16 requests of one dp index at most 1 have tasks of one owner; in every draw one owner gets exactly 1 from every dp index. `cache_slot`: requests of one owner have distinct slots; one owner uses all 32. `cached_length`: every dp index has a request with 256 cached positions.
All inputs are finite; a program needn't handle non-finite values.
Results may differ from the reference program's by a relative error of at most 0.0073.
Values may be sent and summed in bfloat16 or wider, within the bound.
A program may use at most 128 MiB of HBM per device.

```python
import math
import jax
import jax.numpy as jnp
from jax import lax

D = 8192
KEY_VALUE_HEADS = 8
HEAD_SIZE = 128
QUERY_HEADS = 64
TASK_TOTAL = 256
REQUESTS_PER_DP = 16
MAX_POSITIONS = 256
QUERY_PER_KV = 8
REQUEST_TOTAL = 512
CAP = 1
OWN_CAP = 32
CACHE_ROWS = 1024
N_DP = 32


def routing(key):
    shuffle = jax.random.permutation(jax.random.fold_in(key, 11), TASK_TOTAL)
    task_owner = (shuffle % N_DP).astype(jnp.int32)
    hot_owner = jax.random.randint(jax.random.fold_in(key, 12), (), 0, N_DP)
    position = jnp.arange(REQUESTS_PER_DP)
    rotation = jax.random.randint(jax.random.fold_in(key, 13), (N_DP, 1), 0, N_DP - 1)
    others = (hot_owner + 1 + (position[None, :] - CAP + rotation) % (N_DP - 1)) % N_DP
    owners_block = jnp.where(position[None, :] < CAP, hot_owner, others)
    block_keys = jax.random.split(jax.random.fold_in(key, 14), N_DP)
    orders = jax.vmap(lambda one_key: jax.random.permutation(one_key, REQUESTS_PER_DP))(block_keys)
    owners = jnp.take_along_axis(owners_block, orders, axis=1).reshape(REQUEST_TOTAL)
    within = jax.random.randint(jax.random.fold_in(key, 15), (REQUEST_TOTAL,), 0, TASK_TOTAL // N_DP)
    inverse = jnp.argsort(shuffle)
    task_id = inverse[owners + N_DP * within].astype(jnp.int32)
    mixing = jax.random.permutation(jax.random.fold_in(key, 16), REQUEST_TOTAL)
    ranking = jnp.argsort(owners * REQUEST_TOTAL + mixing)
    sorted_owner = owners[ranking]
    counts = jnp.sum((sorted_owner[:, None] == jnp.arange(N_DP)[None, :]).astype(jnp.int32), axis=0)
    starts = jnp.cumsum(counts) - counts
    rank_sorted = jnp.arange(REQUEST_TOTAL) - starts[sorted_owner]
    cache_slot = jnp.zeros((REQUEST_TOTAL,), jnp.int32).at[ranking].set(rank_sorted.astype(jnp.int32))
    return (task_owner, task_id, cache_slot)


def draw_task_owner(key, part):
    return routing(key)[0]


def draw_task_id(key, part):
    return routing(key)[1]


def draw_cache_slot(key, part):
    return routing(key)[2]


def draw_cached_length(key, part):
    lengths = jax.random.randint(jax.random.fold_in(key, 21), (N_DP, REQUESTS_PER_DP), 1, MAX_POSITIONS + 1)
    longest = jax.random.randint(jax.random.fold_in(key, 22), (N_DP, 1), 0, REQUESTS_PER_DP)
    lengths = jnp.where(jnp.arange(REQUESTS_PER_DP)[None, :] == longest, MAX_POSITIONS, lengths)
    return lengths.reshape(REQUEST_TOTAL).astype(jnp.int32)


def draw_queries(key, part):
    random_noise = jax.random.normal(jax.random.fold_in(key, 32), (REQUEST_TOTAL, QUERY_HEADS * HEAD_SIZE), jnp.float32)
    value_rows = jnp.clip(2.0 * random_noise, -6.0, 6.0)
    return value_rows.astype(jnp.bfloat16)


def draw_key_cache(key, part):
    random_noise = jax.random.normal(jax.random.fold_in(key, 33), (CACHE_ROWS, MAX_POSITIONS, KEY_VALUE_HEADS * HEAD_SIZE), jnp.float32)
    value_rows = jnp.clip(random_noise, -4.0, 4.0)
    return value_rows.astype(jnp.bfloat16)


def block_levels(key, dims, cuts, least, top_value):
    loudness, own = 1.0, jax.random.fold_in(key, 6)
    for dim, shards_of in cuts:
        draws = jnp.exp(jax.random.uniform(jax.random.fold_in(own, dim), (shards_of,), jnp.float32, least / len(cuts), top_value / len(cuts)))
        loudness = loudness * jnp.repeat(draws, dims[dim] // shards_of).reshape([-1 if axis == dim else 1 for axis in range(len(dims))])
    return loudness


def normal_values(stream_key, shape, scale, most, pieces=(), kind=jnp.bfloat16):
    values = jax.random.normal(stream_key, shape, jnp.float32) * scale
    if len(pieces) > 0:
        values = block_levels(stream_key, shape, pieces, -0.22, 0.18) * values
    return jnp.clip(values, min=-most, max=most).astype(kind)


def setup_inputs(seed: int = 0) -> dict:
    streams_of = jax.random.split(jax.random.key(seed), 13)
    return {
        "queries": draw_queries(jax.random.fold_in(streams_of[12], 71), 0),
        "incoming_key": normal_values(streams_of[1], (REQUEST_TOTAL, KEY_VALUE_HEADS * HEAD_SIZE), 1.0, 4.0, ((0, 32), (1, 8))),
        "incoming_value": normal_values(streams_of[2], (REQUEST_TOTAL, KEY_VALUE_HEADS * HEAD_SIZE), 1.0, 4.0, ((0, 32), (1, 8))),
        "key_cache": draw_key_cache(jax.random.fold_in(streams_of[12], 71), 0),
        "cached_values": normal_values(streams_of[4], (CACHE_ROWS, MAX_POSITIONS, KEY_VALUE_HEADS * HEAD_SIZE), 1.0, 4.0, ((0, 32), (2, 8))),
        "task_key_scale": jnp.clip(1.0 + 0.18 * jax.random.normal(streams_of[5], (TASK_TOTAL, KEY_VALUE_HEADS * HEAD_SIZE), jnp.float32), 0.099609375, 1.8984375).astype(jnp.bfloat16),
        "task_value_scale": jnp.clip(1.0 + 0.18 * jax.random.normal(streams_of[6], (TASK_TOTAL, KEY_VALUE_HEADS * HEAD_SIZE), jnp.float32), 0.099609375, 1.8984375).astype(jnp.bfloat16),
        "out_weight": normal_values(streams_of[7], (QUERY_HEADS * HEAD_SIZE, D), (QUERY_HEADS * HEAD_SIZE) ** -0.5, 0.0625, ((0, 8), (1, 32))),
        "task_id": draw_task_id(jax.random.fold_in(streams_of[12], 71), 0),
        "cached_length": draw_cached_length(jax.random.fold_in(streams_of[12], 71), 0),
        "task_owner": draw_task_owner(jax.random.fold_in(streams_of[12], 71), 0),
        "cache_slot": draw_cache_slot(jax.random.fold_in(streams_of[12], 71), 0),
    }


masked_score = -1e+30

def lowered_program(value_rows):
    return lax.optimization_barrier(value_rows.astype(jnp.bfloat16))

def attend(queries, fresh_key_rows, fresh_value_rows, stored_key_rows, stored_value_rows, lengths):
    entry_count = queries.shape[0]
    inv_root = 1.0 / math.sqrt(HEAD_SIZE)
    query_head_rows = queries.astype(jnp.float32).reshape(entry_count, KEY_VALUE_HEADS, QUERY_PER_KV, HEAD_SIZE)
    previous_keys = stored_key_rows.astype(jnp.float32).reshape(entry_count, MAX_POSITIONS, KEY_VALUE_HEADS, HEAD_SIZE)
    previous_values = stored_value_rows.astype(jnp.float32).reshape(entry_count, MAX_POSITIONS, KEY_VALUE_HEADS, HEAD_SIZE)
    incoming_keys = fresh_key_rows.astype(jnp.float32).reshape(entry_count, KEY_VALUE_HEADS, HEAD_SIZE)
    incoming_values = fresh_value_rows.astype(jnp.float32).reshape(entry_count, KEY_VALUE_HEADS, HEAD_SIZE)
    scores = jnp.einsum('ngqd,njgd->ngqj', query_head_rows, previous_keys, precision=lax.Precision.HIGHEST) * inv_root
    own_score = jnp.einsum('ngqd,ngd->ngq', query_head_rows, incoming_keys, precision=lax.Precision.HIGHEST) * inv_root
    visible = jnp.arange(MAX_POSITIONS)[None, None, None, :] < lengths[:, None, None, None]
    scores = jnp.where(visible, scores, masked_score)
    top_score = jnp.maximum(lax.optimization_barrier(jnp.max(scores, axis=3)), own_score)
    weights = jnp.where(visible, jnp.exp(scores - top_score[..., None]), 0.0)
    own_weight = jnp.exp(own_score - top_score)
    weight_sum = lax.optimization_barrier(jnp.sum(weights, axis=3)) + own_weight
    blended = jnp.einsum('ngqj,njgd->ngqd', lowered_program(weights).astype(jnp.float32), previous_values, precision=lax.Precision.HIGHEST)
    blended = blended + lowered_program(own_weight).astype(jnp.float32)[..., None] * incoming_values[:, :, None, :]
    return (blended / weight_sum[..., None]).astype(jnp.bfloat16).reshape(entry_count, QUERY_HEADS * HEAD_SIZE)

def reference(queries, incoming_key, incoming_value, key_cache, cached_values, task_key_scale, task_value_scale, out_weight, task_id, cached_length, task_owner, cache_slot):
    owner_of = jnp.take(task_owner, task_id).astype(jnp.int32)
    owner_row_index = (owner_of * OWN_CAP + cache_slot).astype(jnp.int32)
    key_factor = jnp.take(task_key_scale, task_id, axis=0).astype(jnp.float32)
    value_factor = jnp.take(task_value_scale, task_id, axis=0).astype(jnp.float32)
    scaled_rows = lowered_program((queries.astype(jnp.float32).reshape(REQUEST_TOTAL, KEY_VALUE_HEADS, QUERY_PER_KV, HEAD_SIZE) * key_factor.reshape(REQUEST_TOTAL, KEY_VALUE_HEADS, 1, HEAD_SIZE)).reshape(REQUEST_TOTAL, QUERY_HEADS * HEAD_SIZE))

    def block_kernel(members):
        block_queries, block_keys, block_values, block_rows, block_lengths = members
        stored_key_rows = jnp.take(key_cache, block_rows, axis=0)
        stored_value_rows = jnp.take(cached_values, block_rows, axis=0)
        return attend(block_queries, block_keys, block_values, stored_key_rows, stored_value_rows, block_lengths)
    attention_output = lax.map(block_kernel, (scaled_rows.reshape(N_DP, REQUESTS_PER_DP, QUERY_HEADS * HEAD_SIZE), incoming_key.reshape(N_DP, REQUESTS_PER_DP, KEY_VALUE_HEADS * HEAD_SIZE), incoming_value.reshape(N_DP, REQUESTS_PER_DP, KEY_VALUE_HEADS * HEAD_SIZE), owner_row_index.reshape(N_DP, REQUESTS_PER_DP), cached_length.reshape(N_DP, REQUESTS_PER_DP)))
    attention_output = attention_output.reshape(REQUEST_TOTAL, QUERY_HEADS * HEAD_SIZE)
    context_rows = lowered_program((attention_output.astype(jnp.float32).reshape(REQUEST_TOTAL, KEY_VALUE_HEADS, QUERY_PER_KV, HEAD_SIZE) * value_factor.reshape(REQUEST_TOTAL, KEY_VALUE_HEADS, 1, HEAD_SIZE)).reshape(REQUEST_TOTAL, QUERY_HEADS * HEAD_SIZE))
    return jnp.dot(context_rows, out_weight, preferred_element_type=jnp.float32).astype(jnp.bfloat16)
```

```python
import functools
import math

import jax
import jax.numpy as jnp
from jax import lax
from jax.experimental import pallas as pl
from jax.experimental.pallas import tpu as pltpu
from jax.sharding import PartitionSpec as P

HEAD_SIZE = 128
META = 128
TOGETHER = 8
MESH = pl.DeviceIdType.MESH

masked_score = -1e30
f32 = jnp.float32
bf16 = jnp.bfloat16


def iota(shape, dim):
    return lax.broadcasted_iota(jnp.int32, shape, dim)


def to_column(row):
    n = row.shape[1]
    eye = iota((n, n), 0) == iota((n, n), 1)
    return jnp.sum(jnp.where(eye, row, 0.0), axis=1, keepdims=True)


def to_row(column):
    n = column.shape[0]
    eye = iota((n, n), 0) == iota((n, n), 1)
    return jnp.sum(jnp.where(eye, column, 0.0), axis=0, keepdims=True)


def dot(a, b):
    return jnp.dot(a, b, preferred_element_type=f32)


def one_hot(mask):
    return jnp.where(mask, 1.0, 0.0).astype(bf16)


def layer_kernel(
    dp,
    mp,
    query_ref,
    new_key_ref,
    new_value_ref,
    key_scale_ref,
    value_scale_ref,
    task_ref,
    length_ref,
    slot_ref,
    owner_ref,
    key_hbm,
    value_hbm,
    weight_hbm,
    out_ref,
    keys,
    values,
    weights_in,
    rows_f32,
    send_rows,
    recv_rows,
    slot_query,
    slot_small,
    slot_length,
    slot_context,
    home_f32,
    home_send,
    home_recv,
    contexts,
    send_part,
    recv_part,
    local_sem,
    request_send,
    request_recv,
    home_send_sem,
    home_recv_sem,
    weight_send,
    weight_recv,
    context_send,
    context_recv,
    part_send,
    part_recv,
):
    me = lax.axis_index("dp")
    part = lax.axis_index("mp")
    rows, query_width = query_ref.shape
    kv_width = new_key_ref.shape[1]
    heads = query_width // HEAD_SIZE
    task_total = key_scale_ref.shape[0]
    slots, positions, _ = keys.shape
    columns = weights_in.shape[3]
    meta_at = query_width + 2 * kv_width
    inner = dp // mp
    outer = mp
    z, y = me // inner, lax.rem(me, inner)

    with jax.named_scope("a_greet"):
        fetches = [
            pltpu.make_async_copy(key_hbm, keys, local_sem.at[0]),
            pltpu.make_async_copy(value_hbm, values, local_sem.at[1]),
            pltpu.make_async_copy(weight_hbm, weights_in.at[y], local_sem.at[2]),
        ]
        barrier = pltpu.get_barrier_semaphore()
        for k in range(1, dp):
            pl.semaphore_signal(
                barrier, inc=1, device_id=(lax.rem(me + k, dp), part), device_id_type=MESH
            )
        for k in range(1, mp):
            pl.semaphore_signal(
                barrier, inc=1, device_id=(me, lax.rem(part + k, mp)), device_id_type=MESH
            )
        for fetch in fetches:
            fetch.start()

    with jax.named_scope("b_pack"):
        task_column = to_column(task_ref[...].astype(f32))
        length_column = to_column(length_ref[...].astype(f32))
        slot_column = to_column(slot_ref[...].astype(f32))
        picked = task_column == iota((rows, task_total), 1).astype(f32)
        owner_column = jnp.sum(
            jnp.where(picked, owner_ref[...].astype(f32), 0.0), axis=1, keepdims=True
        )
        owner_row = to_row(owner_column)
        packer = one_hot(owner_row == iota((dp, rows), 0).astype(f32))
        unpacker = one_hot(owner_column == iota((rows, dp), 1).astype(f32))
        task_rows = one_hot(picked)
        key_factor = dot(task_rows, key_scale_ref[...])
        value_factor = dot(task_rows, value_scale_ref[...])
        for h in range(heads):
            lanes = slice(h * HEAD_SIZE, (h + 1) * HEAD_SIZE)
            scaled = (query_ref[:, lanes].astype(f32) * key_factor).astype(bf16)
            rows_f32[:, lanes] = dot(packer, scaled)
        rows_f32[:, query_width : query_width + kv_width] = dot(packer, new_key_ref[...])
        rows_f32[:, query_width + kv_width : meta_at] = dot(packer, new_value_ref[...])
        lane = iota((rows, META), 1)
        facts = jnp.where(lane == 0, slot_column + 1.0, 0.0) + jnp.where(
            lane == 1, length_column, 0.0
        )
        rows_f32[:, meta_at:] = dot(packer, facts.astype(bf16))
        for d in range(dp):
            send_rows[d] = rows_f32[d : d + 1, :].astype(bf16)

    with jax.named_scope("c_barwait"):
        pl.semaphore_wait(barrier, dp + mp - 2)

    def row_copy(source, target, sends, recvs, k):
        return pltpu.make_async_remote_copy(
            src_ref=source.at[lax.rem(me + k, dp)],
            dst_ref=target.at[me],
            send_sem=sends.at[k],
            recv_sem=recvs.at[k],
            device_id=(lax.rem(me + k, dp), part),
            device_id_type=MESH,
        )

    def row_arrival(source, target, sends, recvs, k):
        return pltpu.make_async_remote_copy(
            src_ref=source.at[0],
            dst_ref=target.at[lax.rem(me + dp - k, dp)],
            send_sem=sends.at[k],
            recv_sem=recvs.at[k],
            device_id=(lax.rem(me + k, dp), part),
            device_id_type=MESH,
        )

    request = (send_rows, recv_rows, request_send, request_recv)
    homeward = (home_send, home_recv, home_send_sem, home_recv_sem)

    up = z * inner + lax.rem(y + 1, inner)
    down = z * inner + lax.rem(y + inner - 1, inner)

    def weight_copy(k, block, half, target):
        return pltpu.make_async_remote_copy(
            src_ref=weights_in.at[block, half],
            dst_ref=weights_in.at[block, half],
            send_sem=weight_send.at[k],
            recv_sem=weight_recv.at[k],
            device_id=(target, part),
            device_id_type=MESH,
        )

    y_down, y_up = lax.rem(y + inner - 1, inner), lax.rem(y + 1, inner)
    y_far = lax.rem(y + 2, inner)

    with jax.named_scope("d_reqsend"):
        for k in range(1, dp):
            row_copy(*request, k).start()
        recv_rows[me] = send_rows[me]
        fetches[2].wait()
        weight_copy(0, y, 0, up).start()
        weight_copy(1, y, 1, down).start()
        slot_query[...] = jnp.zeros_like(slot_query)
    with jax.named_scope("e_reqwait"):
        for k in range(1, dp):
            row_arrival(*request, k).wait_recv()

    with jax.named_scope("f_place"):
        for s in range(dp):
            rows_f32[s : s + 1, :] = recv_rows[s].astype(f32)
        facts_in = rows_f32[:, meta_at:]
        placing_row = to_row(facts_in[:, 0:1])
        placer = one_hot(placing_row == iota((slots, dp), 0).astype(f32) + 1.0)
        chooser = one_hot(facts_in[:, 0:1] == iota((dp, slots), 1).astype(f32) + 1.0)
        for h in range(heads):
            slot_query[:, h, :] = dot(
                placer, rows_f32[:, h * HEAD_SIZE : (h + 1) * HEAD_SIZE].astype(bf16)
            )
        slot_small[0] = dot(placer, rows_f32[:, query_width : query_width + kv_width].astype(bf16))
        slot_small[1] = dot(placer, rows_f32[:, query_width + kv_width : meta_at].astype(bf16))
        slot_facts = dot(placer, facts_in.astype(bf16))
        slot_length[...] = jnp.broadcast_to(slot_facts[:, 1:2], (slots, positions))
        fetches[0].wait()
        fetches[1].wait()

    inv_root = 1.0 / math.sqrt(HEAD_SIZE)
    key_line = iota((heads, positions), 1).astype(f32)

    def attend(n, carry):
        picks = [n * TOGETHER + i for i in range(TOGETHER)]
        scores, owns, weights, own_weights, sums, tops = [], [], [], [], [], []
        for s in picks:
            scores.append(
                lax.dot_general(
                    slot_query[s].astype(bf16),
                    keys[s],
                    (((1,), (1,)), ((), ())),
                    preferred_element_type=f32,
                )
                * inv_root
            )
        for s in picks:
            owns.append(
                jnp.sum(slot_query[s] * slot_small[0, pl.ds(s, 1), :], axis=1, keepdims=True)
                * inv_root
            )
        for i, s in enumerate(picks):
            visible = key_line < slot_length[pl.ds(s, 1), :]
            shown = jnp.where(visible, scores[i], masked_score)
            tops.append(jnp.maximum(jnp.max(shown, axis=1, keepdims=True), owns[i]))
        for i, s in enumerate(picks):
            visible = key_line < slot_length[pl.ds(s, 1), :]
            shown = jnp.where(visible, scores[i], masked_score)
            weights.append(jnp.where(visible, jnp.exp(shown - tops[i]), 0.0))
            own_weights.append(jnp.exp(owns[i] - tops[i]))
        blends = [dot(weights[i].astype(bf16), values[s]) for i, s in enumerate(picks)]
        for i in range(TOGETHER):
            sums.append(jnp.sum(weights[i], axis=1, keepdims=True) + own_weights[i])
        for i, s in enumerate(picks):
            one = pl.ds(s, 1)
            blended = blends[i] + own_weights[i].astype(bf16).astype(f32) * slot_small[1, one, :]
            slot_context[s] = blended / sums[i]
        return carry

    with jax.named_scope("g_attend"):
        lax.fori_loop(0, slots // TOGETHER, attend, 0)

    with jax.named_scope("h_choose"):
        for h in range(heads):
            home_f32[:, h * HEAD_SIZE : (h + 1) * HEAD_SIZE] = dot(
                chooser, slot_context[:, h, :].astype(bf16)
            )
        for d in range(dp):
            home_send[d] = home_f32[d : d + 1, :].astype(bf16)

    with jax.named_scope("i_homesend"):
        for k in range(1, dp):
            row_copy(*homeward, k).start()
        home_recv[me] = home_send[me]
    with jax.named_scope("j_relay"):
        weight_copy(2, y, 1, up).start()
        weight_copy(3, y, 0, down).start()
        weight_copy(0, y_down, 0, up).wait_recv()
        weight_copy(4, y_down, 0, up).start()
        weight_copy(1, y_up, 1, down).wait_recv()
        weight_copy(5, y_up, 1, down).start()
    with jax.named_scope("k_homewait"):
        for k in range(1, dp):
            row_arrival(*homeward, k).wait_recv()

    with jax.named_scope("l_compact"):
        for s in range(dp):
            home_f32[s : s + 1, :] = home_recv[s].astype(f32)
        for h in range(heads):
            lanes = slice(h * HEAD_SIZE, (h + 1) * HEAD_SIZE)
            mine = dot(unpacker, home_f32[:, lanes].astype(bf16))
            contexts[z, :, lanes] = (mine * value_factor).astype(bf16)

    def context_copy(k, block):
        return pltpu.make_async_remote_copy(
            src_ref=contexts.at[block],
            dst_ref=contexts.at[block],
            send_sem=context_send.at[k],
            recv_sem=context_recv.at[k],
            device_id=(lax.rem(z + k, outer) * inner + y, part),
            device_id_type=MESH,
        )

    with jax.named_scope("m_ctxsend"):
        for k in (4, 3, 5, 2, 6, 1, 7):
            context_copy(k, z).start()
    with jax.named_scope("n_weightwait"):
        weight_copy(2, y_down, 1, up).wait_recv()
        weight_copy(3, y_up, 0, down).wait_recv()
        weight_copy(4, y_far, 0, up).wait_recv()
        weight_copy(5, y_far, 1, down).wait_recv()
    with jax.named_scope("o_ctxwait"):
        for k in range(1, outer):
            context_copy(k, lax.rem(z + outer - k, outer)).wait_recv()

    def part_copy(n, k):
        target = lax.rem(z + k, outer)
        return pltpu.make_async_remote_copy(
            src_ref=send_part.at[n, target],
            dst_ref=recv_part.at[n, part],
            send_sem=part_send.at[n, k],
            recv_sem=part_recv.at[n, part],
            device_id=(target * inner + y, z),
            device_id_type=MESH,
        )

    def part_arrival(n, j):
        return pltpu.make_async_remote_copy(
            src_ref=send_part.at[n, 0],
            dst_ref=recv_part.at[n, j],
            send_sem=part_send.at[n, 0],
            recv_sem=part_recv.at[n, j],
            device_id=(me, part),
            device_id_type=MESH,
        )

    with jax.named_scope("p_project"):
        gathered = contexts[...].reshape(outer * rows, query_width)
        half = query_width // 2
        for n in range(inner):
            summed = dot(gathered[:, :half], weights_in[n, 0]) + dot(
                gathered[:, half:], weights_in[n, 1]
            )
            send_part[n] = summed.astype(bf16).reshape(outer, rows, columns)
            for k in (4, 3, 5, 2, 6, 1, 7):
                part_copy(n, k).start()

            @pl.when(z != part)
            def _():
                part_copy(n, 0).start()

            @pl.when(z == part)
            def _():
                recv_part[n, part] = send_part[n, z]

    with jax.named_scope("q_partwait"):
        for n in range(inner):
            for j in range(mp):

                @pl.when(jnp.logical_not((z == part) & (part == j)))
                def _():
                    part_arrival(n, j).wait_recv()

            summed = recv_part[n, 0].astype(f32)
            for j in range(1, mp):
                summed = summed + recv_part[n, j].astype(f32)
            out_ref[:, n * columns : (n + 1) * columns] = summed.astype(bf16)

    with jax.named_scope("r_drain"):
        for k in range(1, dp):
            row_copy(*request, k).wait_send()
            row_copy(*homeward, k).wait_send()
        weight_copy(0, y, 0, up).wait_send()
        weight_copy(1, y, 1, down).wait_send()
        weight_copy(2, y, 1, up).wait_send()
        weight_copy(3, y, 0, down).wait_send()
        weight_copy(4, y_down, 0, up).wait_send()
        weight_copy(5, y_up, 1, down).wait_send()
        for k in range(1, outer):
            context_copy(k, z).wait_send()
        for n in range(inner):
            for k in range(1, outer):
                part_copy(n, k).wait_send()

        @pl.when(z != part)
        def _():
            for n in range(inner):
                part_copy(n, 0).wait_send()


def on_device(
    dp,
    mp,
    queries,
    incoming_key,
    incoming_value,
    key_cache,
    cached_values,
    task_key_scale,
    task_value_scale,
    out_weight,
    task_id,
    cached_length,
    task_owner,
    cache_slot,
):
    rows, query_width = queries.shape
    kv_width = incoming_key.shape[1]
    slots = key_cache.shape[0]
    depth, columns = out_weight.shape
    row_width = query_width + 2 * kv_width + META
    heads = query_width // HEAD_SIZE
    inner = dp // mp
    vmem = pl.BlockSpec(memory_space=pltpu.VMEM)
    away = pl.BlockSpec(memory_space=pl.ANY)
    return pl.pallas_call(
        functools.partial(layer_kernel, dp, mp),
        out_shape=jax.ShapeDtypeStruct((rows, inner * columns), bf16),
        in_specs=[vmem] * 9 + [away] * 3,
        out_specs=vmem,
        scratch_shapes=[
            pltpu.VMEM(key_cache.shape, bf16),
            pltpu.VMEM(cached_values.shape, bf16),
            pltpu.VMEM((inner, 2, depth // 2, columns), bf16),
            pltpu.VMEM((dp, row_width), f32),
            pltpu.VMEM((dp, 1, row_width), bf16),
            pltpu.VMEM((dp, 1, row_width), bf16),
            pltpu.VMEM((slots, heads, kv_width), f32),
            pltpu.VMEM((2, slots, kv_width), f32),
            pltpu.VMEM((slots, key_cache.shape[1]), f32),
            pltpu.VMEM((slots, heads, HEAD_SIZE), f32),
            pltpu.VMEM((dp, query_width), f32),
            pltpu.VMEM((dp, 1, query_width), bf16),
            pltpu.VMEM((dp, 1, query_width), bf16),
            pltpu.VMEM((mp, rows, query_width), bf16),
            pltpu.VMEM((inner, mp, rows, columns), bf16),
            pltpu.VMEM((inner, mp, rows, columns), bf16),
            pltpu.SemaphoreType.DMA((3,)),
            pltpu.SemaphoreType.DMA((dp,)),
            pltpu.SemaphoreType.DMA((dp,)),
            pltpu.SemaphoreType.DMA((dp,)),
            pltpu.SemaphoreType.DMA((dp,)),
            pltpu.SemaphoreType.DMA((6,)),
            pltpu.SemaphoreType.DMA((6,)),
            pltpu.SemaphoreType.DMA((mp,)),
            pltpu.SemaphoreType.DMA((mp,)),
            pltpu.SemaphoreType.DMA((inner, mp)),
            pltpu.SemaphoreType.DMA((inner, mp)),
        ],
        compiler_params=pltpu.CompilerParams(
            collective_id=0, has_side_effects=True, vmem_limit_bytes=60 * 1024 * 1024
        ),
    )(
        queries,
        incoming_key,
        incoming_value,
        task_key_scale,
        task_value_scale,
        task_id.reshape(1, -1),
        cached_length.reshape(1, -1),
        cache_slot.reshape(1, -1),
        task_owner.reshape(1, -1),
        key_cache,
        cached_values,
        out_weight.reshape(2, depth // 2, columns),
    )


def solution(mesh):
    placed = (
        P("dp", "mp"),
        P("dp", "mp"),
        P("dp", "mp"),
        P("dp", None, "mp"),
        P("dp", None, "mp"),
        P(None, "mp"),
        P(None, "mp"),
        P("mp", "dp"),
        P("dp"),
        P("dp"),
        P(),
        P("dp"),
    )
    return jax.shard_map(
        functools.partial(on_device, mesh.shape["dp"], mesh.shape["mp"]),
        mesh=mesh,
        in_specs=placed,
        out_specs=P("dp", "mp"),
        check_vma=False,
    )
```

```python
import functools
import math

import jax
import jax.numpy as jnp
from jax import lax
from jax.experimental import pallas as pl
from jax.experimental.pallas import tpu as pltpu
from jax.sharding import PartitionSpec as P

HEAD_SIZE = 128
PAGE = 16
TOGETHER = 8
MESH = pl.DeviceIdType.MESH

masked_score = -1e30
f32 = jnp.float32
bf16 = jnp.bfloat16


def iota(shape, dim):
    return lax.broadcasted_iota(jnp.int32, shape, dim)


def ring(k, n):
    return min(k, n - k)


def to_column(row):
    n = row.shape[1]
    eye = iota((n, n), 0) == iota((n, n), 1)
    return jnp.sum(jnp.where(eye, row, 0.0), axis=1, keepdims=True)


def to_row(column):
    n = column.shape[0]
    eye = iota((n, n), 0) == iota((n, n), 1)
    return jnp.sum(jnp.where(eye, column, 0.0), axis=0, keepdims=True)


def dot(a, b):
    return jnp.dot(a, b, preferred_element_type=f32)


def one_hot(mask):
    return jnp.where(mask, 1.0, 0.0).astype(bf16)


def layer_kernel(
    dp,
    mp,
    query_hbm,
    new_key_hbm,
    new_value_hbm,
    key_scale_hbm,
    value_scale_hbm,
    task_hbm,
    length_hbm,
    slot_hbm,
    owner_hbm,
    key_hbm,
    value_hbm,
    weight_hbm,
    out_ref,
    query_ref,
    new_key_ref,
    new_value_ref,
    key_scale_ref,
    value_scale_ref,
    task_ref,
    length_ref,
    slot_ref,
    owner_ref,
    keys,
    values,
    weights_in,
    weights_over,
    send_rows,
    recv_rows,
    home_send,
    home_recv,
    selector,
    factor,
    contexts,
    block,
    send_part,
    recv_part,
    local_sem,
    small_sem,
    request_send,
    request_recv,
    home_send_sem,
    home_recv_sem,
    weight_send,
    weight_recv,
    over_send,
    over_recv,
    context_send,
    context_recv,
    part_send,
    part_recv,
):
    me = lax.axis_index("dp")
    part = lax.axis_index("mp")
    rows, query_width = query_ref.shape
    heads = query_width // HEAD_SIZE
    task_total = key_scale_ref.shape[0]
    slots, positions, _ = keys.shape
    columns = weights_in.shape[3]
    inner = dp // mp
    outer = mp
    z, y = me // inner, lax.rem(me, inner)
    chip, core = part // 2, lax.rem(part, 2)
    other = 2 * chip + 1 - core

    def at(kz, ky):
        return lax.rem(z + kz, outer) * inner + lax.rem(y + ky, inner)

    def distance(offset):
        return ring(offset[0], outer) + ring(offset[1], inner)

    def back(offset):
        return (outer - offset[0]) % outer, (inner - offset[1]) % inner

    near = sorted(((kz, ky) for kz in range(outer) for ky in range(inner)), key=distance)
    far = near[:0:-1]

    with jax.named_scope("a_greet"):
        small = [
            pltpu.make_async_copy(away, here, small_sem.at[i])
            for i, (away, here) in enumerate(
                (
                    (task_hbm, task_ref),
                    (owner_hbm, owner_ref),
                    (slot_hbm, slot_ref),
                    (length_hbm, length_ref),
                    (query_hbm, query_ref),
                    (key_scale_hbm, key_scale_ref),
                    (value_scale_hbm, value_scale_ref),
                    (new_key_hbm, new_key_ref),
                    (new_value_hbm, new_value_ref),
                )
            )
        ]
        for copy in small:
            copy.start()
        barrier = pltpu.get_barrier_semaphore()
        for kz, ky in far:
            pl.semaphore_signal(
                barrier, inc=1, device_id=(at(kz, ky), part), device_id_type=MESH
            )
        for k in range(1, mp):
            pl.semaphore_signal(
                barrier, inc=1, device_id=(me, lax.rem(part + k, mp)), device_id_type=MESH
            )
        fetches = [
            pltpu.make_async_copy(weight_hbm, weights_in.at[y], local_sem.at[2]),
            pltpu.make_async_copy(key_hbm, keys, local_sem.at[0]),
            pltpu.make_async_copy(value_hbm, values, local_sem.at[1]),
        ]
        for fetch in fetches:
            fetch.start()
        for copy in small:
            copy.wait()

    with jax.named_scope("b_pack"):
        task_column = to_column(task_ref[...].astype(f32))
        length_column = to_column(length_ref[...].astype(f32))
        slot_column = to_column(slot_ref[...].astype(f32))
        picked = task_column == iota((rows, task_total), 1).astype(f32)
        owner_column = jnp.sum(
            jnp.where(picked, owner_ref[...].astype(f32), 0.0), axis=1, keepdims=True
        )
        owner_row = to_row(owner_column)
        task_rows = one_hot(picked)
        key_factor = dot(task_rows, key_scale_ref[...])
        factor[...] = dot(task_rows, value_scale_ref[...])
        pieces = []
        for h in range(heads):
            lanes = slice(h * HEAD_SIZE, (h + 1) * HEAD_SIZE)
            pieces.append((query_ref[:, lanes].astype(f32) * key_factor).astype(bf16))
        pieces.append(new_key_ref[...])
        pieces.append(new_value_ref[...])
        pieces.append(jnp.broadcast_to(slot_column, (rows, HEAD_SIZE)).astype(bf16))
        pieces.append(jnp.broadcast_to(length_column, (rows, HEAD_SIZE)).astype(bf16))
        wide = len(pieces) * rows
        spread = one_hot(lax.rem(iota((rows, wide), 1), rows) == iota((rows, wide), 0))
        owner_wide = dot(owner_row.astype(bf16), spread)
        line = iota((dp * PAGE, wide), 0)
        lane = iota((dp * PAGE, wide), 1)
        packer = one_hot(
            (lax.rem(line, PAGE) == lane // rows) & ((line // PAGE).astype(f32) == owner_wide)
        )
        packed = dot(packer, jnp.concatenate(pieces, axis=0))
        send_rows[...] = packed.astype(bf16).reshape(dp, PAGE, HEAD_SIZE)
        line = iota((heads * rows, dp * heads), 0)
        lane = iota((heads * rows, dp * heads), 1)
        same = lax.rem(iota((heads * rows, rows), 0), rows) == iota((heads * rows, rows), 1)
        owner_tall = jnp.sum(jnp.where(same, owner_row, 0.0), axis=1, keepdims=True)
        selector[...] = one_hot(
            (line // rows == lax.rem(lane, heads)) & ((lane // heads).astype(f32) == owner_tall)
        )

    with jax.named_scope("c_barwait"):
        pl.semaphore_wait(barrier, dp + mp - 2)

    def row_copy(source, target, sends, recvs, offset, slot):
        k = offset[0] * inner + offset[1]
        return pltpu.make_async_remote_copy(
            src_ref=source.at[at(*offset)],
            dst_ref=target.at[slot],
            send_sem=sends.at[k],
            recv_sem=recvs.at[k],
            device_id=(at(*offset), part),
            device_id_type=MESH,
        )

    request = (send_rows, recv_rows, request_send, request_recv)
    homeward = (home_send, home_recv, home_send_sem, home_recv_sem)

    up, down = at(0, 1), at(0, inner - 1)
    y_up, y_down, y_far = (lax.rem(y + k, inner) for k in (1, inner - 1, 2))

    def weight_copy(k, source, half, target):
        return pltpu.make_async_remote_copy(
            src_ref=weights_in.at[source, half],
            dst_ref=weights_in.at[source, half],
            send_sem=weight_send.at[k],
            recv_sem=weight_recv.at[k],
            device_id=(target, part),
            device_id_type=MESH,
        )

    def over_copy(k, source, half):
        return pltpu.make_async_remote_copy(
            src_ref=weights_in.at[source, half],
            dst_ref=weights_over.at[source, half],
            send_sem=over_send.at[k, half],
            recv_sem=over_recv.at[k, half],
            device_id=(me, other),
            device_id_type=MESH,
        )

    with jax.named_scope("d_reqsend"):
        for offset in far:
            row_copy(*request, offset, me).start()
        recv_rows[me] = send_rows[me]
        fetches[0].wait()
        weight_copy(0, y, 0, up).start()
        weight_copy(1, y, 1, down).start()
        over_copy(0, y, 0).start()
        over_copy(0, y, 1).start()
        fetches[1].wait()
        fetches[2].wait()

    inv_root = 1.0 / math.sqrt(HEAD_SIZE)
    key_line = lax.rem(iota((heads, positions), 1), HEAD_SIZE).astype(f32)

    def attend(sources):
        queries, extras, picks, limits = [], [], [], []
        for s in sources:
            page = recv_rows[s]
            queries.append(page[:heads])
            extra = page[heads:].astype(f32)
            extras.append(extra)
            picks.append(jnp.clip(jnp.max(extra[2:3]).astype(jnp.int32), 0, slots - 1))
            length = jnp.broadcast_to(extra[3:4], (heads, HEAD_SIZE))
            limits.append(
                jnp.concatenate(
                    [length - i * HEAD_SIZE for i in range(positions // HEAD_SIZE)], axis=1
                )
            )
        scores = [
            lax.dot_general(
                q, keys[p], (((1,), (1,)), ((), ())), preferred_element_type=f32
            )
            * inv_root
            for q, p in zip(queries, picks)
        ]
        owns = [
            jnp.sum(q.astype(f32) * extra[0:1], axis=1, keepdims=True) * inv_root
            for q, extra in zip(queries, extras)
        ]
        shown = [
            jnp.where(key_line < limit, score, masked_score)
            for score, limit in zip(scores, limits)
        ]
        tops = [
            jnp.maximum(jnp.max(score, axis=1, keepdims=True), own)
            for score, own in zip(shown, owns)
        ]
        weights = [
            jnp.where(key_line < limit, jnp.exp(score - top), 0.0)
            for score, limit, top in zip(shown, limits, tops)
        ]
        own_weights = [jnp.exp(own - top) for own, top in zip(owns, tops)]
        blends = [dot(weight.astype(bf16), values[p]) for weight, p in zip(weights, picks)]
        sums = [
            jnp.sum(weight, axis=1, keepdims=True) + own
            for weight, own in zip(weights, own_weights)
        ]
        for s, blend, own, extra, total in zip(sources, blends, own_weights, extras, sums):
            blended = blend + own.astype(bf16).astype(f32) * extra[1:2]
            home_send[s] = (blended / total).astype(bf16)

    for g in range(0, dp, TOGETHER):
        group = near[g : g + TOGETHER]
        with jax.named_scope("e_reqwait"):
            for offset in group:
                if offset != (0, 0):
                    row_copy(*request, offset, at(*back(offset))).wait_recv()
        with jax.named_scope("f_attend"):
            attend([at(*back(offset)) for offset in group])
        with jax.named_scope("g_homesend"):
            for offset in reversed(group):
                if offset != (0, 0):
                    row_copy(*homeward, back(offset), me).start()
            if g == 0:
                home_recv[me] = home_send[me]

    with jax.named_scope("j_relay"):
        weight_copy(2, y, 1, up).start()
        weight_copy(3, y, 0, down).start()
        weight_copy(0, y_down, 0, up).wait_recv()
        weight_copy(4, y_down, 0, up).start()
        over_copy(1, y_down, 0).start()
        weight_copy(1, y_up, 1, down).wait_recv()
        weight_copy(5, y_up, 1, down).start()
        over_copy(2, y_up, 1).start()
    with jax.named_scope("k_homewait"):
        for offset in near[1:]:
            row_copy(*homeward, offset, at(*back(offset))).wait_recv()

    mine = lax.rem(z, 2)

    with jax.named_scope("l_compact"):
        chosen = dot(selector[...], home_recv[...].reshape(dp * heads, HEAD_SIZE))
        for h in range(heads):
            block[:, h * HEAD_SIZE : (h + 1) * HEAD_SIZE] = (
                chosen[h * rows : (h + 1) * rows] * factor[...]
            ).astype(bf16)

    def context_copy(k, home):
        return pltpu.make_async_remote_copy(
            src_ref=block,
            dst_ref=contexts.at[core, home],
            send_sem=context_send.at[k],
            recv_sem=context_recv.at[core, home],
            device_id=(at(k, 0), 2 * chip + mine),
            device_id_type=MESH,
        )

    def context_arrival(source, home):
        return pltpu.make_async_remote_copy(
            src_ref=block,
            dst_ref=contexts.at[source, home],
            send_sem=context_send.at[0],
            recv_sem=context_recv.at[source, home],
            device_id=(me, other),
            device_id_type=MESH,
        )

    with jax.named_scope("m_ctxsend"):
        for k in (4, 3, 5, 2, 6, 1, 7):
            context_copy(k, z // 2).start()

        @pl.when(mine != core)
        def _():
            context_copy(0, z // 2).start()

        @pl.when(mine == core)
        def _():
            contexts[core, z // 2] = block[...]

    with jax.named_scope("n_overs"):
        weight_copy(2, y_down, 1, up).wait_recv()
        over_copy(1, y_down, 1).start()
        weight_copy(3, y_up, 0, down).wait_recv()
        over_copy(2, y_up, 0).start()
        weight_copy(4, y_far, 0, up).wait_recv()
        over_copy(3, y_far, 0).start()
        weight_copy(5, y_far, 1, down).wait_recv()
        over_copy(3, y_far, 1).start()
    with jax.named_scope("o_ctxwait"):
        for source in range(2):
            for home in range(outer // 2):

                @pl.when(jnp.logical_not((source == core) & (2 * home + core == z)))
                def _():
                    context_arrival(source, home).wait_recv()

    with jax.named_scope("o_overwait"):
        for half in range(2):
            over_copy(0, y, half).wait_recv()
            over_copy(1, y_down, half).wait_recv()
            over_copy(2, y_up, half).wait_recv()
            over_copy(3, y_far, half).wait_recv()

    shift = lax.rem(z + core, 2)

    def part_copy(n, i):
        target = lax.rem(z + 2 * i + shift, outer)
        return pltpu.make_async_remote_copy(
            src_ref=send_part.at[n, target // 2],
            dst_ref=recv_part.at[n, chip],
            send_sem=part_send.at[n, i],
            recv_sem=part_recv.at[n, chip],
            device_id=(target * inner + y, z),
            device_id_type=MESH,
        )

    def part_arrival(n, j):
        return pltpu.make_async_remote_copy(
            src_ref=send_part.at[n, 0],
            dst_ref=recv_part.at[n, j],
            send_sem=part_send.at[n, 0],
            recv_sem=part_recv.at[n, j],
            device_id=(me, other),
            device_id_type=MESH,
        )

    with jax.named_scope("p_project"):
        half = query_width // 2
        direct = contexts[core].reshape(outer * rows // 2, query_width)
        over = contexts[1 - core].reshape(outer * rows // 2, query_width)
        for n in range(inner):
            summed = (
                dot(direct[:, :half], weights_in[n, 0])
                + dot(direct[:, half:], weights_in[n, 1])
                + dot(over[:, :half], weights_over[n, 0])
                + dot(over[:, half:], weights_over[n, 1])
            )
            send_part[n] = summed.astype(bf16).reshape(outer // 2, rows, columns)
            for i in (2, 1, 3):
                part_copy(n, i).start()

            @pl.when(z != part)
            def _():
                part_copy(n, 0).start()

            @pl.when(z == part)
            def _():
                recv_part[n, chip] = send_part[n, z // 2]

    with jax.named_scope("q_drain"):
        for offset in far:
            row_copy(*request, offset, me).wait_send()
            row_copy(*homeward, offset, me).wait_send()
        weight_copy(0, y, 0, up).wait_send()
        weight_copy(1, y, 1, down).wait_send()
        weight_copy(2, y, 1, up).wait_send()
        weight_copy(3, y, 0, down).wait_send()
        weight_copy(4, y_down, 0, up).wait_send()
        weight_copy(5, y_up, 1, down).wait_send()
        for half in range(2):
            for k in range(inner):
                over_copy(k, y, half).wait_send()
        for k in range(1, outer):
            context_copy(k, z // 2).wait_send()

        @pl.when(mine != core)
        def _():
            context_copy(0, z // 2).wait_send()

    with jax.named_scope("r_partwait"):
        for n in range(inner):
            for j in range(mp // 2):

                @pl.when(jnp.logical_not((z == part) & (chip == j)))
                def _():
                    part_arrival(n, j).wait_recv()

            summed = recv_part[n, 0].astype(f32)
            for j in range(1, mp // 2):
                summed = summed + recv_part[n, j].astype(f32)
            out_ref[:, n * columns : (n + 1) * columns] = summed.astype(bf16)

    with jax.named_scope("s_drain"):
        for n in range(inner):
            for i in range(1, mp // 2):
                part_copy(n, i).wait_send()

        @pl.when(z != part)
        def _():
            for n in range(inner):
                part_copy(n, 0).wait_send()


def on_device(
    dp,
    mp,
    queries,
    incoming_key,
    incoming_value,
    key_cache,
    cached_values,
    task_key_scale,
    task_value_scale,
    out_weight,
    task_id,
    cached_length,
    task_owner,
    cache_slot,
):
    rows, query_width = queries.shape
    depth, columns = out_weight.shape
    heads = query_width // HEAD_SIZE
    inner = dp // mp
    small = (
        queries,
        incoming_key,
        incoming_value,
        task_key_scale,
        task_value_scale,
        task_id.reshape(1, -1),
        cached_length.reshape(1, -1),
        cache_slot.reshape(1, -1),
        task_owner.reshape(1, -1),
    )
    away = pl.BlockSpec(memory_space=pl.ANY)
    return pl.pallas_call(
        functools.partial(layer_kernel, dp, mp),
        out_shape=jax.ShapeDtypeStruct((rows, inner * columns), bf16),
        in_specs=[away] * 12,
        out_specs=pl.BlockSpec(memory_space=pltpu.VMEM),
        scratch_shapes=[pltpu.VMEM(array.shape, array.dtype) for array in small]
        + [
            pltpu.VMEM(key_cache.shape, bf16),
            pltpu.VMEM(cached_values.shape, bf16),
            pltpu.VMEM((inner, 2, depth // 2, columns), bf16),
            pltpu.VMEM((inner, 2, depth // 2, columns), bf16),
            pltpu.VMEM((dp, PAGE, HEAD_SIZE), bf16),
            pltpu.VMEM((dp, PAGE, HEAD_SIZE), bf16),
            pltpu.VMEM((dp, heads, HEAD_SIZE), bf16),
            pltpu.VMEM((dp, heads, HEAD_SIZE), bf16),
            pltpu.VMEM((heads * rows, dp * heads), bf16),
            pltpu.VMEM((rows, HEAD_SIZE), f32),
            pltpu.VMEM((2, mp // 2, rows, query_width), bf16),
            pltpu.VMEM((rows, query_width), bf16),
            pltpu.VMEM((inner, mp // 2, rows, columns), bf16),
            pltpu.VMEM((inner, mp // 2, rows, columns), bf16),
            pltpu.SemaphoreType.DMA((3,)),
            pltpu.SemaphoreType.DMA((len(small),)),
            pltpu.SemaphoreType.DMA((dp,)),
            pltpu.SemaphoreType.DMA((dp,)),
            pltpu.SemaphoreType.DMA((dp,)),
            pltpu.SemaphoreType.DMA((dp,)),
            pltpu.SemaphoreType.DMA((6,)),
            pltpu.SemaphoreType.DMA((6,)),
            pltpu.SemaphoreType.DMA((inner, 2)),
            pltpu.SemaphoreType.DMA((inner, 2)),
            pltpu.SemaphoreType.DMA((mp,)),
            pltpu.SemaphoreType.DMA((2, mp // 2)),
            pltpu.SemaphoreType.DMA((inner, mp // 2)),
            pltpu.SemaphoreType.DMA((inner, mp // 2)),
        ],
        compiler_params=pltpu.CompilerParams(
            collective_id=0, has_side_effects=True, vmem_limit_bytes=60 * 1024 * 1024
        ),
    )(*small, key_cache, cached_values, out_weight.reshape(2, depth // 2, columns))


def solution(mesh):
    placed = (
        P("dp", "mp"),
        P("dp", "mp"),
        P("dp", "mp"),
        P("dp", None, "mp"),
        P("dp", None, "mp"),
        P(None, "mp"),
        P(None, "mp"),
        P("mp", "dp"),
        P("dp"),
        P("dp"),
        P(),
        P("dp"),
    )
    return jax.shard_map(
        functools.partial(on_device, mesh.shape["dp"], mesh.shape["mp"]),
        mesh=mesh,
        in_specs=placed,
        out_specs=P("dp", "mp"),
        check_vma=False,
    )
```

```python
import functools
import math

import jax
import jax.numpy as jnp
from jax import lax
from jax.experimental import pallas as pl
from jax.experimental.pallas import tpu as pltpu
from jax.sharding import PartitionSpec as P

HEAD_SIZE = 128
PAGE = 16
TOGETHER = 8
MESH = pl.DeviceIdType.MESH

masked_score = -1e30
f32 = jnp.float32
bf16 = jnp.bfloat16


def iota(shape, dim):
    return lax.broadcasted_iota(jnp.int32, shape, dim)


def ring(k, n):
    return min(k, n - k)


def to_column(row):
    n = row.shape[1]
    eye = iota((n, n), 0) == iota((n, n), 1)
    return jnp.sum(jnp.where(eye, row, 0.0), axis=1, keepdims=True)


def to_row(column):
    n = column.shape[0]
    eye = iota((n, n), 0) == iota((n, n), 1)
    return jnp.sum(jnp.where(eye, column, 0.0), axis=0, keepdims=True)


def dot(a, b):
    return jnp.dot(a, b, preferred_element_type=f32)


def one_hot(mask):
    return jnp.where(mask, 1.0, 0.0).astype(bf16)


def layer_kernel(
    dp,
    mp,
    query_hbm,
    new_key_hbm,
    new_value_hbm,
    key_scale_hbm,
    value_scale_hbm,
    task_hbm,
    length_hbm,
    slot_hbm,
    owner_hbm,
    key_hbm,
    value_hbm,
    weight_hbm,
    out_ref,
    query_ref,
    new_key_ref,
    new_value_ref,
    key_scale_ref,
    value_scale_ref,
    task_ref,
    length_ref,
    slot_ref,
    owner_ref,
    keys,
    values,
    weights_in,
    weights_over,
    send_rows,
    recv_rows,
    home_send,
    home_recv,
    selector,
    factor,
    contexts,
    block,
    send_part,
    recv_part,
    local_sem,
    small_sem,
    send_sem,
    request_recv,
    home_recv_sem,
    weight_recv,
    over_recv,
    context_recv,
    part_recv,
):
    me = lax.axis_index("dp")
    part = lax.axis_index("mp")
    rows, query_width = query_ref.shape
    heads = query_width // HEAD_SIZE
    task_total = key_scale_ref.shape[0]
    slots, positions, _ = keys.shape
    columns = weights_in.shape[3]
    inner = dp // mp
    outer = mp
    z, y = me // inner, lax.rem(me, inner)
    chip, core = part // 2, lax.rem(part, 2)
    other = 2 * chip + 1 - core

    def at(kz, ky):
        return lax.rem(z + kz, outer) * inner + lax.rem(y + ky, inner)

    def distance(offset):
        return ring(offset[0], outer) + ring(offset[1], inner)

    def back(offset):
        return (outer - offset[0]) % outer, (inner - offset[1]) % inner

    near = sorted(((kz, ky) for kz in range(outer) for ky in range(inner)), key=distance)
    far = near[:0:-1]
    group_of = {offset: n // TOGETHER for n, offset in enumerate(near)}

    with jax.named_scope("a_greet"):
        small = [
            pltpu.make_async_copy(away, here, small_sem.at[i])
            for i, (away, here) in enumerate(
                (
                    (task_hbm, task_ref),
                    (owner_hbm, owner_ref),
                    (slot_hbm, slot_ref),
                    (length_hbm, length_ref),
                    (query_hbm, query_ref),
                    (key_scale_hbm, key_scale_ref),
                    (value_scale_hbm, value_scale_ref),
                    (new_key_hbm, new_key_ref),
                    (new_value_hbm, new_value_ref),
                )
            )
        ]
        for copy in small:
            copy.start()
        barrier = pltpu.get_barrier_semaphore()
        for kz, ky in far:
            pl.semaphore_signal(
                barrier, inc=1, device_id=(at(kz, ky), part), device_id_type=MESH
            )
        for k in range(1, mp):
            pl.semaphore_signal(
                barrier, inc=1, device_id=(me, lax.rem(part + k, mp)), device_id_type=MESH
            )
        fetches = [
            pltpu.make_async_copy(weight_hbm, weights_in.at[y], local_sem.at[2]),
            pltpu.make_async_copy(key_hbm, keys, local_sem.at[0]),
            pltpu.make_async_copy(value_hbm, values, local_sem.at[1]),
        ]
        for fetch in fetches:
            fetch.start()
        for copy in small:
            copy.wait()

    with jax.named_scope("b_pack"):
        task_column = to_column(task_ref[...].astype(f32))
        length_column = to_column(length_ref[...].astype(f32))
        slot_column = to_column(slot_ref[...].astype(f32))
        picked = task_column == iota((rows, task_total), 1).astype(f32)
        owner_column = jnp.sum(
            jnp.where(picked, owner_ref[...].astype(f32), 0.0), axis=1, keepdims=True
        )
        owner_row = to_row(owner_column)
        task_rows = one_hot(picked)
        key_factor = dot(task_rows, key_scale_ref[...])
        factor[...] = dot(task_rows, value_scale_ref[...])
        pieces = []
        for h in range(heads):
            lanes = slice(h * HEAD_SIZE, (h + 1) * HEAD_SIZE)
            pieces.append((query_ref[:, lanes].astype(f32) * key_factor).astype(bf16))
        pieces.append(new_key_ref[...])
        pieces.append(new_value_ref[...])
        pieces.append(jnp.broadcast_to(slot_column, (rows, HEAD_SIZE)).astype(bf16))
        pieces.append(jnp.broadcast_to(length_column, (rows, HEAD_SIZE)).astype(bf16))
        wide = len(pieces) * rows
        spread = one_hot(lax.rem(iota((rows, wide), 1), rows) == iota((rows, wide), 0))
        owner_wide = dot(owner_row.astype(bf16), spread)
        line = iota((dp * PAGE, wide), 0)
        lane = iota((dp * PAGE, wide), 1)
        packer = one_hot(
            (lax.rem(line, PAGE) == lane // rows) & ((line // PAGE).astype(f32) == owner_wide)
        )
        packed = dot(packer, jnp.concatenate(pieces, axis=0))
        send_rows[...] = packed.astype(bf16).reshape(dp, PAGE, HEAD_SIZE)
        line = iota((heads * rows, dp * heads), 0)
        lane = iota((heads * rows, dp * heads), 1)
        same = lax.rem(iota((heads * rows, rows), 0), rows) == iota((heads * rows, rows), 1)
        owner_tall = jnp.sum(jnp.where(same, owner_row, 0.0), axis=1, keepdims=True)
        selector[...] = one_hot(
            (line // rows == lax.rem(lane, heads)) & ((lane // heads).astype(f32) == owner_tall)
        )

    with jax.named_scope("c_barwait"):
        pl.semaphore_wait(barrier, dp + mp - 2)

    def remote(source, target, send_sem, recv_sem, device):
        return pltpu.make_async_remote_copy(
            src_ref=source,
            dst_ref=target,
            send_sem=send_sem,
            recv_sem=recv_sem,
            device_id=device,
            device_id_type=MESH,
        )

    def request_copy(offset):
        return remote(
            send_rows.at[at(*offset)],
            recv_rows.at[me],
            send_sem.at[0],
            request_recv.at[group_of[offset]],
            (at(*offset), part),
        )

    def requests_in(group, count):
        pages = pl.ds(0, count)
        return remote(
            send_rows.at[pages],
            recv_rows.at[pages],
            send_sem.at[0],
            request_recv.at[group],
            (me, other),
        )

    def home_copy(offset):
        return remote(
            home_send.at[at(*offset)],
            home_recv.at[me],
            send_sem.at[1],
            home_recv_sem.at[0],
            (at(*offset), part),
        )

    def homes_in():
        pages = pl.ds(0, dp - 1)
        return remote(
            home_send.at[pages],
            home_recv.at[pages],
            send_sem.at[1],
            home_recv_sem.at[0],
            (me, other),
        )

    up, down = at(0, 1), at(0, inner - 1)
    y_up, y_down, y_far = (lax.rem(y + k, inner) for k in (1, inner - 1, 2))

    def weight_copy(k, source, half, target):
        return remote(
            weights_in.at[source, half],
            weights_in.at[source, half],
            send_sem.at[2],
            weight_recv.at[k],
            (target, part),
        )

    def over_copy(k, source, half):
        return remote(
            weights_in.at[source, half],
            weights_over.at[source, half],
            send_sem.at[3],
            over_recv.at[k],
            (me, other),
        )

    def over_in(k, source):
        return remote(
            weights_in.at[source],
            weights_over.at[source],
            send_sem.at[3],
            over_recv.at[k],
            (me, other),
        )

    with jax.named_scope("d_reqsend"):
        for offset in far:
            request_copy(offset).start()
        recv_rows[me] = send_rows[me]
        fetches[0].wait()
        weight_copy(0, y, 0, up).start()
        weight_copy(1, y, 1, down).start()
        over_copy(0, y, 0).start()
        over_copy(0, y, 1).start()
        fetches[1].wait()
        fetches[2].wait()

    inv_root = 1.0 / math.sqrt(HEAD_SIZE)
    key_line = lax.rem(iota((heads, positions), 1), HEAD_SIZE).astype(f32)

    def attend(sources):
        queries, extras, picks, limits = [], [], [], []
        for s in sources:
            page = recv_rows[s]
            queries.append(page[:heads])
            extra = page[heads:].astype(f32)
            extras.append(extra)
            picks.append(jnp.clip(jnp.max(extra[2:3]).astype(jnp.int32), 0, slots - 1))
            length = jnp.broadcast_to(extra[3:4], (heads, HEAD_SIZE))
            limits.append(
                jnp.concatenate(
                    [length - i * HEAD_SIZE for i in range(positions // HEAD_SIZE)], axis=1
                )
            )
        scores = [
            lax.dot_general(
                q, keys[p], (((1,), (1,)), ((), ())), preferred_element_type=f32
            )
            * inv_root
            for q, p in zip(queries, picks)
        ]
        owns = [
            jnp.sum(q.astype(f32) * extra[0:1], axis=1, keepdims=True) * inv_root
            for q, extra in zip(queries, extras)
        ]
        shown = [
            jnp.where(key_line < limit, score, masked_score)
            for score, limit in zip(scores, limits)
        ]
        tops = [
            jnp.maximum(jnp.max(score, axis=1, keepdims=True), own)
            for score, own in zip(shown, owns)
        ]
        weights = [
            jnp.where(key_line < limit, jnp.exp(score - top), 0.0)
            for score, limit, top in zip(shown, limits, tops)
        ]
        own_weights = [jnp.exp(own - top) for own, top in zip(owns, tops)]
        blends = [dot(weight.astype(bf16), values[p]) for weight, p in zip(weights, picks)]
        sums = [
            jnp.sum(weight, axis=1, keepdims=True) + own
            for weight, own in zip(weights, own_weights)
        ]
        for s, blend, own, extra, total in zip(sources, blends, own_weights, extras, sums):
            blended = blend + own.astype(bf16).astype(f32) * extra[1:2]
            home_send[s] = (blended / total).astype(bf16)

    for g in range(0, dp, TOGETHER):
        group = near[g : g + TOGETHER]
        with jax.named_scope("e_reqwait"):
            requests_in(g // TOGETHER, TOGETHER if g > 0 else TOGETHER - 1).wait_recv()
        with jax.named_scope("f_attend"):
            attend([at(*back(offset)) for offset in group])
        with jax.named_scope("g_homesend"):
            for offset in reversed(group):
                if offset != (0, 0):
                    home_copy(back(offset)).start()
            if g == 0:
                home_recv[me] = home_send[me]

    with jax.named_scope("j_relay"):
        weight_copy(2, y, 1, up).start()
        weight_copy(3, y, 0, down).start()
        weight_copy(0, y_down, 0, up).wait_recv()
        weight_copy(4, y_down, 0, up).start()
        over_copy(1, y_down, 0).start()
        weight_copy(1, y_up, 1, down).wait_recv()
        weight_copy(5, y_up, 1, down).start()
        over_copy(2, y_up, 1).start()
    with jax.named_scope("k_homewait"):
        homes_in().wait_recv()

    mine = lax.rem(z, 2)

    with jax.named_scope("l_compact"):
        chosen = dot(selector[...], home_recv[...].reshape(dp * heads, HEAD_SIZE))
        for h in range(heads):
            block[:, h * HEAD_SIZE : (h + 1) * HEAD_SIZE] = (
                chosen[h * rows : (h + 1) * rows] * factor[...]
            ).astype(bf16)

    homes = outer // 2
    middle = query_width // 2

    def place(source, home):
        return source * homes + lax.rem(home, outer) // 2

    def context_copy(k):
        return remote(
            block,
            contexts.at[place(core, z)],
            send_sem.at[4],
            context_recv.at[{2: 1, 6: 2}.get(k, 0)],
            (at(k, 0), 2 * chip + mine),
        )

    def context_relay(source, k, half):
        spot = contexts.at[place(source, z + outer - k), :, pl.ds(half * middle, middle)]
        return remote(spot, spot, send_sem.at[4], context_recv.at[0], (at(k, 0), part))

    def contexts_in(k, count):
        blocks = contexts.at[pl.ds(0, count)]
        return remote(blocks, blocks, send_sem.at[4], context_recv.at[k], (me, other))

    with jax.named_scope("m_ctxsend"):
        for k in (2, 6, 3, 5, 1, 7):
            context_copy(k).start()

        @pl.when(mine != core)
        def _():
            context_copy(0).start()

        @pl.when(mine == core)
        def _():
            contexts[place(core, z)] = block[...]

    with jax.named_scope("n_overs"):
        weight_copy(2, y_down, 1, up).wait_recv()
        over_copy(1, y_down, 1).start()
        weight_copy(3, y_up, 0, down).wait_recv()
        over_copy(2, y_up, 0).start()

    with jax.named_scope("n_relay"):

        @pl.when(mine == core)
        def _():
            contexts_in(1, 2).wait_recv()
            for source in range(2):
                context_relay(source, 2, 0).start()
            contexts_in(2, 2).wait_recv()
            for source in range(2):
                context_relay(source, outer - 2, 1).start()

    with jax.named_scope("n_overs2"):
        weight_copy(4, y_far, 0, up).wait_recv()
        over_copy(3, y_far, 0).start()
        weight_copy(5, y_far, 1, down).wait_recv()
        over_copy(3, y_far, 1).start()

    with jax.named_scope("o_ctxwait"):

        @pl.when(mine == core)
        def _():
            contexts_in(0, 3).wait_recv()

        @pl.when(mine != core)
        def _():
            contexts_in(0, 2 * homes).wait_recv()

    shift = lax.rem(z + core, 2)

    def part_copy(n, column, i):
        target = lax.rem(z + 2 * i + shift, outer)
        return remote(
            send_part.at[column, target // 2],
            recv_part.at[column, chip],
            send_sem.at[5],
            part_recv.at[n],
            (target * inner + y, z),
        )

    def parts_in(n, count):
        parts = pl.ds(0, count)
        return remote(
            send_part.at[0, parts],
            recv_part.at[0, parts],
            send_sem.at[5],
            part_recv.at[n],
            (me, other),
        )

    order = (y, y_down, y_up, y_far)

    with jax.named_scope("p_project"):
        direct = contexts[pl.ds(core * homes, homes)].reshape(homes * rows, query_width)
        over = contexts[pl.ds((1 - core) * homes, homes)].reshape(homes * rows, query_width)
        for n, column in enumerate(order):
            over_in(n, column).wait_recv()
            summed = (
                dot(direct[:, :middle], weights_in[column, 0])
                + dot(direct[:, middle:], weights_in[column, 1])
                + dot(over[:, :middle], weights_over[column, 0])
                + dot(over[:, middle:], weights_over[column, 1])
            )
            send_part[column] = summed.astype(bf16).reshape(homes, rows, columns)
            for i in (2, 1, 3):
                part_copy(n, column, i).start()

            @pl.when(z != part)
            def _():
                part_copy(n, column, 0).start()

            @pl.when(z == part)
            def _():
                recv_part[column, chip] = send_part[column, z // 2]

    with jax.named_scope("q_drain"):
        requests_in(0, dp - 1).wait_send()
        homes_in().wait_send()
        three = weights_in.at[pl.ds(0, inner - 1)]
        remote(three, three, send_sem.at[2], weight_recv.at[0], (me, other)).wait_send()
        remote(weights_in, weights_over, send_sem.at[3], over_recv.at[0], (me, other)).wait_send()

        @pl.when(mine == core)
        def _():
            contexts_in(0, 2 * homes).wait_send()

        @pl.when(mine != core)
        def _():
            contexts_in(0, 2 * homes - 1).wait_send()

    with jax.named_scope("r_partwait"):
        for n, column in enumerate(order):

            @pl.when(z != part)
            def _():
                parts_in(n, mp // 2).wait_recv()

            @pl.when(z == part)
            def _():
                parts_in(n, mp // 2 - 1).wait_recv()

            summed = recv_part[column, 0].astype(f32)
            for j in range(1, mp // 2):
                summed = summed + recv_part[column, j].astype(f32)
            start = pl.multiple_of(column * columns, columns)
            out_ref[:, pl.ds(start, columns)] = summed.astype(bf16)

    with jax.named_scope("s_drain"):

        @pl.when(z != part)
        def _():
            remote(send_part, send_part, send_sem.at[5], part_recv.at[0], (me, other)).wait_send()

        @pl.when(z == part)
        def _():
            most = send_part.at[:, pl.ds(0, mp // 2 - 1)]
            remote(most, most, send_sem.at[5], part_recv.at[0], (me, other)).wait_send()


def on_device(
    dp,
    mp,
    queries,
    incoming_key,
    incoming_value,
    key_cache,
    cached_values,
    task_key_scale,
    task_value_scale,
    out_weight,
    task_id,
    cached_length,
    task_owner,
    cache_slot,
):
    rows, query_width = queries.shape
    depth, columns = out_weight.shape
    heads = query_width // HEAD_SIZE
    inner = dp // mp
    small = (
        queries,
        incoming_key,
        incoming_value,
        task_key_scale,
        task_value_scale,
        task_id.reshape(1, -1),
        cached_length.reshape(1, -1),
        cache_slot.reshape(1, -1),
        task_owner.reshape(1, -1),
    )
    away = pl.BlockSpec(memory_space=pl.ANY)
    return pl.pallas_call(
        functools.partial(layer_kernel, dp, mp),
        out_shape=jax.ShapeDtypeStruct((rows, inner * columns), bf16),
        in_specs=[away] * 12,
        out_specs=pl.BlockSpec(memory_space=pltpu.VMEM),
        scratch_shapes=[pltpu.VMEM(array.shape, array.dtype) for array in small]
        + [
            pltpu.VMEM(key_cache.shape, bf16),
            pltpu.VMEM(cached_values.shape, bf16),
            pltpu.VMEM((inner, 2, depth // 2, columns), bf16),
            pltpu.VMEM((inner, 2, depth // 2, columns), bf16),
            pltpu.VMEM((dp, PAGE, HEAD_SIZE), bf16),
            pltpu.VMEM((dp, PAGE, HEAD_SIZE), bf16),
            pltpu.VMEM((dp, heads, HEAD_SIZE), bf16),
            pltpu.VMEM((dp, heads, HEAD_SIZE), bf16),
            pltpu.VMEM((heads * rows, dp * heads), bf16),
            pltpu.VMEM((rows, HEAD_SIZE), f32),
            pltpu.VMEM((mp, rows, query_width), bf16),
            pltpu.VMEM((rows, query_width), bf16),
            pltpu.VMEM((inner, mp // 2, rows, columns), bf16),
            pltpu.VMEM((inner, mp // 2, rows, columns), bf16),
            pltpu.SemaphoreType.DMA((3,)),
            pltpu.SemaphoreType.DMA((len(small),)),
            pltpu.SemaphoreType.DMA((6,)),
            pltpu.SemaphoreType.DMA((dp // TOGETHER,)),
            pltpu.SemaphoreType.DMA((1,)),
            pltpu.SemaphoreType.DMA((6,)),
            pltpu.SemaphoreType.DMA((inner,)),
            pltpu.SemaphoreType.DMA((3,)),
            pltpu.SemaphoreType.DMA((inner,)),
        ],
        compiler_params=pltpu.CompilerParams(
            collective_id=0, has_side_effects=True, vmem_limit_bytes=60 * 1024 * 1024
        ),
    )(*small, key_cache, cached_values, out_weight.reshape(2, depth // 2, columns))


def solution(mesh):
    placed = (
        P("dp", "mp"),
        P("dp", "mp"),
        P("dp", "mp"),
        P("dp", None, "mp"),
        P("dp", None, "mp"),
        P(None, "mp"),
        P(None, "mp"),
        P("mp", "dp"),
        P("dp"),
        P("dp"),
        P(),
        P("dp"),
    )
    return jax.shard_map(
        functools.partial(on_device, mesh.shape["dp"], mesh.shape["mp"]),
        mesh=mesh,
        in_specs=placed,
        out_specs=P("dp", "mp"),
        check_vma=False,
    )
```

```python
import functools
import math

import jax
import jax.numpy as jnp
from jax import lax
from jax.experimental import pallas as pl
from jax.experimental.pallas import tpu as pltpu
from jax.sharding import PartitionSpec as P

HEAD_SIZE = 128
PAGE = 16
TOGETHER = 32
QUARTERS = 4
MESH = pl.DeviceIdType.MESH

masked_score = -1e30
f32 = jnp.float32
bf16 = jnp.bfloat16


def iota(shape, dim):
    return lax.broadcasted_iota(jnp.int32, shape, dim)


def ring(k, n):
    return min(k, n - k)


def to_column(row):
    n = row.shape[1]
    eye = iota((n, n), 0) == iota((n, n), 1)
    return jnp.sum(jnp.where(eye, row, 0.0), axis=1, keepdims=True)


def to_row(column):
    n = column.shape[0]
    eye = iota((n, n), 0) == iota((n, n), 1)
    return jnp.sum(jnp.where(eye, column, 0.0), axis=0, keepdims=True)


def dot(a, b):
    return jnp.dot(a, b, preferred_element_type=f32)


def one_hot(mask):
    return jnp.where(mask, 1.0, 0.0).astype(bf16)


def layer_kernel(
    dp,
    mp,
    query_hbm,
    new_key_hbm,
    new_value_hbm,
    key_scale_hbm,
    value_scale_hbm,
    task_hbm,
    length_hbm,
    slot_hbm,
    owner_hbm,
    key_hbm,
    value_hbm,
    weight_hbm,
    out_ref,
    query_ref,
    new_key_ref,
    new_value_ref,
    key_scale_ref,
    value_scale_ref,
    task_ref,
    length_ref,
    slot_ref,
    owner_ref,
    keys,
    values,
    weights_in,
    weights_over,
    send_rows,
    recv_rows,
    home_send,
    home_recv,
    selector,
    factor,
    contexts,
    block,
    send_part,
    recv_part,
    local_sem,
    small_sem,
    send_sem,
    request_recv,
    home_recv_sem,
    weight_recv,
    over_recv,
    context_recv,
    part_recv,
):
    me = lax.axis_index("dp")
    part = lax.axis_index("mp")
    rows, query_width = query_ref.shape
    heads = query_width // HEAD_SIZE
    task_total = key_scale_ref.shape[0]
    slots, positions, _ = keys.shape
    columns = weights_in.shape[3]
    inner = dp // mp
    outer = mp
    z, y = me // inner, lax.rem(me, inner)
    chip, core = part // 2, lax.rem(part, 2)
    other = 2 * chip + 1 - core

    def at(kz, ky):
        return lax.rem(z + kz, outer) * inner + lax.rem(y + ky, inner)

    def distance(offset):
        return ring(offset[0], outer) + ring(offset[1], inner)

    def back(offset):
        return (outer - offset[0]) % outer, (inner - offset[1]) % inner

    near = sorted(((kz, ky) for kz in range(outer) for ky in range(inner)), key=distance)
    far = near[:0:-1]
    group_of = {offset: n // TOGETHER for n, offset in enumerate(near)}

    def remote(source, target, send_sem, recv_sem, device):
        return pltpu.make_async_remote_copy(
            src_ref=source,
            dst_ref=target,
            send_sem=send_sem,
            recv_sem=recv_sem,
            device_id=device,
            device_id_type=MESH,
        )

    def signal(sem, device):
        pl.semaphore_signal(sem, inc=1, device_id=device, device_id_type=MESH)

    up, down = at(0, 1), at(0, inner - 1)
    y_up, y_down, y_far = (lax.rem(y + k, inner) for k in (1, inner - 1, 2))

    def up_copy(source, q, relay):
        piece = weights_in.at[source, q]
        return remote(piece, piece, send_sem.at[2], weight_recv.at[relay, 0, q], (up, part))

    def down_copy(source, q, relay):
        piece = weights_in.at[source, q]
        return remote(piece, piece, send_sem.at[2], weight_recv.at[relay, 1, q], (down, part))

    def over_copy(k, source, q):
        return remote(
            weights_in.at[source, q],
            weights_over.at[source, q],
            send_sem.at[3],
            over_recv.at[k],
            (me, other),
        )

    def over_in(k, source):
        return remote(
            weights_in.at[source],
            weights_over.at[source],
            send_sem.at[3],
            over_recv.at[k],
            (me, other),
        )

    with jax.named_scope("a_greet"):
        small = [
            pltpu.make_async_copy(away, here, small_sem.at[i])
            for i, (away, here) in enumerate(
                (
                    (task_hbm, task_ref),
                    (owner_hbm, owner_ref),
                    (slot_hbm, slot_ref),
                    (length_hbm, length_ref),
                    (query_hbm, query_ref),
                    (key_scale_hbm, key_scale_ref),
                    (value_scale_hbm, value_scale_ref),
                    (new_key_hbm, new_key_ref),
                    (new_value_hbm, new_value_ref),
                )
            )
        ]
        for copy in small:
            copy.start()
        barrier = pltpu.get_barrier_semaphore()
        for kz, ky in far:
            signal(barrier, (at(kz, ky), part))
        for k in range(1, mp):
            signal(barrier, (me, lax.rem(part + k, mp)))
        fetches = [
            pltpu.make_async_copy(weight_hbm, weights_in.at[y], local_sem.at[2]),
            pltpu.make_async_copy(key_hbm, keys, local_sem.at[0]),
            pltpu.make_async_copy(value_hbm, values, local_sem.at[1]),
        ]
        for fetch in fetches:
            fetch.start()
    with jax.named_scope("a_first"):
        for copy in small:
            copy.wait()

    with jax.named_scope("b_pack"):
        task_column = to_column(task_ref[...].astype(f32))
        length_column = to_column(length_ref[...].astype(f32))
        slot_column = to_column(slot_ref[...].astype(f32))
        picked = task_column == iota((rows, task_total), 1).astype(f32)
        owner_column = jnp.sum(
            jnp.where(picked, owner_ref[...].astype(f32), 0.0), axis=1, keepdims=True
        )
        owner_row = to_row(owner_column)
        task_rows = one_hot(picked)
        key_factor = dot(task_rows, key_scale_ref[...])
        factor[...] = dot(task_rows, value_scale_ref[...])
        pieces = []
        for h in range(heads):
            lanes = slice(h * HEAD_SIZE, (h + 1) * HEAD_SIZE)
            pieces.append((query_ref[:, lanes].astype(f32) * key_factor).astype(bf16))
        pieces.append(new_key_ref[...])
        pieces.append(new_value_ref[...])
        pieces.append(jnp.broadcast_to(slot_column, (rows, HEAD_SIZE)).astype(bf16))
        pieces.append(jnp.broadcast_to(length_column, (rows, HEAD_SIZE)).astype(bf16))
        wide = len(pieces) * rows
        spread = one_hot(lax.rem(iota((rows, wide), 1), rows) == iota((rows, wide), 0))
        owner_wide = dot(owner_row.astype(bf16), spread)
        line = iota((dp * PAGE, wide), 0)
        lane = iota((dp * PAGE, wide), 1)
        packer = one_hot(
            (lax.rem(line, PAGE) == lane // rows) & ((line // PAGE).astype(f32) == owner_wide)
        )
        packed = dot(packer, jnp.concatenate(pieces, axis=0))
        send_rows[...] = packed.astype(bf16).reshape(dp, PAGE, HEAD_SIZE)
        line = iota((heads * rows, dp * heads), 0)
        lane = iota((heads * rows, dp * heads), 1)
        same = lax.rem(iota((heads * rows, rows), 0), rows) == iota((heads * rows, rows), 1)
        owner_tall = jnp.sum(jnp.where(same, owner_row, 0.0), axis=1, keepdims=True)
        selector[...] = one_hot(
            (line // rows == lax.rem(lane, heads)) & ((lane // heads).astype(f32) == owner_tall)
        )

    def request_copy(offset):
        return remote(
            send_rows.at[at(*offset)],
            recv_rows.at[me],
            send_sem.at[0],
            request_recv.at[group_of[offset]],
            (at(*offset), part),
        )

    def requests_in(group, count):
        pages = pl.ds(0, count)
        return remote(
            send_rows.at[pages],
            recv_rows.at[pages],
            send_sem.at[0],
            request_recv.at[group],
            (me, other),
        )

    def home_copy(offset):
        return remote(
            home_send.at[at(*offset)],
            home_recv.at[me],
            send_sem.at[1],
            home_recv_sem.at[0],
            (at(*offset), part),
        )

    def homes_in():
        pages = pl.ds(0, dp - 1)
        return remote(
            home_send.at[pages],
            home_recv.at[pages],
            send_sem.at[1],
            home_recv_sem.at[0],
            (me, other),
        )

    with jax.named_scope("c_barwait"):
        pl.semaphore_wait(barrier, dp + mp - 2)
    with jax.named_scope("d_reqsend"):
        for offset in far:
            request_copy(offset).start()
        recv_rows[me] = send_rows[me]
        fetches[0].wait()
        up_copy(y, 0, 0).start()
        down_copy(y, 2, 0).start()
        up_copy(y, 1, 0).start()
        down_copy(y, 3, 0).start()
        up_copy(y, 2, 0).start()
        down_copy(y, 0, 0).start()
        for q in range(QUARTERS):
            over_copy(0, y, q).start()
        fetches[1].wait()
        fetches[2].wait()

    inv_root = 1.0 / math.sqrt(HEAD_SIZE)
    key_line = lax.rem(iota((heads, positions), 1), HEAD_SIZE).astype(f32)

    def attend(sources):
        queries, extras, picks, limits = [], [], [], []
        for s in sources:
            page = recv_rows[s]
            queries.append(page[:heads])
            extra = page[heads:].astype(f32)
            extras.append(extra)
            picks.append(jnp.clip(jnp.max(extra[2:3]).astype(jnp.int32), 0, slots - 1))
            length = jnp.broadcast_to(extra[3:4], (heads, HEAD_SIZE))
            limits.append(
                jnp.concatenate(
                    [length - i * HEAD_SIZE for i in range(positions // HEAD_SIZE)], axis=1
                )
            )
        scores = [
            lax.dot_general(
                q, keys[p], (((1,), (1,)), ((), ())), preferred_element_type=f32
            )
            * inv_root
            for q, p in zip(queries, picks)
        ]
        owns = [
            jnp.sum(q.astype(f32) * extra[0:1], axis=1, keepdims=True) * inv_root
            for q, extra in zip(queries, extras)
        ]
        shown = [
            jnp.where(key_line < limit, score, masked_score)
            for score, limit in zip(scores, limits)
        ]
        tops = [
            jnp.maximum(jnp.max(score, axis=1, keepdims=True), own)
            for score, own in zip(shown, owns)
        ]
        weights = [
            jnp.where(key_line < limit, jnp.exp(score - top), 0.0)
            for score, limit, top in zip(shown, limits, tops)
        ]
        own_weights = [jnp.exp(own - top) for own, top in zip(owns, tops)]
        blends = [dot(weight.astype(bf16), values[p]) for weight, p in zip(weights, picks)]
        sums = [
            jnp.sum(weight, axis=1, keepdims=True) + own
            for weight, own in zip(weights, own_weights)
        ]
        for s, blend, own, extra, total in zip(sources, blends, own_weights, extras, sums):
            blended = blend + own.astype(bf16).astype(f32) * extra[1:2]
            home_send[s] = (blended / total).astype(bf16)

    for g in range(0, dp, TOGETHER):
        group = near[g : g + TOGETHER]
        with jax.named_scope("e_reqwait"):
            requests_in(g // TOGETHER, TOGETHER if g > 0 else TOGETHER - 1).wait_recv()
        with jax.named_scope("f_attend"):
            attend([at(*back(offset)) for offset in group])
        with jax.named_scope("g_homesend"):
            for offset in reversed(group):
                if offset != (0, 0):
                    home_copy(back(offset)).start()
            if g == 0:
                home_recv[me] = home_send[me]

    with jax.named_scope("j_relay"):
        up_copy(y, 3, 0).start()
        down_copy(y, 1, 0).start()
        for q in (0, 1):
            up_copy(y_down, q, 0).wait_recv()
            up_copy(y_down, q, 1).start()
            over_copy(1, y_down, q).start()
            down_copy(y_up, q + 2, 0).wait_recv()
            down_copy(y_up, q + 2, 1).start()
            over_copy(2, y_up, q + 2).start()
    with jax.named_scope("k_homewait"):
        homes_in().wait_recv()

    mine = lax.rem(z, 2)

    with jax.named_scope("l_compact"):
        chosen = dot(selector[...], home_recv[...].reshape(dp * heads, HEAD_SIZE))
        for h in range(heads):
            block[:, h * HEAD_SIZE : (h + 1) * HEAD_SIZE] = (
                chosen[h * rows : (h + 1) * rows] * factor[...]
            ).astype(bf16)

    homes = outer // 2
    middle = query_width // 2
    quarter = query_width // QUARTERS

    def place(source, home):
        return source * homes + lax.rem(home, outer) // 2

    def context_copy(k):
        return remote(
            block,
            contexts.at[place(core, z)],
            send_sem.at[4],
            context_recv.at[0],
            (at(k, 0), 2 * chip + mine),
        )

    def context_relay(source, k, half):
        spot = contexts.at[place(source, z + outer - k), :, pl.ds(half * middle, middle)]
        return remote(spot, spot, send_sem.at[4], context_recv.at[0], (at(k, 0), part))

    def contexts_in(k, count):
        blocks = contexts.at[pl.ds(0, count)]
        return remote(blocks, blocks, send_sem.at[4], context_recv.at[k], (me, other))

    with jax.named_scope("m_ctxsend"):
        for k in (4, 3, 5, 2, 6, 1, 7):
            context_copy(k).start()

        @pl.when(mine != core)
        def _():
            context_copy(0).start()

        @pl.when(mine == core)
        def _():
            contexts[place(core, z)] = block[...]

    with jax.named_scope("n_overs"):
        for q in (0, 1):
            up_copy(y_down, q + 2, 0).wait_recv()
            over_copy(1, y_down, q + 2).start()
            down_copy(y_up, q, 0).wait_recv()
            over_copy(2, y_up, q).start()

    with jax.named_scope("n_overs2"):
        for q in (0, 1):
            up_copy(y_far, q, 1).wait_recv()
            over_copy(3, y_far, q).start()
            down_copy(y_far, q + 2, 1).wait_recv()
            over_copy(3, y_far, q + 2).start()

    with jax.named_scope("o_ctxwait"):

        @pl.when(mine == core)
        def _():
            contexts_in(0, 7).wait_recv()

        @pl.when(mine != core)
        def _():
            contexts_in(0, 2 * homes).wait_recv()

    shift = lax.rem(z + core, 2)

    def part_copy(n, column, i):
        target = lax.rem(z + 2 * i + shift, outer)
        return remote(
            send_part.at[column, target // 2],
            recv_part.at[column, chip],
            send_sem.at[5],
            part_recv.at[n],
            (target * inner + y, z),
        )

    def parts_in(n, count):
        parts = pl.ds(0, count)
        return remote(
            send_part.at[0, parts],
            recv_part.at[0, parts],
            send_sem.at[5],
            part_recv.at[n],
            (me, other),
        )

    order = (y, y_down, y_up, y_far)

    with jax.named_scope("p_project"):
        direct = contexts[pl.ds(core * homes, homes)].reshape(homes * rows, query_width)
        over = contexts[pl.ds((1 - core) * homes, homes)].reshape(homes * rows, query_width)
        for n, column in enumerate(order):
            over_in(n, column).wait_recv()
            summed = jnp.zeros((homes * rows, columns), f32)
            for q in range(QUARTERS):
                depth = slice(q * quarter, (q + 1) * quarter)
                summed = summed + dot(direct[:, depth], weights_in[column, q])
                summed = summed + dot(over[:, depth], weights_over[column, q])
            send_part[column] = summed.astype(bf16).reshape(homes, rows, columns)
            for i in (2, 1, 3):
                part_copy(n, column, i).start()

            @pl.when(z != part)
            def _():
                part_copy(n, column, 0).start()

            @pl.when(z == part)
            def _():
                recv_part[column, chip] = send_part[column, z // 2]

    with jax.named_scope("q_drain"):
        requests_in(0, dp - 1).wait_send()
        homes_in().wait_send()
        three = weights_in.at[pl.ds(0, inner - 1)]
        remote(three, three, send_sem.at[2], weight_recv.at[0, 0, 0], (me, other)).wait_send()
        remote(weights_in, weights_over, send_sem.at[3], over_recv.at[0], (me, other)).wait_send()

        @pl.when(mine == core)
        def _():
            contexts_in(0, 2 * homes - 1).wait_send()

        @pl.when(mine != core)
        def _():
            contexts_in(0, 2 * homes).wait_send()

    with jax.named_scope("r_partwait"):
        for n, column in enumerate(order):

            @pl.when(z != part)
            def _():
                parts_in(n, mp // 2).wait_recv()

            @pl.when(z == part)
            def _():
                parts_in(n, mp // 2 - 1).wait_recv()

            summed = recv_part[column, 0].astype(f32)
            for j in range(1, mp // 2):
                summed = summed + recv_part[column, j].astype(f32)
            start = pl.multiple_of(column * columns, columns)
            out_ref[:, pl.ds(start, columns)] = summed.astype(bf16)

    with jax.named_scope("s_drain"):

        @pl.when(z != part)
        def _():
            remote(send_part, send_part, send_sem.at[5], part_recv.at[0], (me, other)).wait_send()

        @pl.when(z == part)
        def _():
            most = send_part.at[:, pl.ds(0, mp // 2 - 1)]
            remote(most, most, send_sem.at[5], part_recv.at[0], (me, other)).wait_send()


def on_device(
    dp,
    mp,
    queries,
    incoming_key,
    incoming_value,
    key_cache,
    cached_values,
    task_key_scale,
    task_value_scale,
    out_weight,
    task_id,
    cached_length,
    task_owner,
    cache_slot,
):
    rows, query_width = queries.shape
    depth, columns = out_weight.shape
    heads = query_width // HEAD_SIZE
    inner = dp // mp
    small = (
        queries,
        incoming_key,
        incoming_value,
        task_key_scale,
        task_value_scale,
        task_id.reshape(1, -1),
        cached_length.reshape(1, -1),
        cache_slot.reshape(1, -1),
        task_owner.reshape(1, -1),
    )
    away = pl.BlockSpec(memory_space=pl.ANY)
    return pl.pallas_call(
        functools.partial(layer_kernel, dp, mp),
        out_shape=jax.ShapeDtypeStruct((rows, inner * columns), bf16),
        in_specs=[away] * 12,
        out_specs=pl.BlockSpec(memory_space=pltpu.VMEM),
        scratch_shapes=[pltpu.VMEM(array.shape, array.dtype) for array in small]
        + [
            pltpu.VMEM(key_cache.shape, bf16),
            pltpu.VMEM(cached_values.shape, bf16),
            pltpu.VMEM((inner, QUARTERS, depth // QUARTERS, columns), bf16),
            pltpu.VMEM((inner, QUARTERS, depth // QUARTERS, columns), bf16),
            pltpu.VMEM((dp, PAGE, HEAD_SIZE), bf16),
            pltpu.VMEM((dp, PAGE, HEAD_SIZE), bf16),
            pltpu.VMEM((dp, heads, HEAD_SIZE), bf16),
            pltpu.VMEM((dp, heads, HEAD_SIZE), bf16),
            pltpu.VMEM((heads * rows, dp * heads), bf16),
            pltpu.VMEM((rows, HEAD_SIZE), f32),
            pltpu.VMEM((mp, rows, query_width), bf16),
            pltpu.VMEM((rows, query_width), bf16),
            pltpu.VMEM((inner, mp // 2, rows, columns), bf16),
            pltpu.VMEM((inner, mp // 2, rows, columns), bf16),
            pltpu.SemaphoreType.DMA((3,)),
            pltpu.SemaphoreType.DMA((len(small),)),
            pltpu.SemaphoreType.DMA((6,)),
            pltpu.SemaphoreType.DMA((dp // TOGETHER,)),
            pltpu.SemaphoreType.DMA((1,)),
            pltpu.SemaphoreType.DMA((2, 2, QUARTERS)),
            pltpu.SemaphoreType.DMA((inner,)),
            pltpu.SemaphoreType.DMA((3,)),
            pltpu.SemaphoreType.DMA((inner,)),
        ],
        compiler_params=pltpu.CompilerParams(
            collective_id=0, has_side_effects=True, vmem_limit_bytes=60 * 1024 * 1024
        ),
    )(*small, key_cache, cached_values, out_weight.reshape(QUARTERS, depth // QUARTERS, columns))


def solution(mesh):
    placed = (
        P("dp", "mp"),
        P("dp", "mp"),
        P("dp", "mp"),
        P("dp", None, "mp"),
        P("dp", None, "mp"),
        P(None, "mp"),
        P(None, "mp"),
        P("mp", "dp"),
        P("dp"),
        P("dp"),
        P(),
        P("dp"),
    )
    return jax.shard_map(
        functools.partial(on_device, mesh.shape["dp"], mesh.shape["mp"]),
        mesh=mesh,
        in_specs=placed,
        out_specs=P("dp", "mp"),
        check_vma=False,
    )
```

```python
import functools
import math

import jax
import jax.numpy as jnp
from jax import lax
from jax.experimental import pallas as pl
from jax.experimental.pallas import tpu as pltpu
from jax.sharding import PartitionSpec as P

HEAD_SIZE = 128
PAGE = 16
TOGETHER = 32
QUARTERS = 4
MESH = pl.DeviceIdType.MESH

masked_score = -1e30
f32 = jnp.float32
bf16 = jnp.bfloat16


def iota(shape, dim):
    return lax.broadcasted_iota(jnp.int32, shape, dim)


def ring(k, n):
    return min(k, n - k)


def to_column(row):
    n = row.shape[1]
    eye = iota((n, n), 0) == iota((n, n), 1)
    return jnp.sum(jnp.where(eye, row, 0.0), axis=1, keepdims=True)


def to_row(column):
    n = column.shape[0]
    eye = iota((n, n), 0) == iota((n, n), 1)
    return jnp.sum(jnp.where(eye, column, 0.0), axis=0, keepdims=True)


def dot(a, b):
    return jnp.dot(a, b, preferred_element_type=f32)


def one_hot(mask):
    return jnp.where(mask, 1.0, 0.0).astype(bf16)


def layer_kernel(
    dp,
    mp,
    query_hbm,
    new_key_hbm,
    new_value_hbm,
    key_scale_hbm,
    value_scale_hbm,
    task_hbm,
    length_hbm,
    slot_hbm,
    owner_hbm,
    key_hbm,
    value_hbm,
    weight_hbm,
    out_ref,
    query_ref,
    new_key_ref,
    new_value_ref,
    key_scale_ref,
    value_scale_ref,
    task_ref,
    length_ref,
    slot_ref,
    owner_ref,
    keys,
    values,
    weights_in,
    weights_over,
    send_rows,
    recv_rows,
    home_send,
    home_recv,
    selector,
    factor,
    contexts,
    block,
    send_part,
    recv_part,
    local_sem,
    small_sem,
    send_sem,
    request_recv,
    home_recv_sem,
    weight_recv,
    over_recv,
    context_recv,
    part_recv,
):
    me = lax.axis_index("dp")
    part = lax.axis_index("mp")
    rows, query_width = query_ref.shape
    heads = query_width // HEAD_SIZE
    task_total = key_scale_ref.shape[0]
    slots, positions, _ = keys.shape
    columns = weights_in.shape[3]
    inner = dp // mp
    outer = mp
    z, y = me // inner, lax.rem(me, inner)
    chip, core = part // 2, lax.rem(part, 2)
    other = 2 * chip + 1 - core

    def at(kz, ky):
        return lax.rem(z + kz, outer) * inner + lax.rem(y + ky, inner)

    def distance(offset):
        return ring(offset[0], outer) + ring(offset[1], inner)

    def back(offset):
        return (outer - offset[0]) % outer, (inner - offset[1]) % inner

    near = sorted(((kz, ky) for kz in range(outer) for ky in range(inner)), key=distance)
    far = near[:0:-1]
    group_of = {offset: n // TOGETHER for n, offset in enumerate(near)}

    def remote(source, target, send_sem, recv_sem, device):
        return pltpu.make_async_remote_copy(
            src_ref=source,
            dst_ref=target,
            send_sem=send_sem,
            recv_sem=recv_sem,
            device_id=device,
            device_id_type=MESH,
        )

    def signal(sem, device):
        pl.semaphore_signal(sem, inc=1, device_id=device, device_id_type=MESH)

    up, down = at(0, 1), at(0, inner - 1)
    y_up, y_down, y_far = (lax.rem(y + k, inner) for k in (1, inner - 1, 2))

    def up_copy(source, q, relay):
        piece = weights_in.at[source, q]
        return remote(piece, piece, send_sem.at[2], weight_recv.at[relay, 0, q], (up, part))

    def down_copy(source, q, relay):
        piece = weights_in.at[source, q]
        return remote(piece, piece, send_sem.at[2], weight_recv.at[relay, 1, q], (down, part))

    def over_copy(k, source, q):
        return remote(
            weights_in.at[source, q],
            weights_over.at[source, q],
            send_sem.at[3],
            over_recv.at[k],
            (me, other),
        )

    def over_in(k, source):
        return remote(
            weights_in.at[source],
            weights_over.at[source],
            send_sem.at[3],
            over_recv.at[k],
            (me, other),
        )

    with jax.named_scope("a_greet"):
        small = [
            pltpu.make_async_copy(away, here, small_sem.at[i])
            for i, (away, here) in enumerate(
                (
                    (task_hbm, task_ref),
                    (owner_hbm, owner_ref),
                    (slot_hbm, slot_ref),
                    (length_hbm, length_ref),
                    (query_hbm, query_ref),
                    (key_scale_hbm, key_scale_ref),
                    (value_scale_hbm, value_scale_ref),
                    (new_key_hbm, new_key_ref),
                    (new_value_hbm, new_value_ref),
                )
            )
        ]
        for copy in small:
            copy.start()
        barrier = pltpu.get_barrier_semaphore()
        for kz, ky in far:
            signal(barrier, (at(kz, ky), part))
        for k in range(1, mp):
            signal(barrier, (me, lax.rem(part + k, mp)))
        fetches = [
            pltpu.make_async_copy(weight_hbm, weights_in.at[y], local_sem.at[2]),
            pltpu.make_async_copy(key_hbm, keys, local_sem.at[0]),
            pltpu.make_async_copy(value_hbm, values, local_sem.at[1]),
        ]
        for fetch in fetches:
            fetch.start()
    with jax.named_scope("a_first"):
        for copy in small:
            copy.wait()

    with jax.named_scope("b_pack"):
        task_column = to_column(task_ref[...].astype(f32))
        length_column = to_column(length_ref[...].astype(f32))
        slot_column = to_column(slot_ref[...].astype(f32))
        picked = task_column == iota((rows, task_total), 1).astype(f32)
        owner_column = jnp.sum(
            jnp.where(picked, owner_ref[...].astype(f32), 0.0), axis=1, keepdims=True
        )
        owner_row = to_row(owner_column)
        task_rows = one_hot(picked)
        key_factor = dot(task_rows, key_scale_ref[...])
        factor[...] = dot(task_rows, value_scale_ref[...])
        pieces = []
        for h in range(heads):
            lanes = slice(h * HEAD_SIZE, (h + 1) * HEAD_SIZE)
            pieces.append((query_ref[:, lanes].astype(f32) * key_factor).astype(bf16))
        pieces.append(new_key_ref[...])
        pieces.append(new_value_ref[...])
        pieces.append(jnp.broadcast_to(slot_column, (rows, HEAD_SIZE)).astype(bf16))
        pieces.append(jnp.broadcast_to(length_column, (rows, HEAD_SIZE)).astype(bf16))
        wide = len(pieces) * rows
        spread = one_hot(lax.rem(iota((rows, wide), 1), rows) == iota((rows, wide), 0))
        owner_wide = dot(owner_row.astype(bf16), spread)
        line = iota((dp * PAGE, wide), 0)
        lane = iota((dp * PAGE, wide), 1)
        packer = one_hot(
            (lax.rem(line, PAGE) == lane // rows) & ((line // PAGE).astype(f32) == owner_wide)
        )
        packed = dot(packer, jnp.concatenate(pieces, axis=0))
        send_rows[...] = packed.astype(bf16).reshape(dp, PAGE, HEAD_SIZE)
        line = iota((heads * rows, dp * heads), 0)
        lane = iota((heads * rows, dp * heads), 1)
        same = lax.rem(iota((heads * rows, rows), 0), rows) == iota((heads * rows, rows), 1)
        owner_tall = jnp.sum(jnp.where(same, owner_row, 0.0), axis=1, keepdims=True)
        selector[...] = one_hot(
            (line // rows == lax.rem(lane, heads)) & ((lane // heads).astype(f32) == owner_tall)
        )

    def request_copy(offset):
        return remote(
            send_rows.at[at(*offset)],
            recv_rows.at[me],
            send_sem.at[0],
            request_recv.at[group_of[offset]],
            (at(*offset), part),
        )

    def requests_in(group, count):
        pages = pl.ds(0, count)
        return remote(
            send_rows.at[pages],
            recv_rows.at[pages],
            send_sem.at[0],
            request_recv.at[group],
            (me, other),
        )

    def home_copy(offset):
        return remote(
            home_send.at[at(*offset)],
            home_recv.at[me],
            send_sem.at[1],
            home_recv_sem.at[0],
            (at(*offset), part),
        )

    def homes_in():
        pages = pl.ds(0, dp - 1)
        return remote(
            home_send.at[pages],
            home_recv.at[pages],
            send_sem.at[1],
            home_recv_sem.at[0],
            (me, other),
        )

    with jax.named_scope("c_barwait"):
        pl.semaphore_wait(barrier, dp + mp - 2)
    with jax.named_scope("d_reqsend"):
        for offset in far:
            request_copy(offset).start()
        recv_rows[me] = send_rows[me]
        fetches[0].wait()
        up_copy(y, 0, 0).start()
        down_copy(y, 2, 0).start()
        up_copy(y, 1, 0).start()
        down_copy(y, 3, 0).start()
        up_copy(y, 2, 0).start()
        down_copy(y, 0, 0).start()
        for q in range(QUARTERS):
            over_copy(0, y, q).start()
        fetches[1].wait()
        fetches[2].wait()

    inv_root = 1.0 / math.sqrt(HEAD_SIZE)
    key_line = lax.rem(iota((heads, positions), 1), HEAD_SIZE).astype(f32)

    def attend(sources):
        queries, extras, picks, limits = [], [], [], []
        for s in sources:
            page = recv_rows[s]
            queries.append(page[:heads])
            extra = page[heads:].astype(f32)
            extras.append(extra)
            picks.append(jnp.clip(jnp.max(extra[2:3]).astype(jnp.int32), 0, slots - 1))
            length = jnp.broadcast_to(extra[3:4], (heads, HEAD_SIZE))
            limits.append(
                jnp.concatenate(
                    [length - i * HEAD_SIZE for i in range(positions // HEAD_SIZE)], axis=1
                )
            )
        scores = [
            lax.dot_general(
                q, keys[p], (((1,), (1,)), ((), ())), preferred_element_type=f32
            )
            * inv_root
            for q, p in zip(queries, picks)
        ]
        owns = [
            jnp.sum(q.astype(f32) * extra[0:1], axis=1, keepdims=True) * inv_root
            for q, extra in zip(queries, extras)
        ]
        shown = [
            jnp.where(key_line < limit, score, masked_score)
            for score, limit in zip(scores, limits)
        ]
        tops = [
            jnp.maximum(jnp.max(score, axis=1, keepdims=True), own)
            for score, own in zip(shown, owns)
        ]
        weights = [
            jnp.where(key_line < limit, jnp.exp(score - top), 0.0)
            for score, limit, top in zip(shown, limits, tops)
        ]
        own_weights = [jnp.exp(own - top) for own, top in zip(owns, tops)]
        blends = [dot(weight.astype(bf16), values[p]) for weight, p in zip(weights, picks)]
        sums = [
            jnp.sum(weight, axis=1, keepdims=True) + own
            for weight, own in zip(weights, own_weights)
        ]
        for s, blend, own, extra, total in zip(sources, blends, own_weights, extras, sums):
            blended = blend + own.astype(bf16).astype(f32) * extra[1:2]
            home_send[s] = (blended / total).astype(bf16)

    for g in range(0, dp, TOGETHER):
        group = near[g : g + TOGETHER]
        with jax.named_scope("e_reqwait"):
            requests_in(g // TOGETHER, TOGETHER if g > 0 else TOGETHER - 1).wait_recv()
        with jax.named_scope("f_attend"):
            attend([at(*back(offset)) for offset in group])
        with jax.named_scope("g_homesend"):
            for offset in reversed(group):
                if offset != (0, 0):
                    home_copy(back(offset)).start()
            if g == 0:
                home_recv[me] = home_send[me]

    with jax.named_scope("j_relay"):
        up_copy(y, 3, 0).start()
        down_copy(y, 1, 0).start()
        for q in (0, 1):
            up_copy(y_down, q, 0).wait_recv()
            up_copy(y_down, q, 1).start()
            over_copy(1, y_down, q).start()
            down_copy(y_up, q + 2, 0).wait_recv()
            down_copy(y_up, q + 2, 1).start()
            over_copy(2, y_up, q + 2).start()
    with jax.named_scope("k_homewait"):
        homes_in().wait_recv()

    mine = lax.rem(z, 2)

    with jax.named_scope("l_compact"):
        chosen = dot(selector[...], home_recv[...].reshape(dp * heads, HEAD_SIZE))
        for h in range(heads):
            block[:, h * HEAD_SIZE : (h + 1) * HEAD_SIZE] = (
                chosen[h * rows : (h + 1) * rows] * factor[...]
            ).astype(bf16)

    homes = outer // 2
    middle = query_width // 2
    quarter = query_width // QUARTERS

    def place(source, home):
        return source * homes + lax.rem(home, outer) // 2

    def context_copy(k):
        return remote(
            block,
            contexts.at[place(core, z)],
            send_sem.at[4],
            context_recv.at[0],
            (at(k, 0), 2 * chip + mine),
        )

    def context_relay(source, k, half):
        spot = contexts.at[place(source, z + outer - k), :, pl.ds(half * middle, middle)]
        return remote(spot, spot, send_sem.at[4], context_recv.at[0], (at(k, 0), part))

    def contexts_in(k, count):
        blocks = contexts.at[pl.ds(0, count)]
        return remote(blocks, blocks, send_sem.at[4], context_recv.at[k], (me, other))

    with jax.named_scope("m_ctxsend"):
        for k in (4, 3, 5, 2, 6, 1, 7):
            context_copy(k).start()

        @pl.when(mine != core)
        def _():
            context_copy(0).start()

        @pl.when(mine == core)
        def _():
            contexts[place(core, z)] = block[...]

    with jax.named_scope("n_overs"):
        for q in (0, 1):
            up_copy(y_down, q + 2, 0).wait_recv()
            over_copy(1, y_down, q + 2).start()
            down_copy(y_up, q, 0).wait_recv()
            over_copy(2, y_up, q).start()

    with jax.named_scope("n_overs2"):
        for q in (0, 1):
            up_copy(y_far, q, 1).wait_recv()
            over_copy(3, y_far, q).start()
            down_copy(y_far, q + 2, 1).wait_recv()
            over_copy(3, y_far, q + 2).start()

    with jax.named_scope("o_ctxwait"):

        @pl.when(mine == core)
        def _():
            contexts_in(0, 7).wait_recv()

        @pl.when(mine != core)
        def _():
            contexts_in(0, 2 * homes).wait_recv()

    shift = lax.rem(z + core, 2)

    def part_copy(n, column, i):
        target = lax.rem(z + 2 * i + shift, outer)
        return remote(
            send_part.at[column, target // 2],
            recv_part.at[column, chip],
            send_sem.at[5],
            part_recv.at[n],
            (target * inner + y, z),
        )

    def parts_in(n, count):
        parts = pl.ds(0, count)
        return remote(
            send_part.at[0, parts],
            recv_part.at[0, parts],
            send_sem.at[5],
            part_recv.at[n],
            (me, other),
        )

    order = (y, y_down, y_up, y_far)

    with jax.named_scope("p_project"):
        direct = contexts[pl.ds(core * homes, homes)].reshape(homes * rows, query_width)
        over = contexts[pl.ds((1 - core) * homes, homes)].reshape(homes * rows, query_width)
        for n, column in enumerate(order):
            over_in(n, column).wait_recv()
            summed = jnp.zeros((homes * rows, columns), f32)
            for q in range(QUARTERS):
                depth = slice(q * quarter, (q + 1) * quarter)
                summed = summed + dot(direct[:, depth], weights_in[column, q])
                summed = summed + dot(over[:, depth], weights_over[column, q])
            send_part[column] = summed.astype(bf16).reshape(homes, rows, columns)
            for i in (2, 1, 3):
                part_copy(n, column, i).start()

            @pl.when(z != part)
            def _():
                part_copy(n, column, 0).start()

            @pl.when(z == part)
            def _():
                recv_part[column, chip] = send_part[column, z // 2]

    with jax.named_scope("q_drain"):
        requests_in(0, dp - 1).wait_send()
        homes_in().wait_send()
        three = weights_in.at[pl.ds(0, inner - 1)]
        remote(three, three, send_sem.at[2], weight_recv.at[0, 0, 0], (me, other)).wait_send()
        remote(weights_in, weights_over, send_sem.at[3], over_recv.at[0], (me, other)).wait_send()

        @pl.when(mine == core)
        def _():
            contexts_in(0, 2 * homes - 1).wait_send()

        @pl.when(mine != core)
        def _():
            contexts_in(0, 2 * homes).wait_send()

    with jax.named_scope("r_partwait"):
        for n, column in enumerate(order):

            @pl.when(z != part)
            def _():
                parts_in(n, mp // 2).wait_recv()

            @pl.when(z == part)
            def _():
                parts_in(n, mp // 2 - 1).wait_recv()

            summed = recv_part[column, 0].astype(f32)
            for j in range(1, mp // 2):
                summed = summed + recv_part[column, j].astype(f32)
            start = pl.multiple_of(column * columns, columns)
            out_ref[:, pl.ds(start, columns)] = summed.astype(bf16)

    with jax.named_scope("s_drain"):

        @pl.when(z != part)
        def _():
            remote(send_part, send_part, send_sem.at[5], part_recv.at[0], (me, other)).wait_send()

        @pl.when(z == part)
        def _():
            most = send_part.at[:, pl.ds(0, mp // 2 - 1)]
            remote(most, most, send_sem.at[5], part_recv.at[0], (me, other)).wait_send()


def on_device(
    dp,
    mp,
    queries,
    incoming_key,
    incoming_value,
    key_cache,
    cached_values,
    task_key_scale,
    task_value_scale,
    out_weight,
    task_id,
    cached_length,
    task_owner,
    cache_slot,
):
    rows, query_width = queries.shape
    depth, columns = out_weight.shape
    heads = query_width // HEAD_SIZE
    inner = dp // mp
    small = (
        queries,
        incoming_key,
        incoming_value,
        task_key_scale,
        task_value_scale,
        task_id.reshape(1, -1),
        cached_length.reshape(1, -1),
        cache_slot.reshape(1, -1),
        task_owner.reshape(1, -1),
    )
    away = pl.BlockSpec(memory_space=pltpu.HBM)
    return pl.pallas_call(
        functools.partial(layer_kernel, dp, mp),
        out_shape=jax.ShapeDtypeStruct((rows, inner * columns), bf16),
        in_specs=[away] * 12,
        out_specs=pl.BlockSpec(memory_space=pltpu.VMEM),
        scratch_shapes=[pltpu.VMEM(array.shape, array.dtype) for array in small]
        + [
            pltpu.VMEM(key_cache.shape, bf16),
            pltpu.VMEM(cached_values.shape, bf16),
            pltpu.VMEM((inner, QUARTERS, depth // QUARTERS, columns), bf16),
            pltpu.VMEM((inner, QUARTERS, depth // QUARTERS, columns), bf16),
            pltpu.VMEM((dp, PAGE, HEAD_SIZE), bf16),
            pltpu.VMEM((dp, PAGE, HEAD_SIZE), bf16),
            pltpu.VMEM((dp, heads, HEAD_SIZE), bf16),
            pltpu.VMEM((dp, heads, HEAD_SIZE), bf16),
            pltpu.VMEM((heads * rows, dp * heads), bf16),
            pltpu.VMEM((rows, HEAD_SIZE), f32),
            pltpu.VMEM((mp, rows, query_width), bf16),
            pltpu.VMEM((rows, query_width), bf16),
            pltpu.VMEM((inner, mp // 2, rows, columns), bf16),
            pltpu.VMEM((inner, mp // 2, rows, columns), bf16),
            pltpu.SemaphoreType.DMA((3,)),
            pltpu.SemaphoreType.DMA((len(small),)),
            pltpu.SemaphoreType.DMA((6,)),
            pltpu.SemaphoreType.DMA((dp // TOGETHER,)),
            pltpu.SemaphoreType.DMA((1,)),
            pltpu.SemaphoreType.DMA((2, 2, QUARTERS)),
            pltpu.SemaphoreType.DMA((inner,)),
            pltpu.SemaphoreType.DMA((3,)),
            pltpu.SemaphoreType.DMA((inner,)),
        ],
        compiler_params=pltpu.CompilerParams(
            collective_id=0, has_side_effects=True, vmem_limit_bytes=20 * 1024 * 1024
        ),
    )(
        *[
            pltpu.with_memory_space_constraint(array, pltpu.HBM)
            for array in (
                *small,
                key_cache,
                cached_values,
                out_weight.reshape(QUARTERS, depth // QUARTERS, columns),
            )
        ]
    )


def solution(mesh):
    placed = (
        P("dp", "mp"),
        P("dp", "mp"),
        P("dp", "mp"),
        P("dp", None, "mp"),
        P("dp", None, "mp"),
        P(None, "mp"),
        P(None, "mp"),
        P("mp", "dp"),
        P("dp"),
        P("dp"),
        P(),
        P("dp"),
    )
    return jax.shard_map(
        functools.partial(on_device, mesh.shape["dp"], mesh.shape["mp"]),
        mesh=mesh,
        in_specs=placed,
        out_specs=P("dp", "mp"),
        check_vma=False,
    )
```

```python
import functools
import math

import jax
import jax.numpy as jnp
from jax import lax
from jax.experimental import pallas as pl
from jax.experimental.pallas import tpu as pltpu
from jax.sharding import PartitionSpec as P

HEAD_SIZE = 128
EXTRA = 4
QUARTERS = 4
MESH = pl.DeviceIdType.MESH

masked_score = -1e30
f32 = jnp.float32
bf16 = jnp.bfloat16


def iota(shape, dim):
    return lax.broadcasted_iota(jnp.int32, shape, dim)


def ring(k, n):
    return min(k, n - k)


def to_column(row):
    n = row.shape[1]
    eye = iota((n, n), 0) == iota((n, n), 1)
    return jnp.sum(jnp.where(eye, row, 0.0), axis=1, keepdims=True)


def to_row(column):
    n = column.shape[0]
    eye = iota((n, n), 0) == iota((n, n), 1)
    return jnp.sum(jnp.where(eye, column, 0.0), axis=0, keepdims=True)


def dot(a, b):
    return jnp.dot(a, b, preferred_element_type=f32)


def one_hot(mask):
    return jnp.where(mask, 1.0, 0.0).astype(bf16)


def layer_kernel(
    dp,
    mp,
    query_hbm,
    new_key_hbm,
    new_value_hbm,
    key_scale_hbm,
    value_scale_hbm,
    task_hbm,
    length_hbm,
    slot_hbm,
    owner_hbm,
    key_hbm,
    value_hbm,
    weight_hbm,
    out_ref,
    query_ref,
    new_key_ref,
    new_value_ref,
    key_scale_ref,
    value_scale_ref,
    task_ref,
    length_ref,
    slot_ref,
    owner_ref,
    keys,
    values,
    weights_in,
    weights_over,
    send_rows,
    send_extra,
    recv_rows,
    recv_extra,
    home_send,
    home_recv,
    selector,
    factor,
    contexts,
    block,
    send_part,
    recv_part,
    local_sem,
    small_sem,
    send_sem,
    request_recv,
    home_recv_sem,
    weight_recv,
    over_recv,
    context_recv,
    part_recv,
):
    me = lax.axis_index("dp")
    part = lax.axis_index("mp")
    rows, query_width = query_ref.shape
    heads = query_width // HEAD_SIZE
    task_total = key_scale_ref.shape[0]
    slots, positions, _ = keys.shape
    columns = weights_in.shape[3]
    inner = dp // mp
    outer = mp
    z, y = me // inner, lax.rem(me, inner)
    chip, core = part // 2, lax.rem(part, 2)
    other = 2 * chip + 1 - core

    def at(kz, ky):
        return lax.rem(z + kz, outer) * inner + lax.rem(y + ky, inner)

    def distance(offset):
        return ring(offset[0], outer) + ring(offset[1], inner)

    def back(offset):
        return (outer - offset[0]) % outer, (inner - offset[1]) % inner

    near = sorted(((kz, ky) for kz in range(outer) for ky in range(inner)), key=distance)
    far = near[:0:-1]

    def remote(source, target, send_sem, recv_sem, device):
        return pltpu.make_async_remote_copy(
            src_ref=source,
            dst_ref=target,
            send_sem=send_sem,
            recv_sem=recv_sem,
            device_id=device,
            device_id_type=MESH,
        )

    def signal(sem, device):
        pl.semaphore_signal(sem, inc=1, device_id=device, device_id_type=MESH)

    up, down = at(0, 1), at(0, inner - 1)
    y_up, y_down, y_far = (lax.rem(y + k, inner) for k in (1, inner - 1, 2))

    def up_copy(source, q, relay):
        piece = weights_in.at[source, q]
        return remote(piece, piece, send_sem.at[2], weight_recv.at[relay, 0, q], (up, part))

    def down_copy(source, q, relay):
        piece = weights_in.at[source, q]
        return remote(piece, piece, send_sem.at[2], weight_recv.at[relay, 1, q], (down, part))

    def over_copy(k, source, q):
        return remote(
            weights_in.at[source, q],
            weights_over.at[source, q],
            send_sem.at[3],
            over_recv.at[k],
            (me, other),
        )

    def over_in(k, source):
        return remote(
            weights_in.at[source],
            weights_over.at[source],
            send_sem.at[3],
            over_recv.at[k],
            (me, other),
        )

    with jax.named_scope("a_greet"):
        small = [
            pltpu.make_async_copy(away, here, small_sem.at[i])
            for i, (away, here) in enumerate(
                (
                    (task_hbm, task_ref),
                    (owner_hbm, owner_ref),
                    (slot_hbm, slot_ref),
                    (length_hbm, length_ref),
                    (query_hbm, query_ref),
                    (key_scale_hbm, key_scale_ref),
                    (value_scale_hbm, value_scale_ref),
                    (new_key_hbm, new_key_ref),
                    (new_value_hbm, new_value_ref),
                )
            )
        ]
        for copy in small:
            copy.start()
        barrier = pltpu.get_barrier_semaphore()
        for kz, ky in far:
            signal(barrier, (at(kz, ky), part))
        for k in range(1, mp):
            signal(barrier, (me, lax.rem(part + k, mp)))
        fetches = [
            pltpu.make_async_copy(weight_hbm, weights_in.at[y], local_sem.at[2]),
            pltpu.make_async_copy(key_hbm, keys, local_sem.at[0]),
            pltpu.make_async_copy(value_hbm, values, local_sem.at[1]),
        ]
        for fetch in fetches:
            fetch.start()
    with jax.named_scope("a_first"):
        for copy in small:
            copy.wait()

    with jax.named_scope("b_pack"):
        task_column = to_column(task_ref[...].astype(f32))
        length_column = to_column(length_ref[...].astype(f32))
        slot_column = to_column(slot_ref[...].astype(f32))
        picked = task_column == iota((rows, task_total), 1).astype(f32)
        owner_column = jnp.sum(
            jnp.where(picked, owner_ref[...].astype(f32), 0.0), axis=1, keepdims=True
        )
        owner_row = to_row(owner_column)
        task_rows = one_hot(picked)
        key_factor = dot(task_rows, key_scale_ref[...])
        factor[...] = dot(task_rows, value_scale_ref[...])
        pieces = []
        for h in range(heads):
            lanes = slice(h * HEAD_SIZE, (h + 1) * HEAD_SIZE)
            pieces.append((query_ref[:, lanes].astype(f32) * key_factor).astype(bf16))
        pieces.append(new_key_ref[...])
        pieces.append(new_value_ref[...])
        pieces.append(jnp.broadcast_to(slot_column, (rows, HEAD_SIZE)).astype(bf16))
        pieces.append(jnp.broadcast_to(length_column, (rows, HEAD_SIZE)).astype(bf16))
        wide = len(pieces) * rows
        spread = one_hot(lax.rem(iota((rows, wide), 1), rows) == iota((rows, wide), 0))
        owner_wide = dot(owner_row.astype(bf16), spread)
        ready_rows = jnp.concatenate(pieces, axis=0)
        for into, first, count in ((send_rows, 0, heads), (send_extra, heads, EXTRA)):
            line = iota((dp * count, wide), 0)
            lane = iota((dp * count, wide), 1)
            packer = one_hot(
                (lax.rem(line, count) + first == lane // rows)
                & ((line // count).astype(f32) == owner_wide)
            )
            into[...] = dot(packer, ready_rows).astype(bf16).reshape(dp, count, HEAD_SIZE)
        line = iota((heads * rows, dp * heads), 0)
        lane = iota((heads * rows, dp * heads), 1)
        same = lax.rem(iota((heads * rows, rows), 0), rows) == iota((heads * rows, rows), 1)
        owner_tall = jnp.sum(jnp.where(same, owner_row, 0.0), axis=1, keepdims=True)
        selector[...] = one_hot(
            (line // rows == lax.rem(lane, heads)) & ((lane // heads).astype(f32) == owner_tall)
        )

    def request_copy(offset):
        return [
            remote(
                source.at[at(*offset)],
                target.at[me],
                send_sem.at[sem],
                request_recv.at[n],
                (at(*offset), part),
            )
            for n, (source, target, sem) in enumerate(
                ((send_rows, recv_rows, 0), (send_extra, recv_extra, 6))
            )
        ]

    def requests_in():
        pages = pl.ds(0, dp - 1)
        return [
            remote(
                source.at[pages],
                target.at[pages],
                send_sem.at[sem],
                request_recv.at[n],
                (me, other),
            )
            for n, (source, target, sem) in enumerate(
                ((send_rows, recv_rows, 0), (send_extra, recv_extra, 6))
            )
        ]

    def home_copy(offset):
        return remote(
            home_send.at[at(*offset)],
            home_recv.at[me],
            send_sem.at[1],
            home_recv_sem.at[0],
            (at(*offset), part),
        )

    def homes_in():
        pages = pl.ds(0, dp - 1)
        return remote(
            home_send.at[pages],
            home_recv.at[pages],
            send_sem.at[1],
            home_recv_sem.at[0],
            (me, other),
        )

    with jax.named_scope("c_barwait"):
        pl.semaphore_wait(barrier, dp + mp - 2)
    with jax.named_scope("d_reqsend"):
        for offset in far:
            for copy in request_copy(offset):
                copy.start()
        recv_rows[me] = send_rows[me]
        recv_extra[me] = send_extra[me]
        fetches[0].wait()
        up_copy(y, 0, 0).start()
        down_copy(y, 2, 0).start()
        up_copy(y, 1, 0).start()
        down_copy(y, 3, 0).start()
        up_copy(y, 2, 0).start()
        down_copy(y, 0, 0).start()
        for q in range(QUARTERS):
            over_copy(0, y, q).start()
        fetches[1].wait()
        fetches[2].wait()

    inv_root = 1.0 / math.sqrt(HEAD_SIZE)
    key_line = lax.rem(iota((heads, positions), 1), HEAD_SIZE).astype(f32)

    def attend(sources):
        queries, extras, picks, limits = [], [], [], []
        for s in sources:
            queries.append(recv_rows[s])
            extra = recv_extra[s].astype(f32)
            extras.append(extra)
            picks.append(jnp.clip(jnp.max(extra[2:3]).astype(jnp.int32), 0, slots - 1))
            length = jnp.broadcast_to(extra[3:4], (heads, HEAD_SIZE))
            limits.append(
                jnp.concatenate(
                    [length - i * HEAD_SIZE for i in range(positions // HEAD_SIZE)], axis=1
                )
            )
        scores = [
            lax.dot_general(
                q, keys[p], (((1,), (1,)), ((), ())), preferred_element_type=f32
            )
            * inv_root
            for q, p in zip(queries, picks)
        ]
        owns = [
            jnp.sum(q.astype(f32) * extra[0:1], axis=1, keepdims=True) * inv_root
            for q, extra in zip(queries, extras)
        ]
        shown = [
            jnp.where(key_line < limit, score, masked_score)
            for score, limit in zip(scores, limits)
        ]
        tops = [
            jnp.maximum(jnp.max(score, axis=1, keepdims=True), own)
            for score, own in zip(shown, owns)
        ]
        weights = [
            jnp.where(key_line < limit, jnp.exp(score - top), 0.0)
            for score, limit, top in zip(shown, limits, tops)
        ]
        own_weights = [jnp.exp(own - top) for own, top in zip(owns, tops)]
        blends = [dot(weight.astype(bf16), values[p]) for weight, p in zip(weights, picks)]
        sums = [
            jnp.sum(weight, axis=1, keepdims=True) + own
            for weight, own in zip(weights, own_weights)
        ]
        for s, blend, own, extra, total in zip(sources, blends, own_weights, extras, sums):
            blended = blend + own.astype(bf16).astype(f32) * extra[1:2]
            home_send[s] = (blended / total).astype(bf16)

    with jax.named_scope("e_reqwait"):
        for copy in requests_in():
            copy.wait_recv()
    with jax.named_scope("f_attend"):
        attend([at(*back(offset)) for offset in near])
    with jax.named_scope("g_homesend"):
        for offset in reversed(near[1:]):
            home_copy(back(offset)).start()
        home_recv[me] = home_send[me]

    with jax.named_scope("j_relay"):
        up_copy(y, 3, 0).start()
        down_copy(y, 1, 0).start()
        for q in (0, 1):
            up_copy(y_down, q, 0).wait_recv()
            up_copy(y_down, q, 1).start()
            over_copy(1, y_down, q).start()
            down_copy(y_up, q + 2, 0).wait_recv()
            down_copy(y_up, q + 2, 1).start()
            over_copy(2, y_up, q + 2).start()
    with jax.named_scope("k_homewait"):
        homes_in().wait_recv()

    mine = lax.rem(z, 2)

    with jax.named_scope("l_compact"):
        chosen = dot(selector[...], home_recv[...].reshape(dp * heads, HEAD_SIZE))
        for h in range(heads):
            block[:, h * HEAD_SIZE : (h + 1) * HEAD_SIZE] = (
                chosen[h * rows : (h + 1) * rows] * factor[...]
            ).astype(bf16)

    homes = outer // 2
    middle = query_width // 2
    quarter = query_width // QUARTERS

    def place(source, home):
        return source * homes + lax.rem(home, outer) // 2

    def context_copy(k):
        return remote(
            block,
            contexts.at[place(core, z)],
            send_sem.at[4],
            context_recv.at[0],
            (at(k, 0), 2 * chip + mine),
        )

    def context_relay(source, k, half):
        spot = contexts.at[place(source, z + outer - k), :, pl.ds(half * middle, middle)]
        return remote(spot, spot, send_sem.at[4], context_recv.at[0], (at(k, 0), part))

    def contexts_in(k, count):
        blocks = contexts.at[pl.ds(0, count)]
        return remote(blocks, blocks, send_sem.at[4], context_recv.at[k], (me, other))

    with jax.named_scope("m_ctxsend"):
        for k in (4, 3, 5, 2, 6, 1, 7):
            context_copy(k).start()

        @pl.when(mine != core)
        def _():
            context_copy(0).start()

        @pl.when(mine == core)
        def _():
            contexts[place(core, z)] = block[...]

    with jax.named_scope("n_overs"):
        for q in (0, 1):
            up_copy(y_down, q + 2, 0).wait_recv()
            over_copy(1, y_down, q + 2).start()
            down_copy(y_up, q, 0).wait_recv()
            over_copy(2, y_up, q).start()

    with jax.named_scope("o_ctxwait"):

        @pl.when(mine == core)
        def _():
            contexts_in(0, 7).wait_recv()

        @pl.when(mine != core)
        def _():
            contexts_in(0, 2 * homes).wait_recv()

    shift = lax.rem(z + core, 2)

    def part_copy(n, column, i):
        target = lax.rem(z + 2 * i + shift, outer)
        return remote(
            send_part.at[column, target // 2],
            recv_part.at[column, chip],
            send_sem.at[5],
            part_recv.at[n],
            (target * inner + y, z),
        )

    def parts_in(n, count):
        parts = pl.ds(0, count)
        return remote(
            send_part.at[0, parts],
            recv_part.at[0, parts],
            send_sem.at[5],
            part_recv.at[n],
            (me, other),
        )

    order = (y, y_down, y_up, y_far)

    with jax.named_scope("p_project"):
        direct = contexts[pl.ds(core * homes, homes)].reshape(homes * rows, query_width)
        over = contexts[pl.ds((1 - core) * homes, homes)].reshape(homes * rows, query_width)
        for n, column in enumerate(order):
            if n == 3:
                for m in (0, 1):
                    up_copy(y_far, m, 1).wait_recv()
                    over_copy(3, y_far, m).start()
                    down_copy(y_far, m + 2, 1).wait_recv()
                    over_copy(3, y_far, m + 2).start()
            over_in(n, column).wait_recv()
            summed = jnp.zeros((homes * rows, columns), f32)
            for q in range(QUARTERS):
                depth = slice(q * quarter, (q + 1) * quarter)
                summed = summed + dot(direct[:, depth], weights_in[column, q])
                summed = summed + dot(over[:, depth], weights_over[column, q])
            send_part[column] = summed.astype(bf16).reshape(homes, rows, columns)
            for i in (2, 1, 3):
                part_copy(n, column, i).start()

            @pl.when(z != part)
            def _():
                part_copy(n, column, 0).start()

            @pl.when(z == part)
            def _():
                recv_part[column, chip] = send_part[column, z // 2]

    with jax.named_scope("q_drain"):
        for copy in requests_in():
            copy.wait_send()
        homes_in().wait_send()
        three = weights_in.at[pl.ds(0, inner - 1)]
        remote(three, three, send_sem.at[2], weight_recv.at[0, 0, 0], (me, other)).wait_send()
        remote(weights_in, weights_over, send_sem.at[3], over_recv.at[0], (me, other)).wait_send()

        @pl.when(mine == core)
        def _():
            contexts_in(0, 2 * homes - 1).wait_send()

        @pl.when(mine != core)
        def _():
            contexts_in(0, 2 * homes).wait_send()

    with jax.named_scope("r_partwait"):
        for n, column in enumerate(order):

            @pl.when(z != part)
            def _():
                parts_in(n, mp // 2).wait_recv()

            @pl.when(z == part)
            def _():
                parts_in(n, mp // 2 - 1).wait_recv()

            summed = recv_part[column, 0].astype(f32)
            for j in range(1, mp // 2):
                summed = summed + recv_part[column, j].astype(f32)
            start = pl.multiple_of(column * columns, columns)
            out_ref[:, pl.ds(start, columns)] = summed.astype(bf16)

    with jax.named_scope("s_drain"):

        @pl.when(z != part)
        def _():
            remote(send_part, send_part, send_sem.at[5], part_recv.at[0], (me, other)).wait_send()

        @pl.when(z == part)
        def _():
            most = send_part.at[:, pl.ds(0, mp // 2 - 1)]
            remote(most, most, send_sem.at[5], part_recv.at[0], (me, other)).wait_send()


def on_device(
    dp,
    mp,
    queries,
    incoming_key,
    incoming_value,
    key_cache,
    cached_values,
    task_key_scale,
    task_value_scale,
    out_weight,
    task_id,
    cached_length,
    task_owner,
    cache_slot,
):
    rows, query_width = queries.shape
    depth, columns = out_weight.shape
    heads = query_width // HEAD_SIZE
    inner = dp // mp
    small = (
        queries,
        incoming_key,
        incoming_value,
        task_key_scale,
        task_value_scale,
        task_id.reshape(1, -1),
        cached_length.reshape(1, -1),
        cache_slot.reshape(1, -1),
        task_owner.reshape(1, -1),
    )
    away = pl.BlockSpec(memory_space=pltpu.HBM)
    return pl.pallas_call(
        functools.partial(layer_kernel, dp, mp),
        out_shape=jax.ShapeDtypeStruct((rows, inner * columns), bf16),
        in_specs=[away] * 12,
        out_specs=pl.BlockSpec(memory_space=pltpu.VMEM),
        scratch_shapes=[pltpu.VMEM(array.shape, array.dtype) for array in small]
        + [
            pltpu.VMEM(key_cache.shape, bf16),
            pltpu.VMEM(cached_values.shape, bf16),
            pltpu.VMEM((inner, QUARTERS, depth // QUARTERS, columns), bf16),
            pltpu.VMEM((inner, QUARTERS, depth // QUARTERS, columns), bf16),
            pltpu.VMEM((dp, heads, HEAD_SIZE), bf16),
            pltpu.VMEM((dp, EXTRA, HEAD_SIZE), bf16),
            pltpu.VMEM((dp, heads, HEAD_SIZE), bf16),
            pltpu.VMEM((dp, EXTRA, HEAD_SIZE), bf16),
            pltpu.VMEM((dp, heads, HEAD_SIZE), bf16),
            pltpu.VMEM((dp, heads, HEAD_SIZE), bf16),
            pltpu.VMEM((heads * rows, dp * heads), bf16),
            pltpu.VMEM((rows, HEAD_SIZE), f32),
            pltpu.VMEM((mp, rows, query_width), bf16),
            pltpu.VMEM((rows, query_width), bf16),
            pltpu.VMEM((inner, mp // 2, rows, columns), bf16),
            pltpu.VMEM((inner, mp // 2, rows, columns), bf16),
            pltpu.SemaphoreType.DMA((3,)),
            pltpu.SemaphoreType.DMA((len(small),)),
            pltpu.SemaphoreType.DMA((7,)),
            pltpu.SemaphoreType.DMA((2,)),
            pltpu.SemaphoreType.DMA((1,)),
            pltpu.SemaphoreType.DMA((2, 2, QUARTERS)),
            pltpu.SemaphoreType.DMA((inner,)),
            pltpu.SemaphoreType.DMA((3,)),
            pltpu.SemaphoreType.DMA((inner,)),
        ],
        compiler_params=pltpu.CompilerParams(
            collective_id=0, has_side_effects=True, vmem_limit_bytes=20 * 1024 * 1024
        ),
    )(
        *[
            pltpu.with_memory_space_constraint(array, pltpu.HBM)
            for array in (
                *small,
                key_cache,
                cached_values,
                out_weight.reshape(QUARTERS, depth // QUARTERS, columns),
            )
        ]
    )


def solution(mesh):
    placed = (
        P("dp", "mp"),
        P("dp", "mp"),
        P("dp", "mp"),
        P("dp", None, "mp"),
        P("dp", None, "mp"),
        P(None, "mp"),
        P(None, "mp"),
        P("mp", "dp"),
        P("dp"),
        P("dp"),
        P(),
        P("dp"),
    )
    return jax.shard_map(
        functools.partial(on_device, mesh.shape["dp"], mesh.shape["mp"]),
        mesh=mesh,
        in_specs=placed,
        out_specs=P("dp", "mp"),
        check_vma=False,
    )
```

```python
import functools
import math

import jax
import jax.numpy as jnp
from jax import lax
from jax.experimental import pallas as pl
from jax.experimental.pallas import tpu as pltpu
from jax.sharding import PartitionSpec as P

HEAD_SIZE = 128
EXTRA = 4
QUARTERS = 4
MESH = pl.DeviceIdType.MESH

masked_score = -1e30
f32 = jnp.float32
bf16 = jnp.bfloat16


def iota(shape, dim):
    return lax.broadcasted_iota(jnp.int32, shape, dim)


def ring(k, n):
    return min(k, n - k)


def to_column(row):
    n = row.shape[1]
    eye = iota((n, n), 0) == iota((n, n), 1)
    return jnp.sum(jnp.where(eye, row, 0.0), axis=1, keepdims=True)


def to_row(column):
    n = column.shape[0]
    eye = iota((n, n), 0) == iota((n, n), 1)
    return jnp.sum(jnp.where(eye, column, 0.0), axis=0, keepdims=True)


def dot(a, b):
    return jnp.dot(a, b, preferred_element_type=f32)


def one_hot(mask):
    return jnp.where(mask, 1.0, 0.0).astype(bf16)


def layer_kernel(
    dp,
    mp,
    query_hbm,
    new_key_hbm,
    new_value_hbm,
    key_scale_hbm,
    value_scale_hbm,
    task_hbm,
    length_hbm,
    slot_hbm,
    owner_hbm,
    key_hbm,
    value_hbm,
    weight_hbm,
    out_ref,
    query_ref,
    new_key_ref,
    new_value_ref,
    key_scale_ref,
    value_scale_ref,
    task_ref,
    length_ref,
    slot_ref,
    owner_ref,
    keys,
    values,
    weights_in,
    weights_over,
    send_rows,
    send_extra,
    recv_rows,
    recv_extra,
    home_send,
    home_recv,
    selector,
    factor,
    contexts,
    block,
    partial,
    send_part,
    recv_part,
    local_sem,
    small_sem,
    send_sem,
    request_recv,
    home_recv_sem,
    weight_recv,
    over_recv,
    context_recv,
    part_recv,
):
    me = lax.axis_index("dp")
    part = lax.axis_index("mp")
    rows, query_width = query_ref.shape
    heads = query_width // HEAD_SIZE
    task_total = key_scale_ref.shape[0]
    slots, positions, _ = keys.shape
    columns = weights_in.shape[3]
    inner = dp // mp
    outer = mp
    z, y = me // inner, lax.rem(me, inner)
    chip, core = part // 2, lax.rem(part, 2)
    other = 2 * chip + 1 - core

    def at(kz, ky):
        return lax.rem(z + kz, outer) * inner + lax.rem(y + ky, inner)

    def distance(offset):
        return ring(offset[0], outer) + ring(offset[1], inner)

    def back(offset):
        return (outer - offset[0]) % outer, (inner - offset[1]) % inner

    near = sorted(((kz, ky) for kz in range(outer) for ky in range(inner)), key=distance)
    far = near[:0:-1]

    def remote(source, target, send_sem, recv_sem, device):
        return pltpu.make_async_remote_copy(
            src_ref=source,
            dst_ref=target,
            send_sem=send_sem,
            recv_sem=recv_sem,
            device_id=device,
            device_id_type=MESH,
        )

    def signal(sem, device):
        pl.semaphore_signal(sem, inc=1, device_id=device, device_id_type=MESH)

    up, down = at(0, 1), at(0, inner - 1)
    y_up, y_down, y_far = (lax.rem(y + k, inner) for k in (1, inner - 1, 2))

    def up_copy(source, q, relay):
        piece = weights_in.at[source, q]
        return remote(piece, piece, send_sem.at[2], weight_recv.at[relay, 0, q], (up, part))

    def down_copy(source, q, relay):
        piece = weights_in.at[source, q]
        return remote(piece, piece, send_sem.at[2], weight_recv.at[relay, 1, q], (down, part))

    def over_copy(k, source, q):
        return remote(
            weights_in.at[source, q],
            weights_over.at[source, q],
            send_sem.at[3],
            over_recv.at[k],
            (me, other),
        )

    def over_in(k, source):
        return remote(
            weights_in.at[source],
            weights_over.at[source],
            send_sem.at[3],
            over_recv.at[k],
            (me, other),
        )

    with jax.named_scope("a_greet"):
        small = [
            pltpu.make_async_copy(away, here, small_sem.at[i])
            for i, (away, here) in enumerate(
                (
                    (task_hbm, task_ref),
                    (owner_hbm, owner_ref),
                    (slot_hbm, slot_ref),
                    (length_hbm, length_ref),
                    (query_hbm, query_ref),
                    (key_scale_hbm, key_scale_ref),
                    (value_scale_hbm, value_scale_ref),
                    (new_key_hbm, new_key_ref),
                    (new_value_hbm, new_value_ref),
                )
            )
        ]
        for copy in small:
            copy.start()
        barrier = pltpu.get_barrier_semaphore()
        for kz, ky in far:
            signal(barrier, (at(kz, ky), part))
        for k in range(1, mp):
            signal(barrier, (me, lax.rem(part + k, mp)))
        fetches = [
            pltpu.make_async_copy(weight_hbm, weights_in.at[y], local_sem.at[2]),
            pltpu.make_async_copy(key_hbm, keys, local_sem.at[0]),
            pltpu.make_async_copy(value_hbm, values, local_sem.at[1]),
        ]
        for fetch in fetches:
            fetch.start()
    with jax.named_scope("a_first"):
        for copy in small:
            copy.wait()

    with jax.named_scope("b_pack"):
        task_column = to_column(task_ref[...].astype(f32))
        length_column = to_column(length_ref[...].astype(f32))
        slot_column = to_column(slot_ref[...].astype(f32))
        picked = task_column == iota((rows, task_total), 1).astype(f32)
        owner_column = jnp.sum(
            jnp.where(picked, owner_ref[...].astype(f32), 0.0), axis=1, keepdims=True
        )
        owner_row = to_row(owner_column)
        task_rows = one_hot(picked)
        key_factor = dot(task_rows, key_scale_ref[...])
        factor[...] = dot(task_rows, value_scale_ref[...])
        pieces = []
        for h in range(heads):
            lanes = slice(h * HEAD_SIZE, (h + 1) * HEAD_SIZE)
            pieces.append((query_ref[:, lanes].astype(f32) * key_factor).astype(bf16))
        pieces.append(new_key_ref[...])
        pieces.append(new_value_ref[...])
        pieces.append(jnp.broadcast_to(slot_column, (rows, HEAD_SIZE)).astype(bf16))
        pieces.append(jnp.broadcast_to(length_column, (rows, HEAD_SIZE)).astype(bf16))
        wide = len(pieces) * rows
        spread = one_hot(lax.rem(iota((rows, wide), 1), rows) == iota((rows, wide), 0))
        owner_wide = dot(owner_row.astype(bf16), spread)
        ready_rows = jnp.concatenate(pieces, axis=0)
        for into, first, count in ((send_rows, 0, heads), (send_extra, heads, EXTRA)):
            line = iota((dp * count, wide), 0)
            lane = iota((dp * count, wide), 1)
            packer = one_hot(
                (lax.rem(line, count) + first == lane // rows)
                & ((line // count).astype(f32) == owner_wide)
            )
            into[...] = dot(packer, ready_rows).astype(bf16).reshape(dp, count, HEAD_SIZE)
        line = iota((heads * rows, dp * heads), 0)
        lane = iota((heads * rows, dp * heads), 1)
        same = lax.rem(iota((heads * rows, rows), 0), rows) == iota((heads * rows, rows), 1)
        owner_tall = jnp.sum(jnp.where(same, owner_row, 0.0), axis=1, keepdims=True)
        selector[...] = one_hot(
            (line // rows == lax.rem(lane, heads)) & ((lane // heads).astype(f32) == owner_tall)
        )

    def request_copy(offset):
        return [
            remote(
                source.at[at(*offset)],
                target.at[me],
                send_sem.at[sem],
                request_recv.at[n],
                (at(*offset), part),
            )
            for n, (source, target, sem) in enumerate(
                ((send_rows, recv_rows, 0), (send_extra, recv_extra, 6))
            )
        ]

    def requests_in():
        pages = pl.ds(0, dp - 1)
        return [
            remote(
                source.at[pages],
                target.at[pages],
                send_sem.at[sem],
                request_recv.at[n],
                (me, other),
            )
            for n, (source, target, sem) in enumerate(
                ((send_rows, recv_rows, 0), (send_extra, recv_extra, 6))
            )
        ]

    def home_copy(offset):
        return remote(
            home_send.at[at(*offset)],
            home_recv.at[me],
            send_sem.at[1],
            home_recv_sem.at[0],
            (at(*offset), part),
        )

    def homes_in():
        pages = pl.ds(0, dp - 1)
        return remote(
            home_send.at[pages],
            home_recv.at[pages],
            send_sem.at[1],
            home_recv_sem.at[0],
            (me, other),
        )

    with jax.named_scope("c_barwait"):
        pl.semaphore_wait(barrier, dp + mp - 2)
    with jax.named_scope("d_reqsend"):
        for offset in far:
            for copy in request_copy(offset):
                copy.start()
        recv_rows[me] = send_rows[me]
        recv_extra[me] = send_extra[me]
        fetches[0].wait()
        up_copy(y, 0, 0).start()
        down_copy(y, 2, 0).start()
        up_copy(y, 1, 0).start()
        down_copy(y, 3, 0).start()
        up_copy(y, 2, 0).start()
        down_copy(y, 0, 0).start()
        for q in range(QUARTERS):
            over_copy(0, y, q).start()
        fetches[1].wait()
        fetches[2].wait()

    inv_root = 1.0 / math.sqrt(HEAD_SIZE)
    key_line = lax.rem(iota((heads, positions), 1), HEAD_SIZE).astype(f32)

    def attend(sources):
        queries, extras, picks, limits = [], [], [], []
        for s in sources:
            queries.append(recv_rows[s])
            extra = recv_extra[s].astype(f32)
            extras.append(extra)
            picks.append(jnp.clip(jnp.max(extra[2:3]).astype(jnp.int32), 0, slots - 1))
            length = jnp.broadcast_to(extra[3:4], (heads, HEAD_SIZE))
            limits.append(
                jnp.concatenate(
                    [length - i * HEAD_SIZE for i in range(positions // HEAD_SIZE)], axis=1
                )
            )
        scores = [
            lax.dot_general(
                q, keys[p], (((1,), (1,)), ((), ())), preferred_element_type=f32
            )
            * inv_root
            for q, p in zip(queries, picks)
        ]
        owns = [
            jnp.sum(q.astype(f32) * extra[0:1], axis=1, keepdims=True) * inv_root
            for q, extra in zip(queries, extras)
        ]
        shown = [
            jnp.where(key_line < limit, score, masked_score)
            for score, limit in zip(scores, limits)
        ]
        tops = [
            jnp.maximum(jnp.max(score, axis=1, keepdims=True), own)
            for score, own in zip(shown, owns)
        ]
        weights = [
            jnp.where(key_line < limit, jnp.exp(score - top), 0.0)
            for score, limit, top in zip(shown, limits, tops)
        ]
        own_weights = [jnp.exp(own - top) for own, top in zip(owns, tops)]
        blends = [dot(weight.astype(bf16), values[p]) for weight, p in zip(weights, picks)]
        sums = [
            jnp.sum(weight, axis=1, keepdims=True) + own
            for weight, own in zip(weights, own_weights)
        ]
        for s, blend, own, extra, total in zip(sources, blends, own_weights, extras, sums):
            blended = blend + own.astype(bf16).astype(f32) * extra[1:2]
            home_send[s] = (blended / total).astype(bf16)

    with jax.named_scope("e_reqwait"):
        for copy in requests_in():
            copy.wait_recv()
    for group in (near[-12:], near[:-12]):
        with jax.named_scope("f_attend"):
            attend([at(*back(offset)) for offset in group])
        with jax.named_scope("g_homesend"):
            for offset in reversed(group):
                if offset != (0, 0):
                    home_copy(back(offset)).start()
    home_recv[me] = home_send[me]

    with jax.named_scope("j_relay"):
        up_copy(y, 3, 0).start()
        down_copy(y, 1, 0).start()
        for q in (0, 1):
            up_copy(y_down, q, 0).wait_recv()
            up_copy(y_down, q, 1).start()
            over_copy(1, y_down, q).start()
            down_copy(y_up, q + 2, 0).wait_recv()
            down_copy(y_up, q + 2, 1).start()
            over_copy(2, y_up, q + 2).start()
    with jax.named_scope("k_homewait"):
        homes_in().wait_recv()

    mine = lax.rem(z, 2)

    with jax.named_scope("l_compact"):
        chosen = dot(selector[...], home_recv[...].reshape(dp * heads, HEAD_SIZE))
        for h in range(heads):
            block[:, h * HEAD_SIZE : (h + 1) * HEAD_SIZE] = (
                chosen[h * rows : (h + 1) * rows] * factor[...]
            ).astype(bf16)

    homes = outer // 2
    middle = query_width // 2
    quarter = query_width // QUARTERS

    def place(source, home):
        return source * homes + lax.rem(home, outer) // 2

    def half_of(ref, half):
        return ref.at[..., pl.ds(half * middle, middle)]

    def context_copy(k, half):
        return remote(
            half_of(block, half),
            half_of(contexts.at[place(core, z)], half),
            send_sem.at[4],
            context_recv.at[half],
            (at(k, 0), 2 * chip + mine),
        )

    def contexts_in(half, count):
        blocks = half_of(contexts.at[pl.ds(0, count)], half)
        return remote(blocks, blocks, send_sem.at[4], context_recv.at[half], (me, other))

    def contexts_out(count):
        blocks = contexts.at[pl.ds(0, count)]
        return remote(blocks, blocks, send_sem.at[4], context_recv.at[0], (me, other))

    with jax.named_scope("m_ctxsend"):
        for half in range(2):
            for k in (4, 3, 5, 2, 6, 1, 7):
                context_copy(k, half).start()

            @pl.when(mine != core)
            def _():
                context_copy(0, half).start()

        @pl.when(mine == core)
        def _():
            contexts[place(core, z)] = block[...]

    with jax.named_scope("n_overs"):
        for q in (0, 1):
            up_copy(y_down, q + 2, 0).wait_recv()
            over_copy(1, y_down, q + 2).start()
            down_copy(y_up, q, 0).wait_recv()
            over_copy(2, y_up, q).start()

    def context_wait(half):
        @pl.when(mine == core)
        def _():
            contexts_in(half, 2 * homes - 1).wait_recv()

        @pl.when(mine != core)
        def _():
            contexts_in(half, 2 * homes).wait_recv()

    shift = lax.rem(z + core, 2)

    def part_copy(n, column, i):
        target = lax.rem(z + 2 * i + shift, outer)
        return remote(
            send_part.at[column, target // 2],
            recv_part.at[column, chip],
            send_sem.at[5],
            part_recv.at[n],
            (target * inner + y, z),
        )

    def parts_in(n, count):
        parts = pl.ds(0, count)
        return remote(
            send_part.at[0, parts],
            recv_part.at[0, parts],
            send_sem.at[5],
            part_recv.at[n],
            (me, other),
        )

    order = (y, y_down, y_up, y_far)

    def half_sum(column, half):
        total = jnp.zeros((homes * rows, columns), f32)
        for q in range(half * QUARTERS // 2, (half + 1) * QUARTERS // 2):
            lanes = slice(q * quarter, (q + 1) * quarter)
            for source, weight in ((core, weights_in), (1 - core, weights_over)):
                piece = contexts[pl.ds(source * homes, homes), :, lanes]
                total = total + dot(
                    piece.reshape(homes * rows, quarter), weight[column, q]
                )
        return total

    def far_sum(column):
        total = jnp.zeros((homes * rows, columns), f32)
        for source, weight in ((core, weights_in), (1 - core, weights_over)):
            if weight is weights_over:
                over_in(inner - 1, column).wait_recv()
            for q in range(QUARTERS):
                piece = contexts[
                    pl.ds(source * homes, homes), :, q * quarter : (q + 1) * quarter
                ]
                total = total + dot(
                    piece.reshape(homes * rows, quarter), weight[column, q]
                )
        return total

    with jax.named_scope("o_ctxwait"):
        context_wait(0)
    with jax.named_scope("o_first"):
        for n, column in enumerate(order[:-1]):
            over_in(n, column).wait_recv()
            partial[n] = half_sum(column, 0)
    with jax.named_scope("o_ctxwait2"):
        context_wait(1)
    with jax.named_scope("p_project"):
        for n, column in enumerate(order):
            if n == 2:
                for m in (0, 1):
                    up_copy(y_far, m, 1).wait_recv()
                    over_copy(3, y_far, m).start()
                    down_copy(y_far, m + 2, 1).wait_recv()
                    over_copy(3, y_far, m + 2).start()
            if n < inner - 1:
                summed = partial[n] + half_sum(column, 1)
            else:
                summed = far_sum(column)
            send_part[column] = summed.astype(bf16).reshape(homes, rows, columns)
            for i in (2, 1, 3):
                part_copy(n, column, i).start()

            @pl.when(z != part)
            def _():
                part_copy(n, column, 0).start()

            @pl.when(z == part)
            def _():
                recv_part[column, chip] = send_part[column, z // 2]

    with jax.named_scope("q_drain"):
        for copy in requests_in():
            copy.wait_send()
        homes_in().wait_send()
        three = weights_in.at[pl.ds(0, inner - 1)]
        remote(three, three, send_sem.at[2], weight_recv.at[0, 0, 0], (me, other)).wait_send()
        remote(weights_in, weights_over, send_sem.at[3], over_recv.at[0], (me, other)).wait_send()

        @pl.when(mine == core)
        def _():
            contexts_out(2 * homes - 1).wait_send()

        @pl.when(mine != core)
        def _():
            contexts_out(2 * homes).wait_send()

    with jax.named_scope("r_partwait"):
        for n, column in enumerate(order):

            @pl.when(z != part)
            def _():
                parts_in(n, mp // 2).wait_recv()

            @pl.when(z == part)
            def _():
                parts_in(n, mp // 2 - 1).wait_recv()

            summed = recv_part[column, 0].astype(f32)
            for j in range(1, mp // 2):
                summed = summed + recv_part[column, j].astype(f32)
            start = pl.multiple_of(column * columns, columns)
            out_ref[:, pl.ds(start, columns)] = summed.astype(bf16)

    with jax.named_scope("s_drain"):

        @pl.when(z != part)
        def _():
            remote(send_part, send_part, send_sem.at[5], part_recv.at[0], (me, other)).wait_send()

        @pl.when(z == part)
        def _():
            most = send_part.at[:, pl.ds(0, mp // 2 - 1)]
            remote(most, most, send_sem.at[5], part_recv.at[0], (me, other)).wait_send()


def on_device(
    dp,
    mp,
    queries,
    incoming_key,
    incoming_value,
    key_cache,
    cached_values,
    task_key_scale,
    task_value_scale,
    out_weight,
    task_id,
    cached_length,
    task_owner,
    cache_slot,
):
    rows, query_width = queries.shape
    depth, columns = out_weight.shape
    heads = query_width // HEAD_SIZE
    inner = dp // mp
    small = (
        queries,
        incoming_key,
        incoming_value,
        task_key_scale,
        task_value_scale,
        task_id.reshape(1, -1),
        cached_length.reshape(1, -1),
        cache_slot.reshape(1, -1),
        task_owner.reshape(1, -1),
    )
    away = pl.BlockSpec(memory_space=pltpu.HBM)
    return pl.pallas_call(
        functools.partial(layer_kernel, dp, mp),
        out_shape=jax.ShapeDtypeStruct((rows, inner * columns), bf16),
        in_specs=[away] * 12,
        out_specs=pl.BlockSpec(memory_space=pltpu.VMEM),
        scratch_shapes=[pltpu.VMEM(array.shape, array.dtype) for array in small]
        + [
            pltpu.VMEM(key_cache.shape, bf16),
            pltpu.VMEM(cached_values.shape, bf16),
            pltpu.VMEM((inner, QUARTERS, depth // QUARTERS, columns), bf16),
            pltpu.VMEM((inner, QUARTERS, depth // QUARTERS, columns), bf16),
            pltpu.VMEM((dp, heads, HEAD_SIZE), bf16),
            pltpu.VMEM((dp, EXTRA, HEAD_SIZE), bf16),
            pltpu.VMEM((dp, heads, HEAD_SIZE), bf16),
            pltpu.VMEM((dp, EXTRA, HEAD_SIZE), bf16),
            pltpu.VMEM((dp, heads, HEAD_SIZE), bf16),
            pltpu.VMEM((dp, heads, HEAD_SIZE), bf16),
            pltpu.VMEM((heads * rows, dp * heads), bf16),
            pltpu.VMEM((rows, HEAD_SIZE), f32),
            pltpu.VMEM((mp, rows, query_width), bf16),
            pltpu.VMEM((rows, query_width), bf16),
            pltpu.VMEM((inner - 1, mp // 2 * rows, columns), f32),
            pltpu.VMEM((inner, mp // 2, rows, columns), bf16),
            pltpu.VMEM((inner, mp // 2, rows, columns), bf16),
            pltpu.SemaphoreType.DMA((3,)),
            pltpu.SemaphoreType.DMA((len(small),)),
            pltpu.SemaphoreType.DMA((7,)),
            pltpu.SemaphoreType.DMA((2,)),
            pltpu.SemaphoreType.DMA((1,)),
            pltpu.SemaphoreType.DMA((2, 2, QUARTERS)),
            pltpu.SemaphoreType.DMA((inner,)),
            pltpu.SemaphoreType.DMA((3,)),
            pltpu.SemaphoreType.DMA((inner,)),
        ],
        compiler_params=pltpu.CompilerParams(
            collective_id=0, has_side_effects=True, vmem_limit_bytes=20 * 1024 * 1024
        ),
    )(
        *[
            pltpu.with_memory_space_constraint(array, pltpu.HBM)
            for array in (
                *small,
                key_cache,
                cached_values,
                out_weight.reshape(QUARTERS, depth // QUARTERS, columns),
            )
        ]
    )


def solution(mesh):
    placed = (
        P("dp", "mp"),
        P("dp", "mp"),
        P("dp", "mp"),
        P("dp", None, "mp"),
        P("dp", None, "mp"),
        P(None, "mp"),
        P(None, "mp"),
        P("mp", "dp"),
        P("dp"),
        P("dp"),
        P(),
        P("dp"),
    )
    return jax.shard_map(
        functools.partial(on_device, mesh.shape["dp"], mesh.shape["mp"]),
        mesh=mesh,
        in_specs=placed,
        out_specs=P("dp", "mp"),
        check_vma=False,
    )
```

```python
import functools
import math

import jax
import jax.numpy as jnp
from jax import lax
from jax.experimental import pallas as pl
from jax.experimental.pallas import tpu as pltpu
from jax.sharding import PartitionSpec as P

HEAD_SIZE = 128
EXTRA = 4
QUARTERS = 4
MESH = pl.DeviceIdType.MESH

masked_score = -1e30
f32 = jnp.float32
bf16 = jnp.bfloat16


def iota(shape, dim):
    return lax.broadcasted_iota(jnp.int32, shape, dim)


def ring(k, n):
    return min(k, n - k)


def to_column(row):
    n = row.shape[1]
    eye = iota((n, n), 0) == iota((n, n), 1)
    return jnp.sum(jnp.where(eye, row, 0.0), axis=1, keepdims=True)


def to_row(column):
    n = column.shape[0]
    eye = iota((n, n), 0) == iota((n, n), 1)
    return jnp.sum(jnp.where(eye, column, 0.0), axis=0, keepdims=True)


def dot(a, b):
    return jnp.dot(a, b, preferred_element_type=f32)


def one_hot(mask):
    return jnp.where(mask, 1.0, 0.0).astype(bf16)


def layer_kernel(
    dp,
    mp,
    query_hbm,
    new_key_hbm,
    new_value_hbm,
    key_scale_hbm,
    value_scale_hbm,
    task_hbm,
    length_hbm,
    slot_hbm,
    owner_hbm,
    key_hbm,
    value_hbm,
    weight_hbm,
    out_ref,
    query_ref,
    new_key_ref,
    new_value_ref,
    key_scale_ref,
    value_scale_ref,
    task_ref,
    length_ref,
    slot_ref,
    owner_ref,
    keys,
    values,
    weights_in,
    weights_over,
    send_rows,
    send_extra,
    recv_rows,
    recv_extra,
    home_send,
    home_recv,
    selector,
    factor,
    contexts,
    block,
    partial,
    send_part,
    recv_part,
    local_sem,
    small_sem,
    send_sem,
    request_recv,
    home_recv_sem,
    weight_recv,
    over_recv,
    context_recv,
    part_recv,
):
    me = lax.axis_index("dp")
    part = lax.axis_index("mp")
    rows, query_width = query_ref.shape
    heads = query_width // HEAD_SIZE
    task_total = key_scale_ref.shape[0]
    slots, positions, _ = keys.shape
    columns = weights_in.shape[3]
    inner = dp // mp
    outer = mp
    z, y = me // inner, lax.rem(me, inner)
    chip, core = part // 2, lax.rem(part, 2)
    other = 2 * chip + 1 - core

    def at(kz, ky):
        return lax.rem(z + kz, outer) * inner + lax.rem(y + ky, inner)

    def distance(offset):
        return ring(offset[0], outer) + ring(offset[1], inner)

    def back(offset):
        return (outer - offset[0]) % outer, (inner - offset[1]) % inner

    near = sorted(((kz, ky) for kz in range(outer) for ky in range(inner)), key=distance)
    far = near[:0:-1]

    def remote(source, target, send_sem, recv_sem, device):
        return pltpu.make_async_remote_copy(
            src_ref=source,
            dst_ref=target,
            send_sem=send_sem,
            recv_sem=recv_sem,
            device_id=device,
            device_id_type=MESH,
        )

    def signal(sem, device):
        pl.semaphore_signal(sem, inc=1, device_id=device, device_id_type=MESH)

    up, down = at(0, 1), at(0, inner - 1)
    y_up, y_down, y_far = (lax.rem(y + k, inner) for k in (1, inner - 1, 2))

    def up_copy(source, q, relay):
        piece = weights_in.at[source, q]
        return remote(piece, piece, send_sem.at[2], weight_recv.at[q + 4 * relay], (up, part))

    def down_copy(source, q, relay):
        piece = weights_in.at[source, q]
        return remote(piece, piece, send_sem.at[2], weight_recv.at[6 + q + 2 * relay], (down, part))

    def over_copy(k, source, q):
        return remote(
            weights_in.at[source, q],
            weights_over.at[source, q],
            send_sem.at[3],
            over_recv.at[k],
            (me, other),
        )

    def over_in(k, source):
        return remote(
            weights_in.at[source],
            weights_over.at[source],
            send_sem.at[3],
            over_recv.at[k],
            (me, other),
        )

    with jax.named_scope("a_greet"):
        small = [
            pltpu.make_async_copy(away, here, small_sem.at[i])
            for i, (away, here) in enumerate(
                (
                    (task_hbm, task_ref),
                    (owner_hbm, owner_ref),
                    (slot_hbm, slot_ref),
                    (length_hbm, length_ref),
                    (query_hbm, query_ref),
                    (key_scale_hbm, key_scale_ref),
                    (value_scale_hbm, value_scale_ref),
                    (new_key_hbm, new_key_ref),
                    (new_value_hbm, new_value_ref),
                )
            )
        ]
        for copy in small:
            copy.start()
        barrier = pltpu.get_barrier_semaphore()
        for kz, ky in far:
            signal(barrier, (at(kz, ky), part))
        for k in range(1, mp):
            signal(barrier, (me, lax.rem(part + k, mp)))
        fetches = [
            pltpu.make_async_copy(weight_hbm, weights_in.at[y], local_sem.at[2]),
            pltpu.make_async_copy(key_hbm, keys, local_sem.at[0]),
            pltpu.make_async_copy(value_hbm, values, local_sem.at[1]),
        ]
        for fetch in fetches:
            fetch.start()
    with jax.named_scope("a_first"):
        for copy in small:
            copy.wait()

    with jax.named_scope("b_pack"):
        task_column = to_column(task_ref[...].astype(f32))
        length_column = to_column(length_ref[...].astype(f32))
        slot_column = to_column(slot_ref[...].astype(f32))
        picked = task_column == iota((rows, task_total), 1).astype(f32)
        owner_column = jnp.sum(
            jnp.where(picked, owner_ref[...].astype(f32), 0.0), axis=1, keepdims=True
        )
        owner_row = to_row(owner_column)
        task_rows = one_hot(picked)
        key_factor = dot(task_rows, key_scale_ref[...])
        factor[...] = dot(task_rows, value_scale_ref[...])
        pieces = []
        for h in range(heads):
            lanes = slice(h * HEAD_SIZE, (h + 1) * HEAD_SIZE)
            pieces.append((query_ref[:, lanes].astype(f32) * key_factor).astype(bf16))
        pieces.append(new_key_ref[...])
        pieces.append(new_value_ref[...])
        pieces.append(jnp.broadcast_to(slot_column, (rows, HEAD_SIZE)).astype(bf16))
        pieces.append(jnp.broadcast_to(length_column, (rows, HEAD_SIZE)).astype(bf16))
        wide = len(pieces) * rows
        spread = one_hot(lax.rem(iota((rows, wide), 1), rows) == iota((rows, wide), 0))
        owner_wide = dot(owner_row.astype(bf16), spread)
        ready_rows = jnp.concatenate(pieces, axis=0)
        for into, first, count in ((send_rows, 0, heads), (send_extra, heads, EXTRA)):
            line = iota((dp * count, wide), 0)
            lane = iota((dp * count, wide), 1)
            packer = one_hot(
                (lax.rem(line, count) + first == lane // rows)
                & ((line // count).astype(f32) == owner_wide)
            )
            into[...] = dot(packer, ready_rows).astype(bf16).reshape(dp, count, HEAD_SIZE)
        line = iota((heads * rows, dp * heads), 0)
        lane = iota((heads * rows, dp * heads), 1)
        same = lax.rem(iota((heads * rows, rows), 0), rows) == iota((heads * rows, rows), 1)
        owner_tall = jnp.sum(jnp.where(same, owner_row, 0.0), axis=1, keepdims=True)
        selector[...] = one_hot(
            (line // rows == lax.rem(lane, heads)) & ((lane // heads).astype(f32) == owner_tall)
        )

    def request_copy(offset):
        return [
            remote(
                source.at[at(*offset)],
                target.at[me],
                send_sem.at[sem],
                request_recv.at[n],
                (at(*offset), part),
            )
            for n, (source, target, sem) in enumerate(
                ((send_rows, recv_rows, 0), (send_extra, recv_extra, 6))
            )
        ]

    def requests_in():
        pages = pl.ds(0, dp - 1)
        return [
            remote(
                source.at[pages],
                target.at[pages],
                send_sem.at[sem],
                request_recv.at[n],
                (me, other),
            )
            for n, (source, target, sem) in enumerate(
                ((send_rows, recv_rows, 0), (send_extra, recv_extra, 6))
            )
        ]

    def home_copy(offset):
        return remote(
            home_send.at[at(*offset)],
            home_recv.at[me],
            send_sem.at[1],
            home_recv_sem.at[0],
            (at(*offset), part),
        )

    def homes_in():
        pages = pl.ds(0, dp - 1)
        return remote(
            home_send.at[pages],
            home_recv.at[pages],
            send_sem.at[1],
            home_recv_sem.at[0],
            (me, other),
        )

    with jax.named_scope("c_barwait"):
        pl.semaphore_wait(barrier, dp + mp - 2)
    with jax.named_scope("d_reqsend"):
        for offset in far:
            for copy in request_copy(offset):
                copy.start()
        recv_rows[me] = send_rows[me]
        recv_extra[me] = send_extra[me]
        fetches[0].wait()
        up_copy(y, 0, 0).start()
        down_copy(y, 2, 0).start()
        up_copy(y, 1, 0).start()
        down_copy(y, 3, 0).start()
        for q in range(QUARTERS):
            over_copy(0, y, q).start()
        fetches[1].wait()
        fetches[2].wait()

    inv_root = 1.0 / math.sqrt(HEAD_SIZE)
    key_line = lax.rem(iota((heads, positions), 1), HEAD_SIZE).astype(f32)

    def attend(sources):
        queries, extras, picks, limits = [], [], [], []
        for s in sources:
            queries.append(recv_rows[s])
            extra = recv_extra[s].astype(f32)
            extras.append(extra)
            picks.append(jnp.clip(jnp.max(extra[2:3]).astype(jnp.int32), 0, slots - 1))
            length = jnp.broadcast_to(extra[3:4], (heads, HEAD_SIZE))
            limits.append(
                jnp.concatenate(
                    [length - i * HEAD_SIZE for i in range(positions // HEAD_SIZE)], axis=1
                )
            )
        scores = [
            lax.dot_general(
                q, keys[p], (((1,), (1,)), ((), ())), preferred_element_type=f32
            )
            * inv_root
            for q, p in zip(queries, picks)
        ]
        owns = [
            jnp.sum(q.astype(f32) * extra[0:1], axis=1, keepdims=True) * inv_root
            for q, extra in zip(queries, extras)
        ]
        shown = [
            jnp.where(key_line < limit, score, masked_score)
            for score, limit in zip(scores, limits)
        ]
        tops = [
            jnp.maximum(jnp.max(score, axis=1, keepdims=True), own)
            for score, own in zip(shown, owns)
        ]
        weights = [
            jnp.where(key_line < limit, jnp.exp(score - top), 0.0)
            for score, limit, top in zip(shown, limits, tops)
        ]
        own_weights = [jnp.exp(own - top) for own, top in zip(owns, tops)]
        blends = [dot(weight.astype(bf16), values[p]) for weight, p in zip(weights, picks)]
        sums = [
            jnp.sum(weight, axis=1, keepdims=True) + own
            for weight, own in zip(weights, own_weights)
        ]
        for s, blend, own, extra, total in zip(sources, blends, own_weights, extras, sums):
            blended = blend + own.astype(bf16).astype(f32) * extra[1:2]
            home_send[s] = (blended / total).astype(bf16)

    with jax.named_scope("e_reqwait"):
        for copy in requests_in():
            copy.wait_recv()
    for group in (near[-12:], near[:-12]):
        with jax.named_scope("f_attend"):
            attend([at(*back(offset)) for offset in group])
        with jax.named_scope("g_homesend"):
            for offset in reversed(group):
                if offset != (0, 0):
                    home_copy(back(offset)).start()
    home_recv[me] = home_send[me]

    with jax.named_scope("j_relay"):
        up_copy(y, 2, 0).start()
        down_copy(y, 0, 0).start()
        up_copy(y, 3, 0).start()
        down_copy(y, 1, 0).start()
        for q in (0, 1):
            up_copy(y_down, q, 0).wait_recv()
            up_copy(y_down, q, 1).start()
            over_copy(1, y_down, q).start()
            down_copy(y_up, q + 2, 0).wait_recv()
            down_copy(y_up, q + 2, 1).start()
            over_copy(2, y_up, q + 2).start()
    with jax.named_scope("k_homewait"):
        homes_in().wait_recv()

    mine = lax.rem(z, 2)

    with jax.named_scope("l_compact"):
        chosen = dot(selector[...], home_recv[...].reshape(dp * heads, HEAD_SIZE))
        for h in range(heads):
            block[:, h * HEAD_SIZE : (h + 1) * HEAD_SIZE] = (
                chosen[h * rows : (h + 1) * rows] * factor[...]
            ).astype(bf16)

    homes = outer // 2
    middle = query_width // 2
    quarter = query_width // QUARTERS

    def place(source, home):
        return source * homes + lax.rem(home, outer) // 2

    def half_of(ref, half):
        return ref.at[..., pl.ds(half * middle, middle)]

    def context_copy(k, half):
        return remote(
            half_of(block, half),
            half_of(contexts.at[place(core, z)], half),
            send_sem.at[4],
            context_recv.at[half],
            (at(k, 0), 2 * chip + mine),
        )

    def contexts_in(half, count):
        blocks = half_of(contexts.at[pl.ds(0, count)], half)
        return remote(blocks, blocks, send_sem.at[4], context_recv.at[half], (me, other))

    def contexts_out(count):
        blocks = contexts.at[pl.ds(0, count)]
        return remote(blocks, blocks, send_sem.at[4], context_recv.at[0], (me, other))

    with jax.named_scope("m_ctxsend"):
        for half in range(2):
            for k in (4, 3, 5, 2, 6, 1, 7):
                context_copy(k, half).start()

            @pl.when(mine != core)
            def _():
                context_copy(0, half).start()

        @pl.when(mine == core)
        def _():
            contexts[place(core, z)] = block[...]

    with jax.named_scope("n_overs"):
        for q in (0, 1):
            up_copy(y_down, q + 2, 0).wait_recv()
            over_copy(1, y_down, q + 2).start()
            down_copy(y_up, q, 0).wait_recv()
            over_copy(2, y_up, q).start()

    def context_wait(half):
        @pl.when(mine == core)
        def _():
            contexts_in(half, 2 * homes - 1).wait_recv()

        @pl.when(mine != core)
        def _():
            contexts_in(half, 2 * homes).wait_recv()

    shift = lax.rem(z + core, 2)

    def part_copy(n, column, i):
        target = lax.rem(z + 2 * i + shift, outer)
        return remote(
            send_part.at[column, target // 2],
            recv_part.at[column, chip],
            send_sem.at[5],
            part_recv.at[n],
            (target * inner + y, z),
        )

    def parts_in(n, count):
        parts = pl.ds(0, count)
        return remote(
            send_part.at[0, parts],
            recv_part.at[0, parts],
            send_sem.at[5],
            part_recv.at[n],
            (me, other),
        )

    order = (y, y_down, y_up, y_far)

    def half_sum(column, half):
        total = jnp.zeros((homes * rows, columns), f32)
        for q in range(half * QUARTERS // 2, (half + 1) * QUARTERS // 2):
            lanes = slice(q * quarter, (q + 1) * quarter)
            for source, weight in ((core, weights_in), (1 - core, weights_over)):
                piece = contexts[pl.ds(source * homes, homes), :, lanes]
                total = total + dot(
                    piece.reshape(homes * rows, quarter), weight[column, q]
                )
        return total

    def far_sum(column):
        total = jnp.zeros((homes * rows, columns), f32)
        for source, weight in ((core, weights_in), (1 - core, weights_over)):
            if weight is weights_over:
                over_in(inner - 1, column).wait_recv()
            for q in range(QUARTERS):
                piece = contexts[
                    pl.ds(source * homes, homes), :, q * quarter : (q + 1) * quarter
                ]
                total = total + dot(
                    piece.reshape(homes * rows, quarter), weight[column, q]
                )
        return total

    with jax.named_scope("o_ctxwait"):
        context_wait(0)
    with jax.named_scope("o_first"):
        for n, column in enumerate(order[:-1]):
            over_in(n, column).wait_recv()
            partial[n] = half_sum(column, 0)
    with jax.named_scope("o_ctxwait2"):
        context_wait(1)
    with jax.named_scope("p_project"):
        for n, column in enumerate(order):
            if n == 3:
                for m in (0, 1):
                    up_copy(y_far, m, 1).wait_recv()
                    over_copy(3, y_far, m).start()
                    down_copy(y_far, m + 2, 1).wait_recv()
                    over_copy(3, y_far, m + 2).start()
            if n < inner - 1:
                summed = partial[n] + half_sum(column, 1)
            else:
                summed = far_sum(column)
            send_part[column] = summed.astype(bf16).reshape(homes, rows, columns)
            for i in (2, 1, 3):
                part_copy(n, column, i).start()

            @pl.when(z != part)
            def _():
                part_copy(n, column, 0).start()

            @pl.when(z == part)
            def _():
                recv_part[column, chip] = send_part[column, z // 2]

    with jax.named_scope("q_drain"):
        for copy in requests_in():
            copy.wait_send()
        homes_in().wait_send()
        three = weights_in.at[pl.ds(0, inner - 1)]
        remote(three, three, send_sem.at[2], weight_recv.at[0], (me, other)).wait_send()
        remote(weights_in, weights_over, send_sem.at[3], over_recv.at[0], (me, other)).wait_send()

        @pl.when(mine == core)
        def _():
            contexts_out(2 * homes - 1).wait_send()

        @pl.when(mine != core)
        def _():
            contexts_out(2 * homes).wait_send()

    with jax.named_scope("r_partwait"):
        for n, column in enumerate(order):

            @pl.when(z != part)
            def _():
                parts_in(n, mp // 2).wait_recv()

            @pl.when(z == part)
            def _():
                parts_in(n, mp // 2 - 1).wait_recv()

            summed = recv_part[column, 0].astype(f32)
            for j in range(1, mp // 2):
                summed = summed + recv_part[column, j].astype(f32)
            start = pl.multiple_of(column * columns, columns)
            out_ref[:, pl.ds(start, columns)] = summed.astype(bf16)

    with jax.named_scope("s_drain"):

        @pl.when(z != part)
        def _():
            remote(send_part, send_part, send_sem.at[5], part_recv.at[0], (me, other)).wait_send()

        @pl.when(z == part)
        def _():
            most = send_part.at[:, pl.ds(0, mp // 2 - 1)]
            remote(most, most, send_sem.at[5], part_recv.at[0], (me, other)).wait_send()


def on_device(
    dp,
    mp,
    queries,
    incoming_key,
    incoming_value,
    key_cache,
    cached_values,
    task_key_scale,
    task_value_scale,
    out_weight,
    task_id,
    cached_length,
    task_owner,
    cache_slot,
):
    rows, query_width = queries.shape
    depth, columns = out_weight.shape
    heads = query_width // HEAD_SIZE
    inner = dp // mp
    small = (
        queries,
        incoming_key,
        incoming_value,
        task_key_scale,
        task_value_scale,
        task_id.reshape(1, -1),
        cached_length.reshape(1, -1),
        cache_slot.reshape(1, -1),
        task_owner.reshape(1, -1),
    )
    away = pl.BlockSpec(memory_space=pltpu.HBM)
    return pl.pallas_call(
        functools.partial(layer_kernel, dp, mp),
        out_shape=jax.ShapeDtypeStruct((rows, inner * columns), bf16),
        in_specs=[away] * 12,
        out_specs=pl.BlockSpec(memory_space=pltpu.VMEM),
        scratch_shapes=[pltpu.VMEM(array.shape, array.dtype) for array in small]
        + [
            pltpu.VMEM(key_cache.shape, bf16),
            pltpu.VMEM(cached_values.shape, bf16),
            pltpu.VMEM((inner, QUARTERS, depth // QUARTERS, columns), bf16),
            pltpu.VMEM((inner, QUARTERS, depth // QUARTERS, columns), bf16),
            pltpu.VMEM((dp, heads, HEAD_SIZE), bf16),
            pltpu.VMEM((dp, EXTRA, HEAD_SIZE), bf16),
            pltpu.VMEM((dp, heads, HEAD_SIZE), bf16),
            pltpu.VMEM((dp, EXTRA, HEAD_SIZE), bf16),
            pltpu.VMEM((dp, heads, HEAD_SIZE), bf16),
            pltpu.VMEM((dp, heads, HEAD_SIZE), bf16),
            pltpu.VMEM((heads * rows, dp * heads), bf16),
            pltpu.VMEM((rows, HEAD_SIZE), f32),
            pltpu.VMEM((mp, rows, query_width), bf16),
            pltpu.VMEM((rows, query_width), bf16),
            pltpu.VMEM((inner - 1, mp // 2 * rows, columns), f32),
            pltpu.VMEM((inner, mp // 2, rows, columns), bf16),
            pltpu.VMEM((inner, mp // 2, rows, columns), bf16),
            pltpu.SemaphoreType.DMA((3,)),
            pltpu.SemaphoreType.DMA((len(small),)),
            pltpu.SemaphoreType.DMA((7,)),
            pltpu.SemaphoreType.DMA((2,)),
            pltpu.SemaphoreType.DMA((1,)),
            pltpu.SemaphoreType.DMA((12,)),
            pltpu.SemaphoreType.DMA((inner,)),
            pltpu.SemaphoreType.DMA((3,)),
            pltpu.SemaphoreType.DMA((inner,)),
        ],
        compiler_params=pltpu.CompilerParams(
            collective_id=0, has_side_effects=True, vmem_limit_bytes=20 * 1024 * 1024
        ),
    )(
        *[
            pltpu.with_memory_space_constraint(array, pltpu.HBM)
            for array in (
                *small,
                key_cache,
                cached_values,
                out_weight.reshape(QUARTERS, depth // QUARTERS, columns),
            )
        ]
    )


def solution(mesh):
    placed = (
        P("dp", "mp"),
        P("dp", "mp"),
        P("dp", "mp"),
        P("dp", None, "mp"),
        P("dp", None, "mp"),
        P(None, "mp"),
        P(None, "mp"),
        P("mp", "dp"),
        P("dp"),
        P("dp"),
        P(),
        P("dp"),
    )
    return jax.shard_map(
        functools.partial(on_device, mesh.shape["dp"], mesh.shape["mp"]),
        mesh=mesh,
        in_specs=placed,
        out_specs=P("dp", "mp"),
        check_vma=False,
    )
```

```python
import functools
import math

import jax
import jax.numpy as jnp
from jax import lax
from jax.experimental import pallas as pl
from jax.experimental.pallas import tpu as pltpu
from jax.sharding import PartitionSpec as P

HEAD_SIZE = 128
EXTRA = 4
QUARTERS = 4
MESH = pl.DeviceIdType.MESH

masked_score = -1e30
f32 = jnp.float32
bf16 = jnp.bfloat16


def iota(shape, dim):
    return lax.broadcasted_iota(jnp.int32, shape, dim)


def ring(k, n):
    return min(k, n - k)


def to_column(row):
    n = row.shape[1]
    eye = iota((n, n), 0) == iota((n, n), 1)
    return jnp.sum(jnp.where(eye, row, 0.0), axis=1, keepdims=True)


def to_row(column):
    n = column.shape[0]
    eye = iota((n, n), 0) == iota((n, n), 1)
    return jnp.sum(jnp.where(eye, column, 0.0), axis=0, keepdims=True)


def dot(a, b):
    return jnp.dot(a, b, preferred_element_type=f32)


def one_hot(mask):
    return jnp.where(mask, 1.0, 0.0).astype(bf16)


def layer_kernel(
    dp,
    mp,
    query_hbm,
    new_key_hbm,
    new_value_hbm,
    key_scale_hbm,
    value_scale_hbm,
    task_hbm,
    length_hbm,
    slot_hbm,
    owner_hbm,
    key_hbm,
    value_hbm,
    weight_hbm,
    out_ref,
    query_ref,
    new_key_ref,
    new_value_ref,
    key_scale_ref,
    value_scale_ref,
    task_ref,
    length_ref,
    slot_ref,
    owner_ref,
    keys,
    values,
    weights_in,
    weights_over,
    send_rows,
    send_extra,
    recv_rows,
    recv_extra,
    home_send,
    home_recv,
    selector,
    factor,
    contexts,
    block,
    partial,
    send_part,
    recv_part,
    local_sem,
    small_sem,
    send_sem,
    request_recv,
    home_recv_sem,
    weight_recv,
    over_recv,
    context_recv,
    part_recv,
):
    me = lax.axis_index("dp")
    part = lax.axis_index("mp")
    rows, query_width = query_ref.shape
    heads = query_width // HEAD_SIZE
    task_total = key_scale_ref.shape[0]
    slots, positions, _ = keys.shape
    columns = weights_in.shape[3]
    inner = dp // mp
    outer = mp
    z, y = me // inner, lax.rem(me, inner)
    chip, core = part // 2, lax.rem(part, 2)
    other = 2 * chip + 1 - core

    def at(kz, ky):
        return lax.rem(z + kz, outer) * inner + lax.rem(y + ky, inner)

    def distance(offset):
        return ring(offset[0], outer) + ring(offset[1], inner)

    def back(offset):
        return (outer - offset[0]) % outer, (inner - offset[1]) % inner

    near = sorted(((kz, ky) for kz in range(outer) for ky in range(inner)), key=distance)
    far = near[:0:-1]

    def remote(source, target, send_sem, recv_sem, device):
        return pltpu.make_async_remote_copy(
            src_ref=source,
            dst_ref=target,
            send_sem=send_sem,
            recv_sem=recv_sem,
            device_id=device,
            device_id_type=MESH,
        )

    def signal(sem, device):
        pl.semaphore_signal(sem, inc=1, device_id=device, device_id_type=MESH)

    up, down = at(0, 1), at(0, inner - 1)
    y_up, y_down, y_far = (lax.rem(y + k, inner) for k in (1, inner - 1, 2))

    def up_copy(source, q, relay):
        piece = weights_in.at[source, q]
        return remote(piece, piece, send_sem.at[2], weight_recv.at[q + 4 * relay], (up, part))

    def down_copy(source, q, relay):
        piece = weights_in.at[source, q]
        return remote(piece, piece, send_sem.at[2], weight_recv.at[6 + q + 2 * relay], (down, part))

    def over_copy(k, source, q):
        return remote(
            weights_in.at[source, q],
            weights_over.at[source, q],
            send_sem.at[3],
            over_recv.at[k],
            (me, other),
        )

    def over_in(k, source):
        return remote(
            weights_in.at[source],
            weights_over.at[source],
            send_sem.at[3],
            over_recv.at[k],
            (me, other),
        )

    with jax.named_scope("a_greet"):
        small = [
            pltpu.make_async_copy(away, here, small_sem.at[i])
            for i, (away, here) in enumerate(
                (
                    (task_hbm, task_ref),
                    (owner_hbm, owner_ref),
                    (slot_hbm, slot_ref),
                    (length_hbm, length_ref),
                    (query_hbm, query_ref),
                    (key_scale_hbm, key_scale_ref),
                    (value_scale_hbm, value_scale_ref),
                    (new_key_hbm, new_key_ref),
                    (new_value_hbm, new_value_ref),
                )
            )
        ]
        for copy in small:
            copy.start()
        barrier = pltpu.get_barrier_semaphore()
        for kz, ky in far:
            signal(barrier, (at(kz, ky), part))
        for k in range(1, mp):
            signal(barrier, (me, lax.rem(part + k, mp)))
        fetches = [
            pltpu.make_async_copy(weight_hbm, weights_in.at[y], local_sem.at[2]),
            pltpu.make_async_copy(key_hbm, keys, local_sem.at[0]),
            pltpu.make_async_copy(value_hbm, values, local_sem.at[1]),
        ]
        for fetch in fetches:
            fetch.start()
    with jax.named_scope("a_first"):
        for copy in small:
            copy.wait()

    with jax.named_scope("b_pack"):
        task_column = to_column(task_ref[...].astype(f32))
        length_column = to_column(length_ref[...].astype(f32))
        slot_column = to_column(slot_ref[...].astype(f32))
        picked = task_column == iota((rows, task_total), 1).astype(f32)
        owner_column = jnp.sum(
            jnp.where(picked, owner_ref[...].astype(f32), 0.0), axis=1, keepdims=True
        )
        owner_row = to_row(owner_column)
        task_rows = one_hot(picked)
        key_factor = dot(task_rows, key_scale_ref[...])
        factor[...] = dot(task_rows, value_scale_ref[...])
        pieces = []
        for h in range(heads):
            lanes = slice(h * HEAD_SIZE, (h + 1) * HEAD_SIZE)
            pieces.append((query_ref[:, lanes].astype(f32) * key_factor).astype(bf16))
        pieces.append(new_key_ref[...])
        pieces.append(new_value_ref[...])
        pieces.append(jnp.broadcast_to(slot_column, (rows, HEAD_SIZE)).astype(bf16))
        pieces.append(jnp.broadcast_to(length_column, (rows, HEAD_SIZE)).astype(bf16))
        wide = len(pieces) * rows
        spread = one_hot(lax.rem(iota((rows, wide), 1), rows) == iota((rows, wide), 0))
        owner_wide = dot(owner_row.astype(bf16), spread)
        ready_rows = jnp.concatenate(pieces, axis=0)
        for into, first, count in ((send_rows, 0, heads), (send_extra, heads, EXTRA)):
            line = iota((dp * count, wide), 0)
            lane = iota((dp * count, wide), 1)
            packer = one_hot(
                (lax.rem(line, count) + first == lane // rows)
                & ((line // count).astype(f32) == owner_wide)
            )
            into[...] = dot(packer, ready_rows).astype(bf16).reshape(dp, count, HEAD_SIZE)
        line = iota((heads * rows, dp * heads), 0)
        lane = iota((heads * rows, dp * heads), 1)
        same = lax.rem(iota((heads * rows, rows), 0), rows) == iota((heads * rows, rows), 1)
        owner_tall = jnp.sum(jnp.where(same, owner_row, 0.0), axis=1, keepdims=True)
        selector[...] = one_hot(
            (line // rows == lax.rem(lane, heads)) & ((lane // heads).astype(f32) == owner_tall)
        )

    def request_copy(offset):
        return [
            remote(
                source.at[at(*offset)],
                target.at[me],
                send_sem.at[sem],
                request_recv.at[n],
                (at(*offset), part),
            )
            for n, (source, target, sem) in enumerate(
                ((send_rows, recv_rows, 0), (send_extra, recv_extra, 6))
            )
        ]

    def requests_in():
        pages = pl.ds(0, dp - 1)
        return [
            remote(
                source.at[pages],
                target.at[pages],
                send_sem.at[sem],
                request_recv.at[n],
                (me, other),
            )
            for n, (source, target, sem) in enumerate(
                ((send_rows, recv_rows, 0), (send_extra, recv_extra, 6))
            )
        ]

    def home_copy(offset):
        return remote(
            home_send.at[at(*offset)],
            home_recv.at[me],
            send_sem.at[1],
            home_recv_sem.at[0],
            (at(*offset), part),
        )

    def homes_in():
        pages = pl.ds(0, dp - 1)
        return remote(
            home_send.at[pages],
            home_recv.at[pages],
            send_sem.at[1],
            home_recv_sem.at[0],
            (me, other),
        )

    with jax.named_scope("c_barwait"):
        pl.semaphore_wait(barrier, dp + mp - 2)
    with jax.named_scope("d_reqsend"):
        for offset in far:
            for copy in request_copy(offset):
                copy.start()
        recv_rows[me] = send_rows[me]
        recv_extra[me] = send_extra[me]
        fetches[0].wait()
        up_copy(y, 0, 0).start()
        down_copy(y, 2, 0).start()
        up_copy(y, 1, 0).start()
        down_copy(y, 3, 0).start()
        for q in range(QUARTERS):
            over_copy(0, y, q).start()
        fetches[1].wait()
        fetches[2].wait()

    inv_root = 1.0 / math.sqrt(HEAD_SIZE)
    key_line = lax.rem(iota((heads, positions), 1), HEAD_SIZE).astype(f32)

    def attend(sources):
        queries, extras, picks, limits = [], [], [], []
        for s in sources:
            queries.append(recv_rows[s])
            extra = recv_extra[s].astype(f32)
            extras.append(extra)
            picks.append(jnp.clip(jnp.max(extra[2:3]).astype(jnp.int32), 0, slots - 1))
            length = jnp.broadcast_to(extra[3:4], (heads, HEAD_SIZE))
            limits.append(
                jnp.concatenate(
                    [length - i * HEAD_SIZE for i in range(positions // HEAD_SIZE)], axis=1
                )
            )
        scores = [
            lax.dot_general(
                q, keys[p], (((1,), (1,)), ((), ())), preferred_element_type=f32
            )
            * inv_root
            for q, p in zip(queries, picks)
        ]
        owns = [
            jnp.sum(q.astype(f32) * extra[0:1], axis=1, keepdims=True) * inv_root
            for q, extra in zip(queries, extras)
        ]
        shown = [
            jnp.where(key_line < limit, score, masked_score)
            for score, limit in zip(scores, limits)
        ]
        tops = [
            jnp.maximum(jnp.max(score, axis=1, keepdims=True), own)
            for score, own in zip(shown, owns)
        ]
        weights = [
            jnp.where(key_line < limit, jnp.exp(score - top), 0.0)
            for score, limit, top in zip(shown, limits, tops)
        ]
        own_weights = [jnp.exp(own - top) for own, top in zip(owns, tops)]
        blends = [dot(weight.astype(bf16), values[p]) for weight, p in zip(weights, picks)]
        sums = [
            jnp.sum(weight, axis=1, keepdims=True) + own
            for weight, own in zip(weights, own_weights)
        ]
        for s, blend, own, extra, total in zip(sources, blends, own_weights, extras, sums):
            blended = blend + own.astype(bf16).astype(f32) * extra[1:2]
            home_send[s] = (blended / total).astype(bf16)

    with jax.named_scope("e_reqwait"):
        for copy in requests_in():
            copy.wait_recv()
    for group in (near[-12:], near[:-12]):
        with jax.named_scope("f_attend"):
            attend([at(*back(offset)) for offset in group])
        with jax.named_scope("g_homesend"):
            for offset in reversed(group):
                if offset != (0, 0):
                    home_copy(back(offset)).start()
    home_recv[me] = home_send[me]

    with jax.named_scope("j_relay"):
        up_copy(y, 2, 0).start()
        down_copy(y, 0, 0).start()
        up_copy(y, 3, 0).start()
        down_copy(y, 1, 0).start()
        for q in (0, 1):
            up_copy(y_down, q, 0).wait_recv()
            up_copy(y_down, q, 1).start()
            over_copy(1, y_down, q).start()
            down_copy(y_up, q + 2, 0).wait_recv()
            down_copy(y_up, q + 2, 1).start()
            over_copy(2, y_up, q + 2).start()
    with jax.named_scope("k_homewait"):
        homes_in().wait_recv()

    mine = lax.rem(z, 2)

    with jax.named_scope("l_compact"):
        chosen = dot(selector[...], home_recv[...].reshape(dp * heads, HEAD_SIZE))
        for h in range(heads):
            block[:, h * HEAD_SIZE : (h + 1) * HEAD_SIZE] = (
                chosen[h * rows : (h + 1) * rows] * factor[...]
            ).astype(bf16)

    homes = outer // 2
    middle = query_width // 2
    quarter = query_width // QUARTERS

    def place(source, home):
        return source * homes + lax.rem(home, outer) // 2

    spans = ((0, QUARTERS - 1), (QUARTERS - 1, QUARTERS))

    def half_of(ref, half):
        first, last = spans[half]
        return ref.at[..., pl.ds(first * quarter, (last - first) * quarter)]

    def context_copy(k, half):
        return remote(
            half_of(block, half),
            half_of(contexts.at[place(core, z)], half),
            send_sem.at[4],
            context_recv.at[half],
            (at(k, 0), 2 * chip + mine),
        )

    def contexts_in(half, count):
        blocks = half_of(contexts.at[pl.ds(0, count)], half)
        return remote(blocks, blocks, send_sem.at[4], context_recv.at[half], (me, other))

    def contexts_out(count):
        blocks = contexts.at[pl.ds(0, count)]
        return remote(blocks, blocks, send_sem.at[4], context_recv.at[0], (me, other))

    with jax.named_scope("m_ctxsend"):
        for half in range(2):
            for k in (4, 3, 5, 2, 6, 1, 7):
                context_copy(k, half).start()

            @pl.when(mine != core)
            def _():
                context_copy(0, half).start()

        @pl.when(mine == core)
        def _():
            contexts[place(core, z)] = block[...]

    with jax.named_scope("n_overs"):
        for q in (0, 1):
            up_copy(y_down, q + 2, 0).wait_recv()
            over_copy(1, y_down, q + 2).start()
            down_copy(y_up, q, 0).wait_recv()
            over_copy(2, y_up, q).start()

    def context_wait(half):
        @pl.when(mine == core)
        def _():
            contexts_in(half, 2 * homes - 1).wait_recv()

        @pl.when(mine != core)
        def _():
            contexts_in(half, 2 * homes).wait_recv()

    shift = lax.rem(z + core, 2)

    def part_copy(n, column, i):
        target = lax.rem(z + 2 * i + shift, outer)
        return remote(
            send_part.at[column, target // 2],
            recv_part.at[column, chip],
            send_sem.at[5],
            part_recv.at[n],
            (target * inner + y, z),
        )

    def parts_in(n, count):
        parts = pl.ds(0, count)
        return remote(
            send_part.at[0, parts],
            recv_part.at[0, parts],
            send_sem.at[5],
            part_recv.at[n],
            (me, other),
        )

    order = (y, y_down, y_up, y_far)

    def half_sum(column, half):
        total = jnp.zeros((homes * rows, columns), f32)
        for q in range(*spans[half]):
            lanes = slice(q * quarter, (q + 1) * quarter)
            for source, weight in ((core, weights_in), (1 - core, weights_over)):
                piece = contexts[pl.ds(source * homes, homes), :, lanes]
                total = total + dot(
                    piece.reshape(homes * rows, quarter), weight[column, q]
                )
        return total

    def far_sum(column):
        total = jnp.zeros((homes * rows, columns), f32)
        for source, weight in ((core, weights_in), (1 - core, weights_over)):
            if weight is weights_over:
                over_in(inner - 1, column).wait_recv()
            for q in range(QUARTERS):
                piece = contexts[
                    pl.ds(source * homes, homes), :, q * quarter : (q + 1) * quarter
                ]
                total = total + dot(
                    piece.reshape(homes * rows, quarter), weight[column, q]
                )
        return total

    with jax.named_scope("o_ctxwait"):
        context_wait(0)
    with jax.named_scope("o_first"):
        for n, column in enumerate(order[:-1]):
            over_in(n, column).wait_recv()
            partial[n] = half_sum(column, 0)
    with jax.named_scope("o_ctxwait2"):
        context_wait(1)
    with jax.named_scope("p_project"):
        for n, column in enumerate(order):
            if n == 3:
                for m in (0, 1):
                    up_copy(y_far, m, 1).wait_recv()
                    over_copy(3, y_far, m).start()
                    down_copy(y_far, m + 2, 1).wait_recv()
                    over_copy(3, y_far, m + 2).start()
            if n < inner - 1:
                summed = partial[n] + half_sum(column, 1)
            else:
                summed = far_sum(column)
            send_part[column] = summed.astype(bf16).reshape(homes, rows, columns)
            for i in (2, 1, 3):
                part_copy(n, column, i).start()

            @pl.when(z != part)
            def _():
                part_copy(n, column, 0).start()

            @pl.when(z == part)
            def _():
                recv_part[column, chip] = send_part[column, z // 2]

    with jax.named_scope("q_drain"):
        for copy in requests_in():
            copy.wait_send()
        homes_in().wait_send()
        three = weights_in.at[pl.ds(0, inner - 1)]
        remote(three, three, send_sem.at[2], weight_recv.at[0], (me, other)).wait_send()
        remote(weights_in, weights_over, send_sem.at[3], over_recv.at[0], (me, other)).wait_send()

        @pl.when(mine == core)
        def _():
            contexts_out(2 * homes - 1).wait_send()

        @pl.when(mine != core)
        def _():
            contexts_out(2 * homes).wait_send()

    with jax.named_scope("r_partwait"):
        for n, column in enumerate(order):

            @pl.when(z != part)
            def _():
                parts_in(n, mp // 2).wait_recv()

            @pl.when(z == part)
            def _():
                parts_in(n, mp // 2 - 1).wait_recv()

            summed = recv_part[column, 0].astype(f32)
            for j in range(1, mp // 2):
                summed = summed + recv_part[column, j].astype(f32)
            start = pl.multiple_of(column * columns, columns)
            out_ref[:, pl.ds(start, columns)] = summed.astype(bf16)

    with jax.named_scope("s_drain"):

        @pl.when(z != part)
        def _():
            remote(send_part, send_part, send_sem.at[5], part_recv.at[0], (me, other)).wait_send()

        @pl.when(z == part)
        def _():
            most = send_part.at[:, pl.ds(0, mp // 2 - 1)]
            remote(most, most, send_sem.at[5], part_recv.at[0], (me, other)).wait_send()


def on_device(
    dp,
    mp,
    queries,
    incoming_key,
    incoming_value,
    key_cache,
    cached_values,
    task_key_scale,
    task_value_scale,
    out_weight,
    task_id,
    cached_length,
    task_owner,
    cache_slot,
):
    rows, query_width = queries.shape
    depth, columns = out_weight.shape
    heads = query_width // HEAD_SIZE
    inner = dp // mp
    small = (
        queries,
        incoming_key,
        incoming_value,
        task_key_scale,
        task_value_scale,
        task_id.reshape(1, -1),
        cached_length.reshape(1, -1),
        cache_slot.reshape(1, -1),
        task_owner.reshape(1, -1),
    )
    away = pl.BlockSpec(memory_space=pltpu.HBM)
    return pl.pallas_call(
        functools.partial(layer_kernel, dp, mp),
        out_shape=jax.ShapeDtypeStruct((rows, inner * columns), bf16),
        in_specs=[away] * 12,
        out_specs=pl.BlockSpec(memory_space=pltpu.VMEM),
        scratch_shapes=[pltpu.VMEM(array.shape, array.dtype) for array in small]
        + [
            pltpu.VMEM(key_cache.shape, bf16),
            pltpu.VMEM(cached_values.shape, bf16),
            pltpu.VMEM((inner, QUARTERS, depth // QUARTERS, columns), bf16),
            pltpu.VMEM((inner, QUARTERS, depth // QUARTERS, columns), bf16),
            pltpu.VMEM((dp, heads, HEAD_SIZE), bf16),
            pltpu.VMEM((dp, EXTRA, HEAD_SIZE), bf16),
            pltpu.VMEM((dp, heads, HEAD_SIZE), bf16),
            pltpu.VMEM((dp, EXTRA, HEAD_SIZE), bf16),
            pltpu.VMEM((dp, heads, HEAD_SIZE), bf16),
            pltpu.VMEM((dp, heads, HEAD_SIZE), bf16),
            pltpu.VMEM((heads * rows, dp * heads), bf16),
            pltpu.VMEM((rows, HEAD_SIZE), f32),
            pltpu.VMEM((mp, rows, query_width), bf16),
            pltpu.VMEM((rows, query_width), bf16),
            pltpu.VMEM((inner - 1, mp // 2 * rows, columns), f32),
            pltpu.VMEM((inner, mp // 2, rows, columns), bf16),
            pltpu.VMEM((inner, mp // 2, rows, columns), bf16),
            pltpu.SemaphoreType.DMA((3,)),
            pltpu.SemaphoreType.DMA((len(small),)),
            pltpu.SemaphoreType.DMA((7,)),
            pltpu.SemaphoreType.DMA((2,)),
            pltpu.SemaphoreType.DMA((1,)),
            pltpu.SemaphoreType.DMA((12,)),
            pltpu.SemaphoreType.DMA((inner,)),
            pltpu.SemaphoreType.DMA((3,)),
            pltpu.SemaphoreType.DMA((inner,)),
        ],
        compiler_params=pltpu.CompilerParams(
            collective_id=0, has_side_effects=True, vmem_limit_bytes=20 * 1024 * 1024
        ),
    )(
        *[
            pltpu.with_memory_space_constraint(array, pltpu.HBM)
            for array in (
                *small,
                key_cache,
                cached_values,
                out_weight.reshape(QUARTERS, depth // QUARTERS, columns),
            )
        ]
    )


def solution(mesh):
    placed = (
        P("dp", "mp"),
        P("dp", "mp"),
        P("dp", "mp"),
        P("dp", None, "mp"),
        P("dp", None, "mp"),
        P(None, "mp"),
        P(None, "mp"),
        P("mp", "dp"),
        P("dp"),
        P("dp"),
        P(),
        P("dp"),
    )
    return jax.shard_map(
        functools.partial(on_device, mesh.shape["dp"], mesh.shape["mp"]),
        mesh=mesh,
        in_specs=placed,
        out_specs=P("dp", "mp"),
        check_vma=False,
    )
```
